32 devices in a mesh: gx: 2 (over y), gy: 4 (over z), gz: 4 (over x, core).
Axes of the slice: x: 2, y: 2, z: 4, core: 2. Of those that a mesh axis runs over, the one named last changes fastest.
Arguments:
- density: float32 [64, 64, 512], P('gx', 'gy', 'gz'), may hold values from -8 to 8
Outputs:
- potential: float32 [64, 64, 512], P('gx', 'gy', 'gz')
The draws below stay inside these ranges and needn't reach their ends.
All inputs are finite; a program needn't handle non-finite values.
Results may differ from the reference program's by a relative error of at most 0.00002.
Values sent between devices are 32-bit elements; how exact they have to be, the bound alone decides.
A program may use at most 128 MiB of HBM per device.

```python
import jax
import jax.numpy as jnp
from jax import lax

LEVELS = 7
CSWEEPS = 4
NX = 64
NY = 64
NZ = 512


def rough_field(key, shape):
    return jnp.clip(jax.random.normal(key, shape, jnp.float32), -4.0, 4.0)


def draw_density(key, part):
    first_key = jax.random.fold_in(key, 21)
    second_key = jax.random.fold_in(key, 22)
    shape = (NX, NY, NZ)
    first = rough_field(first_key, shape)
    second = rough_field(second_key, shape)
    beside_all = jnp.zeros(shape, jnp.float32)
    for which in range(3):
        beside_all = beside_all + jnp.roll(first, 1, which) + jnp.roll(first, -1, which)
    sharp = 6.0 * first - beside_all
    total = 0.4 * sharp + 0.4 * second
    return jnp.clip(total, -8.0, 8.0).astype(jnp.float32)


def setup_inputs(seed: int = 0) -> dict:
    key_of = jax.random.split(jax.random.key(seed), 2)
    density = draw_density(jax.random.fold_in(key_of[1], 71), 0)
    return dict(density=density)


rsd_beta = 0.5
centre = 4.0 + 2.0 * (1.0 + rsd_beta)


def stencil_sum(padded):
    plane = padded[2:, 1:-1, 1:-1] + padded[:-2, 1:-1, 1:-1] + padded[1:-1, 2:, 1:-1] + padded[1:-1, :-2, 1:-1]
    sight = padded[1:-1, 1:-1, 2:] + padded[1:-1, 1:-1, :-2]
    return plane + (1.0 + rsd_beta) * sight


def parity_of(shape):
    total = lax.broadcasted_iota(jnp.int32, shape, 0) + lax.broadcasted_iota(jnp.int32, shape, 1)
    total = total + lax.broadcasted_iota(jnp.int32, shape, 2)
    return total % 2


def half_sweep(field, source, scale, chosen):
    update = (source / scale + stencil_sum(jnp.pad(field, 1))) / centre
    return jnp.where(chosen, update, field)


def full_sweep(field, source, scale, parity):
    field = half_sweep(field, source, scale, parity == 0)
    return half_sweep(field, source, scale, parity == 1)


def restrict(residue):
    shape = residue.shape
    blocks = residue.reshape(shape[0] // 2, 2, shape[1] // 2, 2, shape[2] // 2, 2)
    return jnp.mean(blocks, axis=(1, 3, 5))


def prolong(coarse):
    return jnp.repeat(jnp.repeat(jnp.repeat(coarse, 2, 0), 2, 1), 2, 2)


def local_cycle(source, level):
    scale = 0.25 ** level
    parity = parity_of(source.shape)
    field = jnp.zeros_like(source)
    if level == LEVELS - 1:
        for number in range(CSWEEPS):
            field = full_sweep(field, source, scale, parity)
        return field
    for number in range(2):
        field = full_sweep(field, source, scale, parity)
    residue = source - scale * (centre * field - stencil_sum(jnp.pad(field, 1)))
    field = field + prolong(local_cycle(restrict(residue), level + 1))
    for number in range(2):
        field = full_sweep(field, source, scale, parity)
    return field


def reference(density):
    return local_cycle(density, 0)
```

```python
import functools

import jax
import jax.numpy as jnp
import numpy as np
from jax import lax
from jax.experimental import pallas as pl
from jax.experimental.pallas import tpu as pltpu
from jax.sharding import PartitionSpec as P

LEVELS = 7
CSWEEPS = 4
DENSE = 512
rsd_beta = 0.5
centre = 4.0 + 2.0 * (1.0 + rsd_beta)
along = 1.0 + rsd_beta
inverse = 1.0 / centre
F32 = jnp.float32
BF16 = jnp.bfloat16
LANES = 128
AXES = ("gx", "gy", "gz")
MESH = pl.DeviceIdType.MESH
DIRECTIONS = [
    (dx, dy, dz) for dx in (-1, 0, 1) for dy in (-1, 0, 1) for dz in (-1, 0, 1) if (dx, dy, dz) != (0, 0, 0)
]
STEPS_XY = [(dx, dy) for dx in (-1, 0, 1) for dy in (-1, 0, 1) if (dx, dy) != (0, 0)]


def up_to(value, unit):
    return -(-value // unit) * unit


def iota(shape, dim):
    return lax.broadcasted_iota(jnp.int32, shape, dim)


def pieces(value):
    high = value.astype(BF16)
    rest = value - high.astype(F32)
    middle = rest.astype(BF16)
    return high, middle, (rest - middle.astype(F32)).astype(BF16)


def product(left, right):
    return jnp.dot(left, right, preferred_element_type=F32)


def dot(value, chosen):
    chosen = chosen.astype(BF16)
    parts = [product(part, chosen) for part in pieces(value)]
    return parts[0] + (parts[1] + parts[2])


def local_of(index, length, margin, total):
    return jnp.where(index < total - margin, index, index - total)


def half_down(value):
    return jnp.where(value >= 0, lax.div(value, 2), -lax.div(1 - value, 2))


def parity_of(rows, lanes):
    return (iota((rows, lanes), 0) + iota((rows, lanes), 1)) % 2 == 0


def beside(below, here, above, even, colour, edge):
    rows, lanes = here.shape
    down, up = pltpu.roll(here, 1, 0), pltpu.roll(here, rows - 1, 0)
    left, right = pltpu.roll(here, 1, 1), pltpu.roll(here, lanes - 1, 1)
    if edge is not None:
        if edge[0] == rows:
            row = iota(here.shape, 0)
            down = jnp.where(row == 0, 0.0, down)
            up = jnp.where(row == rows - 1, 0.0, up)
        if edge[1] == lanes:
            lane = iota(here.shape, 1)
            left = jnp.where(lane == 0, 0.0, left)
            right = jnp.where(lane == lanes - 1, 0.0, right)
    other = jnp.where(even, below, above) if colour == 0 else jnp.where(even, above, below)
    return (here + other) + (down + up) + along * (left + right)


class Grid:
    def __init__(self, block, margins, edge=False):
        self.block, self.margins = block, margins
        self.inner = block[0] // 2
        self.count = self.inner + 2 * margins[0]
        self.rows = up_to(block[1] + 2 * margins[1], 8)
        self.lanes = up_to(block[2] + 2 * margins[2], LANES)
        self.edge = (block[1], block[2]) if edge else None

    def scratch(self, name):
        field = (self.count + 2, self.rows, self.lanes)
        source = (self.count, self.rows, self.lanes)
        return {
            name + "R": pltpu.VMEM(field, F32),
            name + "B": pltpu.VMEM(field, F32),
            name + "f": pltpu.VMEM(source, F32),
            name + "g": pltpu.VMEM(source, F32),
            name + "m": pltpu.VMEM((3, self.rows, self.lanes), F32),
        }

    def zone(self, number):
        if number < self.margins[0]:
            return 0
        return 2 if number >= self.count - self.margins[0] else 1

    def guard(self, s, name):
        empty = jnp.zeros((self.rows, self.lanes), F32)
        for key in "RB":
            s[name + key][0] = empty
            s[name + key][self.count + 1] = empty

    def masks(self, s, name, place, counts):
        inside = None
        shape = (self.rows, self.lanes)
        for dim in (1, 2):
            index = iota(shape, dim - 1)
            size = shape[dim - 1]
            margin, length = self.margins[dim], self.block[dim]
            used = (index < length + margin) | (index >= size - margin)
            spot = local_of(index, length, margin, size) + place[dim] * length
            used = used & (spot >= 0) & (spot < length * counts[dim])
            inside = used if inside is None else inside & used
        value = jnp.where(inside, inverse, 0.0).astype(F32)
        s[name + "m"][1] = value
        if self.margins[0]:
            low = jnp.where(place[0] > 0, 1.0, 0.0).astype(F32)
            high = jnp.where(place[0] < counts[0] - 1, 1.0, 0.0).astype(F32)
            s[name + "m"][0] = value * low
            s[name + "m"][2] = value * high

    def first(self, s, name, begin, end):
        for number in range(begin, end):
            s[name + "R"][number + 1] = s[name + "f"][number] * s[name + "m"][self.zone(number)]

    def totals(self, other, even, colour, begin, end):
        before, here = other[begin], other[begin + 1]
        for number in range(begin, end):
            after = other[number + 2]
            yield number, beside(before, here, after, even, colour, self.edge)
            before, here = here, after

    def half(self, s, name, colour, even, begin, end):
        target, other = (s[name + "R"], s[name + "B"]) if colour == 0 else (s[name + "B"], s[name + "R"])
        source = s[name + ("f" if colour == 0 else "g")]
        for number, total in self.totals(other, even, colour, begin, end):
            target[number + 1] = (source[number] + total) * s[name + "m"][self.zone(number)]

    def residue(self, s, name, even, begin, end):
        for number, total in self.totals(s[name + "B"], even, 0, begin, end):
            yield number, s[name + "f"][number] - centre * s[name + "R"][number + 1] + total

    def planes(self, s, name, even, plane):
        red, black = s[name + "R"][plane // 2 + 1], s[name + "B"][plane // 2 + 1]
        return jnp.where(even, red, black) if plane % 2 == 0 else jnp.where(even, black, red)


def exists(place, steps, counts):
    found = None
    for which in range(3):
        if steps[which] == 0:
            continue
        other = place[which] + steps[which]
        here = (other >= 0) & (other < counts[which])
        found = here if found is None else found & here
    return found


def device(place, steps):
    return tuple(place[which] + steps[which] for which in range(3))


def back(steps):
    return tuple(-step for step in steps)


class Exchange:
    def __init__(self, level, place, counts, array, refs):
        self.level, self.place, self.counts, self.array = level, place, counts, array
        self.block = (level.inner, level.block[1], level.block[2])
        self.margins = level.margins
        self.per = LANES // level.margins[2]
        self.packs = -(-level.count // self.per)
        (self.stage_x, self.land_x, self.land_y, self.stage_y) = refs[:4]
        (self.stage_z, self.land_z, self.sent, self.got) = refs[4:]

    @staticmethod
    def scratch(level, name):
        per = LANES // level.margins[2]
        packs = -(-level.count // per)
        margin, rows = level.margins, level.block[1]
        shapes = [
            (2, margin[0], rows, LANES),
            (2, margin[0], rows, LANES),
            (2, level.count, margin[1], LANES),
            (2, level.inner, margin[1], LANES),
            (2, packs, level.rows, LANES),
            (2, packs, level.rows, LANES),
        ]
        out = {name + str(number): pltpu.VMEM(shape, F32) for number, shape in enumerate(shapes)}
        out[name + "6"] = pltpu.SemaphoreType.DMA((10,))
        out[name + "7"] = pltpu.SemaphoreType.DMA((10,))
        return out

    def xy(self, number):
        dx, dy = STEPS_XY[number]
        margin, length = self.margins[0], self.block[0]
        place = {1: 0, 0: margin, -1: margin + length}[dx]
        count = length if dx == 0 else margin
        origin = length - margin if dx == 1 else 0
        if dy == 0:
            source = self.stage_x.at[(dx + 1) // 2]
            target = self.land_x.at[(dx + 1) // 2]
        else:
            source = self.stage_y.at[(dy + 1) // 2, pl.ds(origin, count)]
            target = self.land_y.at[(dy + 1) // 2, pl.ds(place, count)]
        return (dx, dy, 0), (place, count), pltpu.make_async_remote_copy(
            src_ref=source,
            dst_ref=target,
            send_sem=self.sent.at[number],
            recv_sem=self.got.at[number],
            device_id=device(self.place, (dx, dy, 0)),
            device_id_type=MESH,
        )

    def start_xy(self):
        array, margin = self.array, self.margins
        low = 1 + margin[0]
        length, rows = self.block[0], self.block[1]
        self.stage_y[0] = array[low : low + length, 0 : margin[1], 0:LANES]
        self.stage_y[1] = array[low : low + length, rows - margin[1] : rows, 0:LANES]
        self.stage_x[0] = array[low : low + margin[0], 0:rows, 0:LANES]
        self.stage_x[1] = array[low + length - margin[0] : low + length, 0:rows, 0:LANES]
        for number in range(8):
            steps, _, copy = self.xy(number)

            @pl.when(exists(self.place, steps, self.counts))
            def _():
                copy.start()

    def finish_xy(self):
        array, rows, margin = self.array, self.block[1], self.margins[1]
        for number in range(8):
            steps, (place, count), copy = self.xy(number)

            @pl.when(exists(self.place, back(steps), self.counts))
            def _():
                copy.wait_recv()
                low = 1 + place
                if steps[1] == 0:
                    array[low : low + count, 0:rows, 0:LANES] = self.land_x[(steps[0] + 1) // 2]
                else:
                    first = self.level.rows - margin if steps[1] == 1 else rows
                    side = (steps[1] + 1) // 2
                    array[low : low + count, first : first + margin, 0:LANES] = self.land_y[
                        side, place : place + count
                    ]

    def z(self, side):
        return pltpu.make_async_remote_copy(
            src_ref=self.stage_z.at[side],
            dst_ref=self.land_z.at[side],
            send_sem=self.sent.at[8 + side],
            recv_sem=self.got.at[8 + side],
            device_id=device(self.place, (0, 0, 2 * side - 1)),
            device_id_type=MESH,
        )

    def start_z(self):
        level, array = self.level, self.array
        margin, length = self.margins[2], self.block[2]
        lane = iota((level.rows, LANES), 1)
        for side in range(2):
            first = length - margin if side == 1 else 0
            for pack in range(self.packs):
                total = jnp.zeros((level.rows, LANES), F32)
                for number in range(min(self.per, level.count - pack * self.per)):
                    plane = array[1 + pack * self.per + number, :, 0:LANES]
                    moved = pltpu.roll(plane, (number * margin - first) % LANES, 1)
                    total = jnp.where(lane // margin == number, moved, total)
                self.stage_z[side, pack] = total
        for side in range(2):
            @pl.when(exists(self.place, (0, 0, 2 * side - 1), self.counts))
            def _():
                self.z(side).start()

    def finish_z(self):
        level, array = self.level, self.array
        margin, length = self.margins[2], self.block[2]
        base = level.lanes - LANES
        lane = iota((level.rows, LANES), 1)
        have = []
        for side in range(2):
            there = exists(self.place, (0, 0, 1 - 2 * side), self.counts)
            have.append(there)

            @pl.when(there)
            def _():
                self.z(side).wait_recv()

        above = length - base
        take_above = (lane >= above) & (lane < above + margin) & have[0]
        take_below = (lane >= LANES - margin) & have[1]
        for pack in range(self.packs):
            from_above, from_below = self.land_z[0, pack], self.land_z[1, pack]
            for number in range(min(self.per, level.count - pack * self.per)):
                plane = 1 + pack * self.per + number
                high = pltpu.roll(from_above, (above - number * margin) % LANES, 1)
                low = pltpu.roll(from_below, (LANES - margin - number * margin) % LANES, 1)
                value = array[plane, :, base : level.lanes]
                value = jnp.where(take_above, high, value)
                array[plane, :, base : level.lanes] = jnp.where(take_below, low, value)

    def drain(self):
        for number in range(8):
            steps, _, copy = self.xy(number)

            @pl.when(exists(self.place, steps, self.counts))
            def _():
                copy.wait_send()

        for side in range(2):
            @pl.when(exists(self.place, (0, 0, 2 * side - 1), self.counts))
            def _():
                self.z(side).wait_send()


class Plan:
    def __init__(self, block, counts):
        self.counts, self.block = counts, block
        self.total = counts[0] * counts[1] * counts[2]
        self.block1 = tuple(size // 2 for size in block)
        self.block2 = tuple(size // 4 for size in block)
        self.top = Grid(block, (2, 4, 4))
        self.wide = Grid(block, (4, 8, 8))
        self.next = Grid(self.block1, (3, 8, 8))
        self.width = up_to(block[2], LANES)
        self.tiles = self.top.lanes // LANES
        self.count = self.top.count
        self.high = self.block1[1] + 8
        self.per = LANES // self.block1[2]
        self.side = 8 // self.per
        self.middle = (self.count - 16) // self.per
        self.vectors = 2 * self.side + self.middle + 1
        self.packs = 1 + (self.count > 16)
        self.far_packs = block[0] // 16
        assert block[0] % 16 == 0 and self.block1[1] % 8 == 0 and self.block2[2] <= LANES
        assert self.next.lanes == LANES and (self.count - 16) % self.per == 0 and 64 % self.block1[2] == 0
        self.levels = []
        size = tuple(block[which] * counts[which] // 4 for which in range(3))
        number = 2
        while size[0] * size[1] * size[2] > DENSE:
            self.levels.append(Grid(size, (0, 0, 0), edge=True))
            assert self.levels[-1].lanes == LANES
            size = tuple(part // 2 for part in size)
            number += 1
        self.dense, self.dense_level = size, number

    def message(self, steps):
        dx, dy, dz = steps
        if dz == 0:
            begin, length = {0: (0, self.vectors), -1: (0, self.side + 1), 1: (self.side, self.side + 1)}[dx]
            if dy == 0:
                return ("part_t", (pl.ds(begin, length),), (length, self.high, LANES))
            return ("part_y", ((dy + 1) // 2, pl.ds(begin, length)), (length, 8, LANES))
        length = self.packs if dx == 0 else 1
        if dy == 0:
            return ("part_z", ((dz + 1) // 2, pl.ds(0, length)), (length, self.high, LANES))
        return (
            "part_zy", ((dz + 1) // 2, (dy + 1) // 2, pl.ds(0, length)), (length, 8, LANES),
        )

    def scratch(self):
        block = self.block
        s = {}
        for name, grid in (("top", self.top), ("wide", self.wide), ("next", self.next)):
            s.update(grid.scratch(name))
        for number, grid in enumerate(self.levels):
            s.update(grid.scratch(f"level{number}"))
        s["own"] = pltpu.VMEM((block[0], block[1], self.width), F32)
        if block[2] != self.width:
            s["raw"] = pltpu.VMEM(block, F32)
        s["field"] = pltpu.VMEM((block[0] + 16, block[1] + 16, self.wide.lanes), F32)
        for tile in range(self.tiles):
            s[f"rows{tile}"] = pltpu.VMEM((self.count, block[1] + 16, LANES), F32)
        s["part"] = pltpu.VMEM((self.count, self.high, LANES), F32)
        s["part_t"] = pltpu.VMEM((self.vectors, self.high, LANES), F32)
        s["part_y"] = pltpu.VMEM((2, self.vectors, 8, LANES), F32)
        s["part_z"] = pltpu.VMEM((2, self.packs, self.high, LANES), F32)
        s["part_zy"] = pltpu.VMEM((2, 2, self.packs, 8, LANES), F32)
        for number, steps in enumerate(DIRECTIONS):
            s[f"land{number}"] = pltpu.VMEM(self.message(steps)[2], F32)
        wide_rows = self.block1[1] + 16
        for dx in (-1, 0, 1):
            length = self.vectors if dx == 0 else self.side + 1
            packs = self.packs if dx == 0 else 1
            s[f"sum{dx}"] = pltpu.VMEM((length, wide_rows, LANES), F32)
            s[f"sumz{dx}"] = pltpu.VMEM((2, packs, wide_rows, LANES), F32)
        s["far"] = pltpu.VMEM((2, self.far_packs, block[1], LANES), F32)
        s["far_land"] = pltpu.VMEM((2, self.far_packs + 2, block[1] + 16, LANES), F32)
        s.update(Exchange.scratch(self.next, "swap"))
        first = self.levels[0]
        coarse = [first] + self.levels[1:]
        s["pairs"] = pltpu.VMEM((max(g.block[0] for g in coarse + [self.next]), 2 * up_to(first.rows, 16), LANES), F32)
        s["solved"] = pltpu.VMEM((first.block[0] + 6, first.rows, LANES), F32)
        s["spread"] = pltpu.VMEM((self.next.count, 2 * first.rows + 32, LANES), F32)
        s["whole"] = pltpu.VMEM((first.block[0], first.rows, LANES), F32)
        s["mine"] = pltpu.VMEM((8, LANES), F32)
        s["slots"] = pltpu.VMEM((self.total, 8, LANES), F32)
        size = self.dense[0] * self.dense[1] * self.dense[2]
        s["matrix"] = pltpu.VMEM((3, size, size), BF16)
        for name, number in (
            ("sent", self.total), ("got", self.total), ("part_sent", 26), ("part_got", 26),
            ("far_sent", 26), ("far_got", 26), ("loads", 3),
        ):
            s["sem_" + name] = pltpu.SemaphoreType.DMA((number,))
        return s


def weights(shape, found, value):
    return jnp.where(found, value, 0.0).astype(F32).reshape(shape)


def pair_sums(s, height, count):
    even = s[0:count, pl.ds(0, height // 2, stride=2), :]
    return even + s[0:count, pl.ds(1, height // 2, stride=2), :]


def send_part(plan, s, place, number):
    steps = DIRECTIONS[number]
    name, index, _ = plan.message(steps)
    return pltpu.make_async_remote_copy(
        src_ref=s[name].at[index],
        dst_ref=s[f"land{number}"],
        send_sem=s["sem_part_sent"].at[number],
        recv_sem=s["sem_part_got"].at[number],
        device_id=device(place, steps),
        device_id_type=MESH,
    )


def send_far(plan, s, place, number):
    dx, dy, dz = steps = DIRECTIONS[number]
    block = plan.block
    rows = {0: (0, block[1], 0), 1: (block[1] - 8, 8, block[1] + 8), -1: (0, 8, block[1])}[dy]
    if dz == 0:
        planes = {0: (0, block[0], 8), 1: (block[0] - 8, 8, 0), -1: (0, 8, block[0] + 8)}[dx]
        source = s["own"].at[pl.ds(planes[0], planes[1]), pl.ds(rows[0], rows[1]), :]
        target = s["field"].at[pl.ds(planes[2], planes[1]), pl.ds(rows[2], rows[1]), pl.ds(0, plan.width)]
    else:
        side, last = (dz + 1) // 2, plan.far_packs - 1
        packs = {0: (0, last + 1, 1), 1: (last, 1, 0), -1: (0, 1, last + 2)}[dx]
        source = s["far"].at[side, pl.ds(packs[0], packs[1]), pl.ds(rows[0], rows[1]), :]
        target = s["far_land"].at[side, pl.ds(packs[2], packs[1]), pl.ds(rows[2], rows[1]), :]
    return pltpu.make_async_remote_copy(
        src_ref=source,
        dst_ref=target,
        send_sem=s["sem_far_sent"].at[number],
        recv_sem=s["sem_far_got"].at[number],
        device_id=device(place, steps),
        device_id_type=MESH,
    )


def each(place, counts, send, action, reverse=False):
    for number, steps in enumerate(DIRECTIONS):
        @pl.when(exists(place, back(steps) if reverse else steps, counts))
        def _():
            getattr(send(number), action)()


def pack_part(plan, s):
    count, per, side, middle, rows = plan.count, plan.per, plan.side, plan.middle, plan.block1[1]
    length = plan.block1[2]
    part = s["part"]
    shape = (plan.high, LANES)
    lane = iota(shape, 1)
    sub = iota((8, LANES), 0)

    def pair_y(value):
        edge = value[rows:]
        minus = jnp.where(sub >= 6, edge, value[:8])
        return minus, jnp.where(sub < 2, edge, value[rows - 8 : rows])

    groups = [(0, 0, side), (side + 1, count - 8, side), (2 * side + 1, 8, middle)]
    for index, first, number in groups:
        for spot in range(number):
            value = part[first + spot]
            for which in range(1, per):
                moved = pltpu.roll(part[first + spot + which * number], which * length, 1)
                value = jnp.where(lane // length == which, moved, value)
            s["part_t"][index + spot] = value
            minus, plus = pair_y(value)
            s["part_y"][0, index + spot] = minus
            s["part_y"][1, index + spot] = plus
    value = jnp.zeros(shape, F32)
    couple = lane // 2
    for number in range(count):
        low = pltpu.roll(part[number], 2 * number, 1)
        high = low if length == 64 else pltpu.roll(part[number], 64 - length + 2 * number, 1)
        value = jnp.where(couple == ((126 + 2 * number) % LANES) // 2, low, value)
        value = jnp.where(couple == 32 + number, high, value)
    s["part_t"][side] = value
    minus, plus = pair_y(value)
    s["part_y"][0, side] = minus
    s["part_y"][1, side] = plus
    for which in range(2):
        begin = LANES - 2 if which == 0 else length - 6
        for pack in range(plan.packs):
            value = jnp.zeros(shape, F32)
            planes = list(range(8)) + list(range(count - 8, count)) if pack == 0 else list(range(8, count - 8))
            for slot, number in enumerate(planes):
                moved = pltpu.roll(part[number], (8 * slot - begin) % LANES, 1)
                value = jnp.where(lane // 8 == slot, moved, value)
            s["part_z"][which, pack] = value
            minus, plus = pair_y(value)
            s["part_zy"][which, 0, pack] = minus
            s["part_zy"][which, 1, pack] = plus


def gather_part(plan, s):
    side, count, rows, per, length = plan.side, plan.count, plan.block1[1], plan.per, plan.block1[2]
    sub = iota((8, LANES), 0)
    land = {steps: s[f"land{number}"] for number, steps in enumerate(DIRECTIONS)}

    def assembled(own, plus, minus):
        edge = own[rows:]
        tiles = [own[8 * number : 8 * number + 8] for number in range(rows // 8)]
        tiles[0] = tiles[0] + jnp.where(sub < 2, minus, 0.0)
        tiles[-1] = tiles[-1] + jnp.where(sub >= 6, plus, 0.0)
        tiles.append(jnp.where(sub < 6, plus, 0.0) + jnp.where(sub < 2, edge, 0.0))
        tiles.append(jnp.where(sub >= 2, minus, 0.0) + jnp.where(sub >= 6, edge, 0.0))
        return jnp.concatenate(tiles, axis=0)

    for dx in (-1, 0, 1):
        own = s["part_t"] if dx == 0 else land[(dx, 0, 0)]
        for index in range(own.shape[0]):
            s[f"sum{dx}"][index] = assembled(own[index], land[(dx, -1, 0)][index], land[(dx, 1, 0)][index])
        for which in range(2):
            dz = 2 * which - 1
            for pack in range(land[(dx, 0, dz)].shape[0]):
                s[f"sumz{dx}"][which, pack] = assembled(
                    land[(dx, 0, dz)][pack], land[(dx, -1, dz)][pack], land[(dx, 1, dz)][pack]
                )

    shape = (rows + 16, LANES)
    lane = iota(shape, 1)
    at_low, at_high = lane >= LANES - 2, (lane == length) | (lane == length + 1)
    inner = lane < length
    above = (lane >= length - 2) & (lane < length + 6)
    below = (lane >= LANES - 6) | (lane < 2)
    even = parity_of(*shape)

    def turned(value, shift):
        shift = shift % LANES
        return pltpu.roll(value, shift, 1) if shift else value

    def plane_of(dx, number):
        if number < 8:
            index, slots, size, first = number, number, side, 0
            base = 0
        elif number >= count - 8:
            index, slots, size, first = number - (count - 8), 8 + number - (count - 8), side, count - 8
            base = side + 1
        else:
            index, slots, size, first = number - 8, number - 8, plan.middle, 8
            base = 2 * side + 1
        pack = 0 if number < 8 or number >= count - 8 else 1
        extra = side
        if dx == -1:
            base, extra = 0, side
        if dx == 1:
            base, extra = 1, 0
        total = s[f"sum{dx}"]
        main = turned(total[base + index % size], -(index // size) * length)
        low = turned(total[extra], -2 * number)
        high = low if length == 64 else turned(total[extra], length - 64 - 2 * number)
        value = jnp.where(inner, main, jnp.where(at_low, low, jnp.where(at_high, high, 0.0)))
        far = s[f"sumz{dx}"]
        from_above = turned(far[0, pack], length - 2 - 8 * slots)
        from_below = turned(far[1, pack], LANES - 6 - 8 * slots)
        return value + (jnp.where(above, from_above, 0.0) + jnp.where(below, from_below, 0.0))

    def plane(number):
        spot = number - 2 * plan.next.margins[0]
        total = None
        for dx, place in ((0, spot), (-1, spot - plan.block1[0]), (1, spot + plan.block1[0])):
            index = place + 2
            allowed = {0: (0, count), -1: (0, 8), 1: (count - 8, count)}[dx]
            if allowed[0] <= index < allowed[1]:
                value = plane_of(dx, index)
                total = value if total is None else total + value
        return total

    for number in range(plan.next.count):
        first, second = plane(2 * number), plane(2 * number + 1)
        s["nextf"][number] = jnp.where(even, first, second)
        s["nextg"][number] = jnp.where(even, second, first)


def solve(plan, s, number):
    grid, name = plan.levels[number], f"level{number}"
    even = parity_of(grid.rows, LANES)
    count = grid.count
    grid.first(s, name, 0, count)
    for colour in (1, 0, 1):
        grid.half(s, name, colour, even, 0, count)
    pairs = s["pairs"]
    height = max(grid.rows, 16)
    if grid.rows < height:
        pairs[0:count, grid.rows : height] = jnp.zeros((count, height - grid.rows, LANES), F32)
    for spot, value in grid.residue(s, name, even, 0, count):
        if grid.rows > grid.block[1]:
            value = jnp.where(iota(value.shape, 0) < grid.block[1], value, 0.0)
        pairs[spot, 0 : grid.rows] = value
    flat = pair_sums(pairs, height, count).reshape(count * (height // 2), LANES)
    row, column = iota((LANES, LANES), 0), iota((LANES, LANES), 1)
    if number + 1 < len(plan.levels):
        below, under = plan.levels[number + 1], f"level{number + 1}"
        down = weights((LANES, LANES), (row // 2 == column) & (row < grid.block[2]), 0.5)
        coarse = dot(flat, down).reshape(count, height // 2, LANES)[:, : below.rows]
        same = parity_of(below.rows, LANES)
        for spot in range(below.count):
            one, two = coarse[2 * spot], coarse[2 * spot + 1]
            s[under + "f"][spot] = jnp.where(same, one, two)
            s[under + "g"][spot] = jnp.where(same, two, one)
        solve(plan, s, number + 1)
        planes = [below.planes(s, under, same, plane) for plane in range(count)]
        spread = weights((LANES, LANES), column // 2 == row, 1.0)
        flat = dot(jnp.concatenate(planes, axis=0), spread).reshape(count, below.rows, LANES)
        pairs[0:count, pl.ds(0, below.rows, stride=2), :] = flat
        pairs[0:count, pl.ds(1, below.rows, stride=2), :] = flat
        for spot in range(count):
            s[name + "B"][spot + 1] = s[name + "B"][spot + 1] + pairs[spot, 0 : grid.rows]
    else:
        nx, ny, nz = plan.dense
        size = nx * ny * nz
        tall = height // 2
        down = weights((LANES, LANES), (row // 2 == column % nz) & (row < grid.block[2]), 0.5)
        many = dot(flat, down).reshape(count, tall, LANES)
        wide = up_to(size, LANES) // LANES
        here, lane = iota((tall, LANES), 0), iota((tall, LANES), 1)
        parts = []
        for vector in range(wide):
            cell = (vector * LANES + lane) // nz
            total = jnp.zeros((tall, LANES), F32)
            for spot in range(nx):
                total = total + jnp.where((cell == spot * ny + here) & (here < ny), many[spot], 0.0)
            parts.append(total)
        left = jnp.concatenate(parts, axis=1)[:, :size]
        high, middle, low = pieces(left)
        stack = jnp.concatenate([high, middle, low], axis=0)
        matrix = s["matrix"]
        one = product(stack, matrix[0])
        two = product(stack[: 2 * tall], matrix[1])
        three = product(high, matrix[2])
        total = one[:tall] + ((one[tall : 2 * tall] + one[2 * tall :]) + ((two[:tall] + two[tall:]) + three))
        answer = jnp.sum(total, axis=0, keepdims=True)
        here, lane = iota((grid.rows, LANES), 0), iota((grid.rows, LANES), 1)
        planes = []
        for spot in range(nx):
            value = jnp.zeros((grid.rows, LANES), F32)
            for vector in range(wide):
                if (vector + 1) * LANES <= spot * ny * nz or vector * LANES >= (spot + 1) * ny * nz:
                    continue
                piece = jnp.broadcast_to(answer[:, vector * LANES : (vector + 1) * LANES], value.shape)
                cell = (vector * LANES + lane) // nz
                value = jnp.where(cell == spot * ny + here // 2, piece, value)
            planes.append(value)
        spread = weights((LANES, LANES), (column // 2 == row % nz) & (column < grid.block[2]), 1.0)
        flat = dot(jnp.concatenate(planes, axis=0), spread).reshape(count, grid.rows, LANES)
        for spot in range(count):
            s[name + "B"][spot + 1] = s[name + "B"][spot + 1] + flat[spot]
    for colour in (0, 1, 0, 1):
        grid.half(s, name, colour, even, 0, count)


def kernel(plan, names, density, dense, potential, *refs):
    s = dict(zip(names, refs))
    counts, block, total = plan.counts, plan.block, plan.total
    top, wide, next_ = plan.top, plan.wide, plan.next
    place = tuple(lax.axis_index(axis) for axis in AXES)
    me = (place[0] * counts[1] + place[1]) * counts[2] + place[2]
    padded = block[2] != plan.width

    loads = [pltpu.make_async_copy(density, s["raw" if padded else "own"], s["sem_loads"].at[0])]
    loads[0].start()
    if not padded:
        loads.append(
            pltpu.make_async_copy(
                density,
                s["field"].at[pl.ds(8, block[0]), pl.ds(0, block[1]), pl.ds(0, block[2])],
                s["sem_loads"].at[1],
            )
        )
        loads[1].start()
    fill = pltpu.make_async_copy(dense, s["matrix"], s["sem_loads"].at[2])
    fill.start()

    for number in range(26):
        ref = s[f"land{number}"]
        ref[...] = jnp.zeros(ref.shape, F32)

    def peer(number):
        other = lax.rem(me + number, total)
        inner = counts[1] * counts[2]
        return (lax.div(other, inner), lax.rem(lax.div(other, counts[2]), counts[1]), lax.rem(other, counts[2])), other

    barrier = pltpu.get_barrier_semaphore()

    def greet(number, carry):
        pl.semaphore_signal(barrier, inc=1, device_id=peer(number)[0], device_id_type=MESH)
        return carry

    lax.fori_loop(1, total, greet, 0)

    for name in ("topf", "topg", "topR", "topB"):
        s[name][...] = jnp.zeros(s[name].shape, F32)
    for name, grid in (("top", top), ("wide", wide), ("next", next_)):
        grid.guard(s, name)
        grid.masks(s, name, place, counts)
    for number, grid in enumerate(plan.levels):
        grid.guard(s, f"level{number}")
        grid.masks(s, f"level{number}", (0, 0, 0), (1, 1, 1))
    loads[0].wait()
    own = s["own"]
    if padded:
        own[...] = jnp.zeros(own.shape, F32)
        own[:, :, 0 : block[2]] = s["raw"][...]

    even_own = parity_of(block[1], plan.width)
    for number in range(top.inner):
        one, two = own[2 * number], own[2 * number + 1]
        red = jnp.where(even_own, one, two)
        spot = number + top.margins[0]
        s["topf"][spot, 0 : block[1], 0 : plan.width] = red
        s["topg"][spot, 0 : block[1], 0 : plan.width] = jnp.where(even_own, two, one)
        s["topR"][spot + 1, 0 : block[1], 0 : plan.width] = red * inverse
    even_top = parity_of(top.rows, top.lanes)
    count = top.count
    top.half(s, "top", 1, even_top, 1, count - 1)
    top.half(s, "top", 0, even_top, 1, count - 1)
    top.half(s, "top", 1, even_top, 0, count)
    for number, value in top.residue(s, "top", even_top, 0, count):
        for tile in range(plan.tiles):
            piece = value[:, tile * LANES : (tile + 1) * LANES]
            s[f"rows{tile}"][number, 0 : top.rows] = piece
            s[f"rows{tile}"][number, top.rows : top.rows + 8] = piece[block[1] :]
    flat = jnp.concatenate(
        [
            pair_sums(s[f"rows{tile}"], block[1] + 16, count).reshape(count * plan.high, LANES)
            for tile in range(plan.tiles)
        ],
        axis=1,
    )

    def fine_cell(shape, dim):
        index = iota(shape, dim)
        used = (index < block[2] + 4) | (index >= top.lanes - 4)
        cell = half_down(local_of(index, block[2], 4, top.lanes))
        return jnp.where(cell < 0, cell + LANES, cell), used

    shape = (top.lanes, LANES)
    cell, used = fine_cell(shape, 0)
    down = weights(shape, (cell == iota(shape, 1)) & used, 0.5)
    s["part"][...] = dot(flat, down).reshape(count, plan.high, LANES)
    pack_part(plan, s)

    pl.semaphore_wait(barrier, total - 1)
    part = functools.partial(send_part, plan, s, place)
    far = functools.partial(send_far, plan, s, place)
    each(place, counts, part, "start")

    lane = iota((block[1], LANES), 1)
    for side in range(2):
        begin = 0 if side == 0 else block[2] - 8
        tile = begin // LANES
        for pack in range(plan.far_packs):
            value = jnp.zeros((block[1], LANES), F32)
            for slot in range(16):
                plane = own[16 * pack + slot, :, tile * LANES : (tile + 1) * LANES]
                moved = pltpu.roll(plane, (8 * slot - begin) % LANES, 1)
                value = jnp.where(lane // 8 == slot, moved, value)
            s["far"][side, pack] = value
    each(place, counts, far, "start")
    field, far_land = s["field"], s["far_land"]
    if padded:
        field[8 : 8 + block[0], 0 : block[1], 0 : plan.width] = own[...]
    for dim, step in ((0, -1), (0, 1), (1, -1), (1, 1), (2, -1), (2, 1)):
        steps = tuple(step if which == dim else 0 for which in range(3))

        @pl.when(jnp.logical_not(exists(place, steps, counts)))
        def _():
            if dim == 0:
                begin = 0 if step < 0 else 8 + block[0]
                field[begin : begin + 8] = jnp.zeros((8,) + field.shape[1:], F32)
                pack = 0 if step < 0 else plan.far_packs + 1
                far_land[:, pack] = jnp.zeros((2,) + far_land.shape[2:], F32)
            if dim == 1:
                begin = block[1] if step > 0 else block[1] + 8
                field[:, begin : begin + 8] = jnp.zeros((field.shape[0], 8, field.shape[2]), F32)
                far_land[:, :, begin : begin + 8] = jnp.zeros(far_land.shape[:2] + (8, LANES), F32)
            if dim == 2:
                far_land[(1 - step) // 2] = jnp.zeros(far_land.shape[1:], F32)

    each(place, counts, part, "wait_recv", reverse=True)
    gather_part(plan, s)
    even_next = parity_of(next_.rows, LANES)
    n = next_.count
    next_.first(s, "next", 0, n)
    next_.half(s, "next", 1, even_next, 1, n - 1)
    next_.half(s, "next", 0, even_next, 2, n - 2)
    next_.half(s, "next", 1, even_next, 2, n - 2)
    pairs = s["pairs"]
    rows1 = plan.block1[1]
    height = max(rows1, 16)
    if rows1 < height:
        pairs[0 : next_.inner, rows1:height] = jnp.zeros((next_.inner, height - rows1, LANES), F32)
    for number, value in next_.residue(s, "next", even_next, 3, n - 3):
        pairs[number - 3, 0:rows1] = value[0:rows1]
    flat = pair_sums(pairs, height, next_.inner).reshape(next_.inner * (height // 2), LANES)
    row, column = iota((LANES, LANES), 0), iota((LANES, LANES), 1)
    down = weights((LANES, LANES), (row // 2 == column) & (row < plan.block1[2]), 0.5)
    below = dot(flat, down).reshape(next_.inner, height // 2, LANES)
    length = plan.block2
    per = LANES // length[2]
    packed = jnp.zeros((8, LANES), F32)
    for plane in range(length[0]):
        moved = below[plane]
        if plane // per:
            moved = pltpu.roll(moved, length[1] * (plane // per), 0)
        if plane % per:
            moved = pltpu.roll(moved, length[2] * (plane % per), 1)
        packed = packed + moved
    s["mine"][...] = packed
    slots = s["slots"]
    slots[me] = packed

    def send(number, slot):
        target, other = peer(number)
        return pltpu.make_async_remote_copy(
            src_ref=s["mine"],
            dst_ref=slots.at[me if slot is None else other],
            send_sem=s["sem_sent"].at[other],
            recv_sem=s["sem_got"].at[me if slot is None else other],
            device_id=target,
            device_id_type=MESH,
        )

    def start_send(number, carry):
        send(number, None).start()
        return carry

    lax.fori_loop(1, total, start_send, 0)
    swap = Exchange(next_, place, counts, s["nextB"], [s[f"swap{number}"] for number in range(8)])
    swap.start_xy()

    each(place, counts, far, "wait_recv", reverse=True)
    if not padded:
        loads[1].wait()
    base = wide.lanes - LANES
    shape = (wide.rows, LANES)
    lane = iota(shape, 1)
    even_wide = parity_of(wide.rows, wide.lanes)
    above = block[2] - base

    def wide_plane(number):
        pack, slot = (number + 8) // 16, (number + 8) % 16
        high = pltpu.roll(far_land[0, pack], (above - 8 * slot) % LANES, 1)
        low = pltpu.roll(far_land[1, pack], (LANES - 8 - 8 * slot) % LANES, 1)
        old = field[number, :, 0:LANES] if base == 0 else 0.0
        value = jnp.where((lane >= above) & (lane < above + 8), high, old)
        value = jnp.where(lane >= LANES - 8, low, value)
        return value if base == 0 else jnp.concatenate([field[number, :, 0:base], value], axis=1)

    for number in range(wide.count):
        one, two = wide_plane(2 * number), wide_plane(2 * number + 1)
        s["widef"][number] = jnp.where(even_wide, one, two)
        s["wideg"][number] = jnp.where(even_wide, two, one)
    n = wide.count
    wide.first(s, "wide", 0, n)
    wide.half(s, "wide", 1, even_wide, 1, n - 1)
    wide.half(s, "wide", 0, even_wide, 1, n - 1)
    wide.half(s, "wide", 1, even_wide, 2, n - 2)
    wider = iota((8, wide.lanes), 0) < 4

    def narrow(value):
        both = jnp.where(wider, value[block[1] : block[1] + 8], value[block[1] + 8 :])
        value = jnp.concatenate([value[: block[1]], both], axis=0)
        if top.lanes != wide.lanes:
            value = jnp.concatenate([value[:, : top.lanes - LANES], value[:, -LANES:]], axis=1)
        return value

    shift = wide.margins[0] - top.margins[0]
    for number in range(count):
        s["topf"][number] = narrow(s["widef"][number + shift])
        s["topg"][number] = narrow(s["wideg"][number + shift])
        s["topB"][number + 1] = narrow(s["wideB"][number + shift + 1])

    swap.finish_xy()
    swap.start_z()

    def finish_send(number, carry):
        copy = send(number, 0)
        copy.wait_recv()
        copy.wait_send()
        return carry

    lax.fori_loop(1, total, finish_send, 0)
    lane = iota((8, LANES), 1)
    whole = s["whole"]
    first = plan.levels[0]

    def place_x(which, carry):
        for second in range(counts[1]):
            start = (which * counts[1] + second) * counts[2]
            tiles = [slots[start + third] for third in range(counts[2])]
            for spot in range(per):
                value = jnp.zeros((8, LANES), F32)
                for third in range(counts[2]):
                    turn = (length[2] * (third - spot)) % LANES
                    moved = pltpu.roll(tiles[third], turn, 1) if turn else tiles[third]
                    value = jnp.where(lane // length[2] == third, moved, value)
                for group in range(8 // length[1]):
                    plane = which * length[0] + group * per + spot
                    whole[plane, second * length[1] : (second + 1) * length[1], :] = value[
                        group * length[1] : (group + 1) * length[1]
                    ]
        return carry

    lax.fori_loop(0, counts[0], place_x, 0)
    even_first = parity_of(first.rows, LANES)
    for number in range(first.count):
        one, two = whole[2 * number], whole[2 * number + 1]
        s["level0f"][number] = jnp.where(even_first, one, two)
        s["level0g"][number] = jnp.where(even_first, two, one)
    fill.wait()
    solve(plan, s, 0)
    solved = s["solved"]
    for number in range(3):
        solved[number] = jnp.zeros((first.rows, LANES), F32)
        solved[first.block[0] + 3 + number] = jnp.zeros((first.rows, LANES), F32)
    for plane in range(first.block[0]):
        solved[plane + 3] = first.planes(s, "level0", even_first, plane)

    swap.finish_z()
    shape = (LANES, LANES)
    index = iota(shape, 1)
    spot = local_of(index, plan.block1[2], 8, LANES)
    used = (index < plan.block1[2] + 8) | (index >= LANES - 8)
    lanes_to = weights(shape, (half_down(spot) + place[2] * length[2] == iota(shape, 0)) & used, 1.0)
    n = next_.count
    flat = jnp.concatenate([solved[place[0] * length[0] + number] for number in range(n)], axis=0)
    flat = dot(flat, lanes_to).reshape(n, first.rows, LANES)
    spread = s["spread"]
    spread[:, 0:16] = jnp.zeros((n, 16, LANES), F32)
    spread[:, 16 + 2 * first.rows :] = jnp.zeros((n, 16, LANES), F32)
    spread[0:n, pl.ds(16, first.rows, stride=2), :] = flat
    spread[0:n, pl.ds(17, first.rows, stride=2), :] = flat
    start = 16 + place[1] * rows1
    for number in range(n):
        tiles = [
            spread[number, pl.ds(pl.multiple_of(start + shift, 8), size), :]
            for shift, size in ((0, rows1), (rows1, 8), (-8, 8))
        ]
        s["nextB"][number + 1] = s["nextB"][number + 1] + jnp.concatenate(tiles, axis=0)
    for colour, skip in ((0, 0), (1, 1), (0, 1), (1, 2)):
        next_.half(s, "next", colour, even_next, skip, n - skip)

    pick = iota((8, LANES), 0) < 4
    planes = []
    for number in range(count):
        value = next_.planes(s, "next", even_next, number + 2 * next_.margins[0] - top.margins[0])
        edge = jnp.where(pick, value[rows1 : rows1 + 8], value[rows1 + 8 :])
        planes.append(jnp.concatenate([value[:rows1], edge], axis=0))
    shape = (LANES, top.lanes)
    cell, used = fine_cell(shape, 1)
    spreading = weights(shape, (cell == iota(shape, 0)) & used, 1.0)
    flat = dot(jnp.concatenate(planes, axis=0), spreading).reshape(count, plan.high, top.lanes)
    for tile in range(plan.tiles):
        piece = flat[:, :, tile * LANES : (tile + 1) * LANES]
        s[f"rows{tile}"][0:count, pl.ds(0, plan.high, stride=2), :] = piece
        s[f"rows{tile}"][0:count, pl.ds(1, plan.high, stride=2), :] = piece
    for number in range(count):
        tiles = []
        for tile in range(plan.tiles):
            rows = s[f"rows{tile}"]
            edge = jnp.where(pick, rows[number, block[1] : block[1] + 8], rows[number, block[1] + 8 : block[1] + 16])
            tiles.append(jnp.concatenate([rows[number, 0 : block[1]], edge], axis=0))
        s["topB"][number + 1] = s["topB"][number + 1] + jnp.concatenate(tiles, axis=1)
    top.half(s, "top", 0, even_top, 0, count)
    top.half(s, "top", 1, even_top, 1, count - 1)
    top.half(s, "top", 0, even_top, 1, count - 1)
    red = s["topR"]
    even_out = parity_of(block[1], block[2])
    for number, value in top.totals(red, even_top, 1, top.margins[0], count - top.margins[0]):
        black = ((s["topg"][number] + value) * inverse)[0 : block[1], 0 : block[2]]
        old = red[number + 1][0 : block[1], 0 : block[2]]
        plane = 2 * (number - top.margins[0])
        potential[plane] = jnp.where(even_out, old, black)
        potential[plane + 1] = jnp.where(even_out, black, old)
    each(place, counts, part, "wait_send")
    each(place, counts, far, "wait_send")
    swap.drain()


def cycle_matrix(size, depth):
    def beside_sum(v):
        p = np.pad(v, ((0, 0), (1, 1), (1, 1), (1, 1)))
        total = p[:, 2:, 1:-1, 1:-1] + p[:, :-2, 1:-1, 1:-1] + p[:, 1:-1, 2:, 1:-1] + p[:, 1:-1, :-2, 1:-1]
        return total + along * (p[:, 1:-1, 1:-1, 2:] + p[:, 1:-1, 1:-1, :-2])

    def cycle(g, left):
        parity = np.indices(g.shape[1:]).sum(0) % 2

        def sweeps(v, number):
            for _ in range(number):
                for colour in (0, 1):
                    v = np.where(parity == colour, (g + beside_sum(v)) / centre, v)
            return v

        v = np.zeros_like(g)
        if left == 0:
            return sweeps(v, CSWEEPS)
        v = sweeps(v, 2)
        r = g - centre * v + beside_sum(v)
        x, y, z = (part // 2 for part in g.shape[1:])
        coarse = 4 * r.reshape(-1, x, 2, y, 2, z, 2).mean((2, 4, 6))
        e = cycle(coarse, left - 1)
        for dim in (1, 2, 3):
            e = np.repeat(e, 2, dim)
        return sweeps(v + e, 2)

    cells = size[0] * size[1] * size[2]
    found = cycle(np.eye(cells).reshape((cells,) + size), depth).reshape(cells, cells)
    parts = []
    for _ in range(3):
        parts.append(found.astype(np.float32).astype(jnp.bfloat16))
        found = found - parts[-1].astype(np.float64)
    return np.stack(parts)


def on_device(counts, density):
    plan = Plan(density.shape, counts)
    scratch = plan.scratch()
    matrix = jnp.asarray(cycle_matrix(plan.dense, LEVELS - 1 - plan.dense_level))
    return pl.pallas_call(
        functools.partial(kernel, plan, list(scratch)),
        out_shape=jax.ShapeDtypeStruct(density.shape, F32),
        in_specs=[pl.BlockSpec(memory_space=pltpu.HBM)] * 2,
        out_specs=pl.BlockSpec(memory_space=pltpu.VMEM),
        scratch_shapes=list(scratch.values()),
        compiler_params=pltpu.CompilerParams(
            collective_id=0, has_side_effects=True, vmem_limit_bytes=48 * 1024 * 1024
        ),
    )(density, matrix)


def solution(mesh):
    counts = tuple(mesh.shape[axis] for axis in AXES)
    return jax.shard_map(
        functools.partial(on_device, counts),
        mesh=mesh,
        in_specs=(P("gx", "gy", "gz"),),
        out_specs=P("gx", "gy", "gz"),
        check_vma=False,
    )
```

```python
import functools
import types

import jax
import jax.numpy as jnp
import numpy as np
from jax import lax
from jax.experimental import pallas as pl
from jax.experimental.pallas import tpu as pltpu
from jax.sharding import PartitionSpec as P

LEVELS = 7
CSWEEPS = 4
DENSE = 512
rsd_beta = 0.5
centre = 4.0 + 2.0 * (1.0 + rsd_beta)
along = 1.0 + rsd_beta
inverse = 1.0 / centre
F32 = jnp.float32
BF16 = jnp.bfloat16
LANES = 128
AXES = ("gx", "gy", "gz")
MESH = pl.DeviceIdType.MESH
DIRECTIONS = [
    (dx, dy, dz) for dx in (-1, 0, 1) for dy in (-1, 0, 1) for dz in (-1, 0, 1) if (dx, dy, dz) != (0, 0, 0)
]


ALL, PART, FAR, SWAP, OWN, FIELD, MATRIX = 0, 2, 4, 6, 8, 9, 10


def up_to(value, unit):
    return -(-value // unit) * unit


def iota(shape, dim):
    return lax.broadcasted_iota(jnp.int32, shape, dim)


def pieces(value):
    high = value.astype(BF16)
    rest = value - high.astype(F32)
    middle = rest.astype(BF16)
    return high, middle, (rest - middle.astype(F32)).astype(BF16)


def product(left, right):
    return jnp.dot(left, right, preferred_element_type=F32)


def dot(value, chosen):
    chosen = chosen.astype(BF16)
    parts = [product(part, chosen) for part in pieces(value)]
    return parts[0] + (parts[1] + parts[2])


def local_of(index, length, margin, total):
    return jnp.where(index < total - margin, index, index - total)


def half_down(value):
    return jnp.where(value >= 0, lax.div(value, 2), -lax.div(1 - value, 2))


def parity_of(rows, lanes):
    return (iota((rows, lanes), 0) + iota((rows, lanes), 1)) % 2 == 0


def beside(below, here, above, even, colour, edge):
    rows, lanes = here.shape
    down, up = pltpu.roll(here, 1, 0), pltpu.roll(here, rows - 1, 0)
    left, right = pltpu.roll(here, 1, 1), pltpu.roll(here, lanes - 1, 1)
    if edge is not None:
        if edge[0] == rows:
            row = iota(here.shape, 0)
            down = jnp.where(row == 0, 0.0, down)
            up = jnp.where(row == rows - 1, 0.0, up)
        if edge[1] == lanes:
            lane = iota(here.shape, 1)
            left = jnp.where(lane == 0, 0.0, left)
            right = jnp.where(lane == lanes - 1, 0.0, right)
    other = jnp.where(even, below, above) if colour == 0 else jnp.where(even, above, below)
    return (here + other) + (down + up) + along * (left + right)


class Grid:
    def __init__(self, block, margins, edge=False):
        self.block, self.margins = block, margins
        self.inner = block[0] // 2
        self.count = self.inner + 2 * margins[0]
        self.rows = up_to(block[1] + 2 * margins[1], 8)
        self.lanes = up_to(block[2] + 2 * margins[2], LANES)
        self.edge = (block[1], block[2]) if edge else None

    def scratch(self):
        field = (self.count + 2, self.rows, self.lanes)
        source = (self.count, self.rows, self.lanes)
        return dict(
            R=pltpu.VMEM(field, F32),
            B=pltpu.VMEM(field, F32),
            f=pltpu.VMEM(source, F32),
            g=pltpu.VMEM(source, F32),
            m=pltpu.VMEM((3, self.rows, self.lanes), F32),
        )

    def zone(self, number):
        if number < self.margins[0]:
            return 0
        return 2 if number >= self.count - self.margins[0] else 1

    def guard(self, v):
        empty = jnp.zeros((self.rows, self.lanes), F32)
        for ref in (v.R, v.B):
            ref[0] = empty
            ref[self.count + 1] = empty

    def masks(self, v, place, counts):
        inside = None
        shape = (self.rows, self.lanes)
        for dim in (1, 2):
            index = iota(shape, dim - 1)
            size = shape[dim - 1]
            margin, length = self.margins[dim], self.block[dim]
            used = (index < length + margin) | (index >= size - margin)
            spot = local_of(index, length, margin, size) + place[dim] * length
            used = used & (spot >= 0) & (spot < length * counts[dim])
            inside = used if inside is None else inside & used
        value = jnp.where(inside, inverse, 0.0).astype(F32)
        v.m[1] = value
        if self.margins[0]:
            low = jnp.where(place[0] > 0, 1.0, 0.0).astype(F32)
            high = jnp.where(place[0] < counts[0] - 1, 1.0, 0.0).astype(F32)
            v.m[0] = value * low
            v.m[2] = value * high

    def first(self, v, begin, end):
        for number in range(begin, end):
            v.R[number + 1] = v.f[number] * v.m[self.zone(number)]

    def totals(self, other, even, colour, begin, end):
        before, here = other[begin], other[begin + 1]
        for number in range(begin, end):
            after = other[number + 2]
            yield number, beside(before, here, after, even, colour, self.edge)
            before, here = here, after

    def half(self, v, colour, even, begin, end):
        target, other = (v.R, v.B) if colour == 0 else (v.B, v.R)
        source = v.f if colour == 0 else v.g
        for number, total in self.totals(other, even, colour, begin, end):
            target[number + 1] = (source[number] + total) * v.m[self.zone(number)]

    def residue(self, v, even, begin, end):
        for number, total in self.totals(v.B, even, 0, begin, end):
            yield number, v.f[number] - centre * v.R[number + 1] + total

    def planes(self, v, even, plane):
        red, black = v.R[plane // 2 + 1], v.B[plane // 2 + 1]
        return jnp.where(even, red, black) if plane % 2 == 0 else jnp.where(even, black, red)


def exists(place, steps, counts):
    found = None
    for which in range(3):
        if steps[which] == 0:
            continue
        other = place[which] + steps[which]
        here = (other >= 0) & (other < counts[which])
        found = here if found is None else found & here
    return found


def device(place, steps):
    return tuple(place[which] + steps[which] for which in range(3))


class Plan:
    def __init__(self, block, counts):
        self.counts, self.block = counts, block
        self.total = counts[0] * counts[1] * counts[2]
        self.block1 = tuple(size // 2 for size in block)
        self.block2 = tuple(size // 4 for size in block)
        self.top = Grid(block, (2, 4, 4))
        self.wide = Grid(block, (4, 8, 8))
        self.next = Grid(self.block1, (3, 8, 8))
        self.width = up_to(block[2], LANES)
        self.tiles = self.top.lanes // LANES
        self.count = self.top.count
        self.high = self.block1[1] + 8
        self.per = LANES // self.block1[2]
        self.side = 8 // self.per
        self.middle = (self.count - 16) // self.per
        self.vectors = 2 * self.side + self.middle + 1
        self.packs = 1 + (self.count > 16)
        self.far_packs = block[0] // 16
        assert block[0] % 16 == 0 and self.block1[1] % 8 == 0 and self.block2[2] <= LANES
        assert self.next.lanes == LANES and (self.count - 16) % self.per == 0 and 64 % self.block1[2] == 0
        self.levels = []
        size = tuple(block[which] * counts[which] // 4 for which in range(3))
        number = 2
        while size[0] * size[1] * size[2] > DENSE:
            self.levels.append(Grid(size, (0, 0, 0), edge=True))
            assert self.levels[-1].lanes == LANES
            size = tuple(part // 2 for part in size)
            number += 1
        self.dense, self.dense_level = size, number

    def message(self, steps):
        dx, dy, dz = steps
        if dz == 0:
            begin, length = {0: (0, self.vectors), -1: (0, self.side + 1), 1: (self.side, self.side + 1)}[dx]
            if dy == 0:
                return ("part_t", (pl.ds(begin, length),), (length, self.high, LANES))
            return ("part_y", ((dy + 1) // 2, pl.ds(begin, length)), (length, 8, LANES))
        length = self.packs if dx == 0 else 1
        if dy == 0:
            return ("part_z", ((dz + 1) // 2, pl.ds(0, length)), (length, self.high, LANES))
        return (
            "part_zy", ((dz + 1) // 2, (dy + 1) // 2, pl.ds(0, length)), (length, 8, LANES),
        )

    def scratch(self):
        block = self.block
        s = types.SimpleNamespace(
            top=self.top.scratch(), wide=self.wide.scratch(), next=self.next.scratch(),
            levels=[grid.scratch() for grid in self.levels],
        )
        s.own = pltpu.VMEM((block[0], block[1], self.width), F32)
        if block[2] != self.width:
            s.raw = pltpu.VMEM(block, F32)
        s.field = pltpu.VMEM((block[0] + 16, block[1] + 16, self.wide.lanes), F32)
        s.rows = [pltpu.VMEM((self.count, block[1] + 16, LANES), F32) for _ in range(self.tiles)]
        s.part = pltpu.VMEM((self.count, self.high, LANES), F32)
        s.part_t = pltpu.VMEM((self.vectors, self.high, LANES), F32)
        s.part_y = pltpu.VMEM((2, self.vectors, 8, LANES), F32)
        s.part_z = pltpu.VMEM((2, self.packs, self.high, LANES), F32)
        s.part_zy = pltpu.VMEM((2, 2, self.packs, 8, LANES), F32)
        s.land = [pltpu.VMEM(self.message(steps)[2], F32) for steps in DIRECTIONS]
        s.sums, s.sumz = [], []
        wide_rows = self.block1[1] + 16
        for dx in (-1, 0, 1):
            length = self.vectors if dx == 0 else self.side + 1
            packs = self.packs if dx == 0 else 1
            s.sums.append(pltpu.VMEM((length, wide_rows, LANES), F32))
            s.sumz.append(pltpu.VMEM((2, packs, wide_rows, LANES), F32))
        s.far = pltpu.VMEM((2, self.far_packs, block[1], LANES), F32)
        s.far_land = pltpu.VMEM((2, self.far_packs + 2, block[1] + 16, LANES), F32)
        s.swap = pltpu.VMEM((2, self.block1[1], LANES), F32)
        s.swap_land = pltpu.VMEM((self.next.count, self.next.rows, LANES), F32)
        s.swap_side = pltpu.VMEM((2, 3, self.next.rows, LANES), F32)
        first = self.levels[0]
        coarse = [first] + self.levels[1:]
        s.pairs = pltpu.VMEM((max(g.block[0] for g in coarse + [self.next]), 2 * up_to(first.rows, 16), LANES), F32)
        s.solved = pltpu.VMEM((first.block[0] + 6, first.rows, LANES), F32)
        s.spread = pltpu.VMEM((self.next.count, 2 * first.rows + 32, LANES), F32)
        s.whole = pltpu.VMEM((first.block[0], first.rows, LANES), F32)
        s.mine = pltpu.VMEM((8, LANES), F32)
        s.slots = pltpu.VMEM((self.total, 8, LANES), F32)
        size = self.dense[0] * self.dense[1] * self.dense[2]
        s.matrix = pltpu.VMEM((3, size, size), BF16)
        most = max(sum(size(self, steps) for steps in DIRECTIONS) for size in (size_part, size_far, size_swap))
        s.bytes = pltpu.VMEM((max(most, self.total), 8, LANES), F32)
        s.sem = pltpu.SemaphoreType.DMA((MATRIX + 1,))
        return vars(s)


def weights(shape, found, value):
    return jnp.where(found, value, 0.0).astype(F32).reshape(shape)


def pair_sums(s, height, count):
    even = s[0:count, pl.ds(0, height // 2, stride=2), :]
    return even + s[0:count, pl.ds(1, height // 2, stride=2), :]


def named(value):
    if isinstance(value, dict):
        return types.SimpleNamespace(**value)
    return [named(one) for one in value] if isinstance(value, list) else value


def sem(s, number):
    return s.sem.at[number]


def size_part(plan, steps):
    shape = plan.message(steps)[2]
    return shape[0] * shape[1] // 8


def size_far(plan, steps):
    rows = plan.block[1] // 8 if steps[1] == 0 else 1
    if steps[2]:
        return rows * (plan.far_packs if steps[0] == 0 else 1)
    return rows * (plan.block[0] if steps[0] == 0 else 8) * (plan.width // LANES)


def size_swap(plan, steps):
    rows = plan.block1[1] // 8 if steps[1] == 0 else 1
    return rows if steps[2] else rows * (plan.next.inner if steps[0] == 0 else plan.next.margins[0])


def wait_all(plan, s, place, size, name, other):
    counts = plan.counts
    beside_of = [
        jnp.where(place[axis] > 0, 1, 0) + jnp.where(place[axis] < counts[axis] - 1, 1, 0) for axis in range(3)
    ]
    choices = [{1: (0,), 2: (1,)}.get(count, (1, 2)) for count in counts]
    for x in choices[0]:
        for y in choices[1]:
            for z in choices[2]:
                number = 0
                for steps in DIRECTIONS:
                    many = [1 if step == 0 else (have if step > 0 else 0) for step, have in zip(steps, (x, y, z))]
                    if min(steps) >= 0:
                        number += many[0] * many[1] * many[2] * size(plan, steps)
                if number == 0:
                    continue
                found = (beside_of[0] == x) & (beside_of[1] == y) & (beside_of[2] == z)

                @pl.when(found)
                def _():
                    pltpu.make_async_remote_copy(
                        src_ref=s.bytes.at[pl.ds(0, number)],
                        dst_ref=s.bytes.at[pl.ds(0, number)],
                        send_sem=sem(s, name),
                        recv_sem=sem(s, name),
                        device_id=other,
                        device_id_type=MESH,
                    ).wait_recv()


def send_part(plan, s, place, number):
    steps = DIRECTIONS[number]
    name, index, _ = plan.message(steps)
    return pltpu.make_async_remote_copy(
        src_ref=getattr(s, name).at[index],
        dst_ref=s.land[number],
        send_sem=sem(s, PART),
        recv_sem=sem(s, PART + 1),
        device_id=device(place, steps),
        device_id_type=MESH,
    )


def send_far(plan, s, place, number):
    dx, dy, dz = steps = DIRECTIONS[number]
    block = plan.block
    rows = {0: (0, block[1], 0), 1: (block[1] - 8, 8, block[1] + 8), -1: (0, 8, block[1])}[dy]
    if dz == 0:
        planes = {0: (0, block[0], 8), 1: (block[0] - 8, 8, 0), -1: (0, 8, block[0] + 8)}[dx]
        source = s.own.at[pl.ds(planes[0], planes[1]), pl.ds(rows[0], rows[1]), :]
        target = s.field.at[pl.ds(planes[2], planes[1]), pl.ds(rows[2], rows[1]), pl.ds(0, plan.width)]
    else:
        side, last = (dz + 1) // 2, plan.far_packs - 1
        packs = {0: (0, last + 1, 1), 1: (last, 1, 0), -1: (0, 1, last + 2)}[dx]
        source = s.far.at[side, pl.ds(packs[0], packs[1]), pl.ds(rows[0], rows[1]), :]
        target = s.far_land.at[side, pl.ds(packs[2], packs[1]), pl.ds(rows[2], rows[1]), :]
    return pltpu.make_async_remote_copy(
        src_ref=source,
        dst_ref=target,
        send_sem=sem(s, FAR),
        recv_sem=sem(s, FAR + 1),
        device_id=device(place, steps),
        device_id_type=MESH,
    )


def send_swap(plan, s, place, number):
    dx, dy, dz = steps = DIRECTIONS[number]
    high, margin, inner = plan.block1[1], plan.next.margins[0], plan.next.inner
    rows = {0: (0, high, 0), 1: (high - 8, 8, high + 8), -1: (0, 8, high)}[dy]
    if dz == 0:
        planes = {0: (margin, inner, margin), 1: (inner, margin, 0), -1: (margin, margin, margin + inner)}[dx]
        source = s.next.B.at[pl.ds(1 + planes[0], planes[1]), pl.ds(rows[0], rows[1]), :]
        target = s.swap_land.at[pl.ds(planes[2], planes[1]), pl.ds(rows[2], rows[1]), :]
    else:
        side = (dz + 1) // 2
        source = s.swap.at[side, pl.ds(rows[0], rows[1]), :]
        target = s.swap_side.at[side, 1 - dx, pl.ds(rows[2], rows[1]), :]
    return pltpu.make_async_remote_copy(
        src_ref=source,
        dst_ref=target,
        send_sem=sem(s, SWAP),
        recv_sem=sem(s, SWAP + 1),
        device_id=device(place, steps),
        device_id_type=MESH,
    )


def pack_swap(plan, s):
    length, margin = plan.block1[2], plan.next.margins[0]
    lane = iota((plan.block1[1], LANES), 1)
    for side in range(2):
        begin = 0 if side == 0 else length - 8
        value = jnp.zeros(lane.shape, F32)
        for slot in range(plan.next.inner):
            plane = s.next.B[1 + margin + slot, 0 : plan.block1[1], :]
            value = jnp.where(lane // 8 == slot, pltpu.roll(plane, (8 * slot - begin) % LANES, 1), value)
        s.swap[side] = value


def swapped(plan, s, number):
    length, rows = plan.block1[2], plan.block1[1]
    margin, inner = plan.next.margins[0], plan.next.inner
    lane = iota((plan.next.rows, LANES), 1)
    which = 0 if number < margin else (2 if number >= margin + inner else 1)
    slot = number - margin + (1 - which) * inner
    value = s.swap_land[number]
    if which == 1:
        value = jnp.concatenate([s.next.B[number + 1, 0:rows, :], value[rows:]], axis=0)
    high = pltpu.roll(s.swap_side[0, which], (length - 8 * slot) % LANES, 1)
    low = pltpu.roll(s.swap_side[1, which], (LANES - 8 - 8 * slot) % LANES, 1)
    edge = jnp.where(lane < length + 8, high, jnp.where(lane >= LANES - 8, low, 0.0))
    return jnp.where(lane < length, value, edge)


def partners(place, count):
    if count & (count - 1):
        return [(lax.rem(place + off, count), lax.rem(place + count - off, count)) for off in range(count)]
    bits = [lax.rem(lax.div(place, 1 << bit), 2) for bit in range(count.bit_length() - 1)]
    out = []
    for off in range(count):
        value = jnp.int32(0)
        for bit, digit in enumerate(bits):
            value = value + ((1 - digit) if off >> bit & 1 else digit) * (1 << bit)
        out.append((value, value))
    return out


def each(place, counts, send):
    for number, steps in enumerate(DIRECTIONS):
        @pl.when(exists(place, steps, counts))
        def _():
            send(number).start()


def pack_part(plan, s):
    count, per, side, middle, rows = plan.count, plan.per, plan.side, plan.middle, plan.block1[1]
    length = plan.block1[2]
    part = s.part
    shape = (plan.high, LANES)
    lane = iota(shape, 1)
    sub = iota((8, LANES), 0)

    def pair_y(value):
        edge = value[rows:]
        minus = jnp.where(sub >= 6, edge, value[:8])
        return minus, jnp.where(sub < 2, edge, value[rows - 8 : rows])

    groups = [(0, 0, side), (side + 1, count - 8, side), (2 * side + 1, 8, middle)]
    for index, first, number in groups:
        for spot in range(number):
            value = part[first + spot]
            for which in range(1, per):
                moved = pltpu.roll(part[first + spot + which * number], which * length, 1)
                value = jnp.where(lane // length == which, moved, value)
            s.part_t[index + spot] = value
            minus, plus = pair_y(value)
            s.part_y[0, index + spot] = minus
            s.part_y[1, index + spot] = plus
    value = jnp.zeros(shape, F32)
    couple = lane // 2
    for number in range(count):
        low = pltpu.roll(part[number], 2 * number, 1)
        high = low if length == 64 else pltpu.roll(part[number], 64 - length + 2 * number, 1)
        value = jnp.where(couple == ((126 + 2 * number) % LANES) // 2, low, value)
        value = jnp.where(couple == 32 + number, high, value)
    s.part_t[side] = value
    minus, plus = pair_y(value)
    s.part_y[0, side] = minus
    s.part_y[1, side] = plus
    for which in range(2):
        begin = LANES - 2 if which == 0 else length - 6
        for pack in range(plan.packs):
            value = jnp.zeros(shape, F32)
            planes = list(range(8)) + list(range(count - 8, count)) if pack == 0 else list(range(8, count - 8))
            for slot, number in enumerate(planes):
                moved = pltpu.roll(part[number], (8 * slot - begin) % LANES, 1)
                value = jnp.where(lane // 8 == slot, moved, value)
            s.part_z[which, pack] = value
            minus, plus = pair_y(value)
            s.part_zy[which, 0, pack] = minus
            s.part_zy[which, 1, pack] = plus


def gather_part(plan, s):
    side, count, rows, per, length = plan.side, plan.count, plan.block1[1], plan.per, plan.block1[2]
    sub = iota((8, LANES), 0)
    land = {steps: s.land[number] for number, steps in enumerate(DIRECTIONS)}

    def assembled(own, plus, minus):
        edge = own[rows:]
        tiles = [own[8 * number : 8 * number + 8] for number in range(rows // 8)]
        tiles[0] = tiles[0] + jnp.where(sub < 2, minus, 0.0)
        tiles[-1] = tiles[-1] + jnp.where(sub >= 6, plus, 0.0)
        tiles.append(jnp.where(sub < 6, plus, 0.0) + jnp.where(sub < 2, edge, 0.0))
        tiles.append(jnp.where(sub >= 2, minus, 0.0) + jnp.where(sub >= 6, edge, 0.0))
        return jnp.concatenate(tiles, axis=0)

    for dx in (-1, 0, 1):
        own = s.part_t if dx == 0 else land[(dx, 0, 0)]
        for index in range(own.shape[0]):
            s.sums[dx + 1][index] = assembled(own[index], land[(dx, -1, 0)][index], land[(dx, 1, 0)][index])
        for which in range(2):
            dz = 2 * which - 1
            for pack in range(land[(dx, 0, dz)].shape[0]):
                s.sumz[dx + 1][which, pack] = assembled(
                    land[(dx, 0, dz)][pack], land[(dx, -1, dz)][pack], land[(dx, 1, dz)][pack]
                )

    shape = (rows + 16, LANES)
    lane = iota(shape, 1)
    at_low, at_high = lane >= LANES - 2, (lane == length) | (lane == length + 1)
    inner = lane < length
    above = (lane >= length - 2) & (lane < length + 6)
    below = (lane >= LANES - 6) | (lane < 2)
    even = parity_of(*shape)

    def turned(value, shift):
        shift = shift % LANES
        return pltpu.roll(value, shift, 1) if shift else value

    def plane_of(dx, number):
        if number < 8:
            index, slots, size, first = number, number, side, 0
            base = 0
        elif number >= count - 8:
            index, slots, size, first = number - (count - 8), 8 + number - (count - 8), side, count - 8
            base = side + 1
        else:
            index, slots, size, first = number - 8, number - 8, plan.middle, 8
            base = 2 * side + 1
        pack = 0 if number < 8 or number >= count - 8 else 1
        extra = side
        if dx == -1:
            base, extra = 0, side
        if dx == 1:
            base, extra = 1, 0
        total = s.sums[dx + 1]
        main = turned(total[base + index % size], -(index // size) * length)
        low = turned(total[extra], -2 * number)
        high = low if length == 64 else turned(total[extra], length - 64 - 2 * number)
        value = jnp.where(inner, main, jnp.where(at_low, low, jnp.where(at_high, high, 0.0)))
        far = s.sumz[dx + 1]
        from_above = turned(far[0, pack], length - 2 - 8 * slots)
        from_below = turned(far[1, pack], LANES - 6 - 8 * slots)
        return value + (jnp.where(above, from_above, 0.0) + jnp.where(below, from_below, 0.0))

    def plane(number):
        spot = number - 2 * plan.next.margins[0]
        total = None
        for dx, place in ((0, spot), (-1, spot - plan.block1[0]), (1, spot + plan.block1[0])):
            index = place + 2
            allowed = {0: (0, count), -1: (0, 8), 1: (count - 8, count)}[dx]
            if allowed[0] <= index < allowed[1]:
                value = plane_of(dx, index)
                total = value if total is None else total + value
        return total

    for number in range(plan.next.count):
        first, second = plane(2 * number), plane(2 * number + 1)
        s.next.f[number] = jnp.where(even, first, second)
        s.next.g[number] = jnp.where(even, second, first)


def solve(plan, s, number):
    grid, v = plan.levels[number], s.levels[number]
    even = parity_of(grid.rows, LANES)
    count = grid.count
    grid.first(v, 0, count)
    for colour in (1, 0, 1):
        grid.half(v, colour, even, 0, count)
    pairs = s.pairs
    height = max(grid.rows, 16)
    if grid.rows < height:
        pairs[0:count, grid.rows : height] = jnp.zeros((count, height - grid.rows, LANES), F32)
    for spot, value in grid.residue(v, even, 0, count):
        if grid.rows > grid.block[1]:
            value = jnp.where(iota(value.shape, 0) < grid.block[1], value, 0.0)
        pairs[spot, 0 : grid.rows] = value
    flat = pair_sums(pairs, height, count).reshape(count * (height // 2), LANES)
    row, column = iota((LANES, LANES), 0), iota((LANES, LANES), 1)
    if number + 1 < len(plan.levels):
        below, under = plan.levels[number + 1], s.levels[number + 1]
        down = weights((LANES, LANES), (row // 2 == column) & (row < grid.block[2]), 0.5)
        coarse = dot(flat, down).reshape(count, height // 2, LANES)[:, : below.rows]
        same = parity_of(below.rows, LANES)
        for spot in range(below.count):
            one, two = coarse[2 * spot], coarse[2 * spot + 1]
            under.f[spot] = jnp.where(same, one, two)
            under.g[spot] = jnp.where(same, two, one)
        solve(plan, s, number + 1)
        planes = [below.planes(under, same, plane) for plane in range(count)]
        spread = weights((LANES, LANES), column // 2 == row, 1.0)
        flat = dot(jnp.concatenate(planes, axis=0), spread).reshape(count, below.rows, LANES)
        pairs[0:count, pl.ds(0, below.rows, stride=2), :] = flat
        pairs[0:count, pl.ds(1, below.rows, stride=2), :] = flat
        for spot in range(count):
            v.B[spot + 1] = v.B[spot + 1] + pairs[spot, 0 : grid.rows]
    else:
        nx, ny, nz = plan.dense
        size = nx * ny * nz
        tall = height // 2
        down = weights((LANES, LANES), (row // 2 == column % nz) & (row < grid.block[2]), 0.5)
        many = dot(flat, down).reshape(count, tall, LANES)
        wide = up_to(size, LANES) // LANES
        here, lane = iota((tall, LANES), 0), iota((tall, LANES), 1)
        parts = []
        for vector in range(wide):
            cell = (vector * LANES + lane) // nz
            total = jnp.zeros((tall, LANES), F32)
            for spot in range(nx):
                total = total + jnp.where((cell == spot * ny + here) & (here < ny), many[spot], 0.0)
            parts.append(total)
        left = jnp.concatenate(parts, axis=1)[:, :size]
        high, middle, low = pieces(left)
        stack = jnp.concatenate([high, middle, low], axis=0)
        matrix = s.matrix
        one = product(stack, matrix[0])
        two = product(stack[: 2 * tall], matrix[1])
        three = product(high, matrix[2])
        total = one[:tall] + ((one[tall : 2 * tall] + one[2 * tall :]) + ((two[:tall] + two[tall:]) + three))
        answer = jnp.sum(total, axis=0, keepdims=True)
        here, lane = iota((grid.rows, LANES), 0), iota((grid.rows, LANES), 1)
        planes = []
        for spot in range(nx):
            value = jnp.zeros((grid.rows, LANES), F32)
            for vector in range(wide):
                if (vector + 1) * LANES <= spot * ny * nz or vector * LANES >= (spot + 1) * ny * nz:
                    continue
                piece = jnp.broadcast_to(answer[:, vector * LANES : (vector + 1) * LANES], value.shape)
                cell = (vector * LANES + lane) // nz
                value = jnp.where(cell == spot * ny + here // 2, piece, value)
            planes.append(value)
        spread = weights((LANES, LANES), (column // 2 == row % nz) & (column < grid.block[2]), 1.0)
        flat = dot(jnp.concatenate(planes, axis=0), spread).reshape(count, grid.rows, LANES)
        for spot in range(count):
            v.B[spot + 1] = v.B[spot + 1] + flat[spot]
    for colour in (0, 1, 0, 1):
        grid.half(v, colour, even, 0, count)


def kernel(plan, tree, density, dense, potential, *refs):
    held = jax.tree.unflatten(tree, refs)
    s = types.SimpleNamespace(**{key: named(value) for key, value in held.items()})
    counts, block, total = plan.counts, plan.block, plan.total
    top, wide, next_ = plan.top, plan.wide, plan.next
    place = tuple(lax.axis_index(axis) for axis in AXES)
    me = (place[0] * counts[1] + place[1]) * counts[2] + place[2]
    padded = block[2] != plan.width

    loads = [pltpu.make_async_copy(density, s.raw if padded else s.own, sem(s, OWN))]
    loads[0].start()
    if not padded:
        loads.append(
            pltpu.make_async_copy(
                density,
                s.field.at[pl.ds(8, block[0]), pl.ds(0, block[1]), pl.ds(0, block[2])],
                sem(s, FIELD),
            )
        )
    fill = pltpu.make_async_copy(dense, s.matrix, sem(s, MATRIX))

    for ref in s.land + [s.swap_land, s.swap_side]:
        ref[...] = jnp.zeros(ref.shape, F32)

    axes = [partners(place[axis], counts[axis]) for axis in range(3)]
    offsets = [
        (a, b, c) for a in range(counts[0]) for b in range(counts[1]) for c in range(counts[2]) if (a, b, c) != (0, 0, 0)
    ]
    offsets.sort(key=lambda off: -(off[0] + off[1] + off[2] / 2))

    def peer(off, way):
        target = tuple(axes[axis][off[axis]][way] for axis in range(3))
        return target, (target[0] * counts[1] + target[1]) * counts[2] + target[2]

    other = peer(offsets[0], 0)[0]
    barrier = pltpu.get_barrier_semaphore()
    for off in offsets:
        pl.semaphore_signal(barrier, inc=1, device_id=peer(off, 0)[0], device_id_type=MESH)

    for ref in (s.top.f, s.top.g, s.top.R, s.top.B):
        ref[...] = jnp.zeros(ref.shape, F32)
    for v, grid in ((s.top, top), (s.wide, wide), (s.next, next_)):
        grid.guard(v)
        grid.masks(v, place, counts)
    for v, grid in zip(s.levels, plan.levels):
        grid.guard(v)
        grid.masks(v, (0, 0, 0), (1, 1, 1))
    loads[0].wait()
    for load in loads[1:] + [fill]:
        load.start()
    own = s.own
    if padded:
        own[...] = jnp.zeros(own.shape, F32)
        own[:, :, 0 : block[2]] = s.raw[...]

    even_own = parity_of(block[1], plan.width)
    for number in range(top.inner):
        one, two = own[2 * number], own[2 * number + 1]
        red = jnp.where(even_own, one, two)
        spot = number + top.margins[0]
        s.top.f[spot, 0 : block[1], 0 : plan.width] = red
        s.top.g[spot, 0 : block[1], 0 : plan.width] = jnp.where(even_own, two, one)
        s.top.R[spot + 1, 0 : block[1], 0 : plan.width] = red * inverse
    even_top = parity_of(top.rows, top.lanes)
    count = top.count
    top.half(s.top, 1, even_top, 1, count - 1)
    top.half(s.top, 0, even_top, 1, count - 1)
    top.half(s.top, 1, even_top, 0, count)
    for number, value in top.residue(s.top, even_top, 0, count):
        for tile in range(plan.tiles):
            piece = value[:, tile * LANES : (tile + 1) * LANES]
            s.rows[tile][number, 0 : top.rows] = piece
            s.rows[tile][number, top.rows : top.rows + 8] = piece[block[1] :]
    flat = jnp.concatenate(
        [
            pair_sums(s.rows[tile], block[1] + 16, count).reshape(count * plan.high, LANES)
            for tile in range(plan.tiles)
        ],
        axis=1,
    )

    def fine_cell(shape, dim):
        index = iota(shape, dim)
        used = (index < block[2] + 4) | (index >= top.lanes - 4)
        cell = half_down(local_of(index, block[2], 4, top.lanes))
        return jnp.where(cell < 0, cell + LANES, cell), used

    shape = (top.lanes, LANES)
    cell, used = fine_cell(shape, 0)
    down = weights(shape, (cell == iota(shape, 1)) & used, 0.5)
    s.part[...] = dot(flat, down).reshape(count, plan.high, LANES)
    pack_part(plan, s)

    pl.semaphore_wait(barrier, total - 1)
    part = functools.partial(send_part, plan, s, place)
    far = functools.partial(send_far, plan, s, place)
    each(place, counts, part)

    lane = iota((block[1], LANES), 1)
    for side in range(2):
        begin = 0 if side == 0 else block[2] - 8
        tile = begin // LANES
        for pack in range(plan.far_packs):
            value = jnp.zeros((block[1], LANES), F32)
            for slot in range(16):
                plane = own[16 * pack + slot, :, tile * LANES : (tile + 1) * LANES]
                moved = pltpu.roll(plane, (8 * slot - begin) % LANES, 1)
                value = jnp.where(lane // 8 == slot, moved, value)
            s.far[side, pack] = value
    each(place, counts, far)
    field, far_land = s.field, s.far_land
    if padded:
        field[8 : 8 + block[0], 0 : block[1], 0 : plan.width] = own[...]
    for dim, step in ((0, -1), (0, 1), (1, -1), (1, 1), (2, -1), (2, 1)):
        steps = tuple(step if which == dim else 0 for which in range(3))

        @pl.when(jnp.logical_not(exists(place, steps, counts)))
        def _():
            if dim == 0:
                begin = 0 if step < 0 else 8 + block[0]
                field[begin : begin + 8] = jnp.zeros((8,) + field.shape[1:], F32)
                pack = 0 if step < 0 else plan.far_packs + 1
                far_land[:, pack] = jnp.zeros((2,) + far_land.shape[2:], F32)
            if dim == 1:
                begin = block[1] if step > 0 else block[1] + 8
                field[:, begin : begin + 8] = jnp.zeros((field.shape[0], 8, field.shape[2]), F32)
                far_land[:, :, begin : begin + 8] = jnp.zeros(far_land.shape[:2] + (8, LANES), F32)
            if dim == 2:
                far_land[(1 - step) // 2] = jnp.zeros(far_land.shape[1:], F32)

    wait_all(plan, s, place, size_part, PART + 1, other)
    gather_part(plan, s)
    even_next = parity_of(next_.rows, LANES)
    n = next_.count
    next_.first(s.next, 0, n)
    next_.half(s.next, 1, even_next, 1, n - 1)
    next_.half(s.next, 0, even_next, 2, n - 2)
    next_.half(s.next, 1, even_next, 2, n - 2)
    pairs = s.pairs
    rows1 = plan.block1[1]
    height = max(rows1, 16)
    if rows1 < height:
        pairs[0 : next_.inner, rows1:height] = jnp.zeros((next_.inner, height - rows1, LANES), F32)
    for number, value in next_.residue(s.next, even_next, 3, n - 3):
        pairs[number - 3, 0:rows1] = value[0:rows1]
    flat = pair_sums(pairs, height, next_.inner).reshape(next_.inner * (height // 2), LANES)
    row, column = iota((LANES, LANES), 0), iota((LANES, LANES), 1)
    down = weights((LANES, LANES), (row // 2 == column) & (row < plan.block1[2]), 0.5)
    below = dot(flat, down).reshape(next_.inner, height // 2, LANES)
    length = plan.block2
    per = LANES // length[2]
    packed = jnp.zeros((8, LANES), F32)
    for plane in range(length[0]):
        moved = below[plane]
        if plane // per:
            moved = pltpu.roll(moved, length[1] * (plane // per), 0)
        if plane % per:
            moved = pltpu.roll(moved, length[2] * (plane % per), 1)
        packed = packed + moved
    s.mine[...] = packed
    slots = s.slots
    slots[me] = packed

    def send(number, slot):
        return pltpu.make_async_remote_copy(
            src_ref=s.mine,
            dst_ref=slots.at[slot],
            send_sem=sem(s, ALL),
            recv_sem=sem(s, ALL + 1),
            device_id=peer(offsets[number], 0)[0],
            device_id_type=MESH,
        )

    def start_sends():
        for number in range(total - 1):
            send(number, me).start()

    start_sends()
    swap = functools.partial(send_swap, plan, s, place)
    pack_swap(plan, s)
    each(place, counts, swap)

    wait_all(plan, s, place, size_far, FAR + 1, other)
    if not padded:
        loads[1].wait()
    base = wide.lanes - LANES
    shape = (wide.rows, LANES)
    lane = iota(shape, 1)
    even_wide = parity_of(wide.rows, wide.lanes)
    above = block[2] - base

    def wide_plane(number):
        pack, slot = (number + 8) // 16, (number + 8) % 16
        high = pltpu.roll(far_land[0, pack], (above - 8 * slot) % LANES, 1)
        low = pltpu.roll(far_land[1, pack], (LANES - 8 - 8 * slot) % LANES, 1)
        old = field[number, :, 0:LANES] if base == 0 else 0.0
        value = jnp.where((lane >= above) & (lane < above + 8), high, old)
        value = jnp.where(lane >= LANES - 8, low, value)
        return value if base == 0 else jnp.concatenate([field[number, :, 0:base], value], axis=1)

    for number in range(wide.count):
        one, two = wide_plane(2 * number), wide_plane(2 * number + 1)
        s.wide.f[number] = jnp.where(even_wide, one, two)
        s.wide.g[number] = jnp.where(even_wide, two, one)
    n = wide.count
    wide.first(s.wide, 0, n)
    wide.half(s.wide, 1, even_wide, 1, n - 1)
    wide.half(s.wide, 0, even_wide, 1, n - 1)
    wide.half(s.wide, 1, even_wide, 2, n - 2)
    wider = iota((8, wide.lanes), 0) < 4

    def narrow(value):
        both = jnp.where(wider, value[block[1] : block[1] + 8], value[block[1] + 8 :])
        value = jnp.concatenate([value[: block[1]], both], axis=0)
        if top.lanes != wide.lanes:
            value = jnp.concatenate([value[:, : top.lanes - LANES], value[:, -LANES:]], axis=1)
        return value

    shift = wide.margins[0] - top.margins[0]
    for number in range(count):
        s.top.f[number] = narrow(s.wide.f[number + shift])
        s.top.g[number] = narrow(s.wide.g[number + shift])
        s.top.B[number + 1] = narrow(s.wide.B[number + shift + 1])

    def finish_sends():
        for name in (ALL + 1, ALL):
            pltpu.make_async_remote_copy(
                src_ref=s.bytes.at[pl.ds(0, total - 1)],
                dst_ref=s.bytes.at[pl.ds(0, total - 1)],
                send_sem=sem(s, name),
                recv_sem=sem(s, name),
                device_id=other,
                device_id_type=MESH,
            ).wait_recv()

    finish_sends()
    lane = iota((8, LANES), 1)
    whole = s.whole
    first = plan.levels[0]

    def place_x(which, carry):
        for second in range(counts[1]):
            start = (which * counts[1] + second) * counts[2]
            tiles = [slots[start + third] for third in range(counts[2])]
            for spot in range(per):
                value = jnp.zeros((8, LANES), F32)
                for third in range(counts[2]):
                    turn = (length[2] * (third - spot)) % LANES
                    moved = pltpu.roll(tiles[third], turn, 1) if turn else tiles[third]
                    value = jnp.where(lane // length[2] == third, moved, value)
                for group in range(8 // length[1]):
                    plane = which * length[0] + group * per + spot
                    whole[plane, second * length[1] : (second + 1) * length[1], :] = value[
                        group * length[1] : (group + 1) * length[1]
                    ]
        return carry

    lax.fori_loop(0, counts[0], place_x, 0)
    even_first = parity_of(first.rows, LANES)
    for number in range(first.count):
        one, two = whole[2 * number], whole[2 * number + 1]
        s.levels[0].f[number] = jnp.where(even_first, one, two)
        s.levels[0].g[number] = jnp.where(even_first, two, one)
    fill.wait()
    solve(plan, s, 0)
    solved = s.solved
    for number in range(3):
        solved[number] = jnp.zeros((first.rows, LANES), F32)
        solved[first.block[0] + 3 + number] = jnp.zeros((first.rows, LANES), F32)
    for plane in range(first.block[0]):
        solved[plane + 3] = first.planes(s.levels[0], even_first, plane)

    wait_all(plan, s, place, size_swap, SWAP + 1, other)
    wait_all(plan, s, place, size_swap, SWAP, other)
    shape = (LANES, LANES)
    index = iota(shape, 1)
    spot = local_of(index, plan.block1[2], 8, LANES)
    used = (index < plan.block1[2] + 8) | (index >= LANES - 8)
    lanes_to = weights(shape, (half_down(spot) + place[2] * length[2] == iota(shape, 0)) & used, 1.0)
    n = next_.count
    flat = jnp.concatenate([solved[place[0] * length[0] + number] for number in range(n)], axis=0)
    flat = dot(flat, lanes_to).reshape(n, first.rows, LANES)
    spread = s.spread
    spread[:, 0:16] = jnp.zeros((n, 16, LANES), F32)
    spread[:, 16 + 2 * first.rows :] = jnp.zeros((n, 16, LANES), F32)
    spread[0:n, pl.ds(16, first.rows, stride=2), :] = flat
    spread[0:n, pl.ds(17, first.rows, stride=2), :] = flat
    start = 16 + place[1] * rows1
    for number in range(n):
        tiles = [
            spread[number, pl.ds(pl.multiple_of(start + shift, 8), size), :]
            for shift, size in ((0, rows1), (rows1, 8), (-8, 8))
        ]
        s.next.B[number + 1] = swapped(plan, s, number) + jnp.concatenate(tiles, axis=0)
    for colour, skip in ((0, 0), (1, 1), (0, 1), (1, 2)):
        next_.half(s.next, colour, even_next, skip, n - skip)

    pick = iota((8, LANES), 0) < 4
    planes = []
    for number in range(count):
        value = next_.planes(s.next, even_next, number + 2 * next_.margins[0] - top.margins[0])
        edge = jnp.where(pick, value[rows1 : rows1 + 8], value[rows1 + 8 :])
        planes.append(jnp.concatenate([value[:rows1], edge], axis=0))
    shape = (LANES, top.lanes)
    cell, used = fine_cell(shape, 1)
    spreading = weights(shape, (cell == iota(shape, 0)) & used, 1.0)
    flat = dot(jnp.concatenate(planes, axis=0), spreading).reshape(count, plan.high, top.lanes)
    for tile in range(plan.tiles):
        piece = flat[:, :, tile * LANES : (tile + 1) * LANES]
        s.rows[tile][0:count, pl.ds(0, plan.high, stride=2), :] = piece
        s.rows[tile][0:count, pl.ds(1, plan.high, stride=2), :] = piece
    for number in range(count):
        tiles = []
        for tile in range(plan.tiles):
            rows = s.rows[tile]
            edge = jnp.where(pick, rows[number, block[1] : block[1] + 8], rows[number, block[1] + 8 : block[1] + 16])
            tiles.append(jnp.concatenate([rows[number, 0 : block[1]], edge], axis=0))
        s.top.B[number + 1] = s.top.B[number + 1] + jnp.concatenate(tiles, axis=1)
    top.half(s.top, 0, even_top, 0, count)
    top.half(s.top, 1, even_top, 1, count - 1)
    top.half(s.top, 0, even_top, 1, count - 1)
    red = s.top.R
    even_out = parity_of(block[1], block[2])
    for number, value in top.totals(red, even_top, 1, top.margins[0], count - top.margins[0]):
        black = ((s.top.g[number] + value) * inverse)[0 : block[1], 0 : block[2]]
        old = red[number + 1][0 : block[1], 0 : block[2]]
        plane = 2 * (number - top.margins[0])
        potential[plane] = jnp.where(even_out, old, black)
        potential[plane + 1] = jnp.where(even_out, black, old)
    wait_all(plan, s, place, size_part, PART, other)
    wait_all(plan, s, place, size_far, FAR, other)


def cycle_matrix(size, depth):
    def beside_sum(v):
        p = np.pad(v, ((0, 0), (1, 1), (1, 1), (1, 1)))
        total = p[:, 2:, 1:-1, 1:-1] + p[:, :-2, 1:-1, 1:-1] + p[:, 1:-1, 2:, 1:-1] + p[:, 1:-1, :-2, 1:-1]
        return total + along * (p[:, 1:-1, 1:-1, 2:] + p[:, 1:-1, 1:-1, :-2])

    def cycle(g, left):
        parity = np.indices(g.shape[1:]).sum(0) % 2

        def sweeps(v, number):
            for _ in range(number):
                for colour in (0, 1):
                    v = np.where(parity == colour, (g + beside_sum(v)) / centre, v)
            return v

        v = np.zeros_like(g)
        if left == 0:
            return sweeps(v, CSWEEPS)
        v = sweeps(v, 2)
        r = g - centre * v + beside_sum(v)
        x, y, z = (part // 2 for part in g.shape[1:])
        coarse = 4 * r.reshape(-1, x, 2, y, 2, z, 2).mean((2, 4, 6))
        e = cycle(coarse, left - 1)
        for dim in (1, 2, 3):
            e = np.repeat(e, 2, dim)
        return sweeps(v + e, 2)

    cells = size[0] * size[1] * size[2]
    found = cycle(np.eye(cells).reshape((cells,) + size), depth).reshape(cells, cells)
    parts = []
    for _ in range(3):
        parts.append(found.astype(np.float32).astype(jnp.bfloat16))
        found = found - parts[-1].astype(np.float64)
    return np.stack(parts)


def on_device(counts, density):
    plan = Plan(density.shape, counts)
    scratch, tree = jax.tree.flatten(plan.scratch())
    matrix = jnp.asarray(cycle_matrix(plan.dense, LEVELS - 1 - plan.dense_level))
    return pl.pallas_call(
        functools.partial(kernel, plan, tree),
        out_shape=jax.ShapeDtypeStruct(density.shape, F32),
        in_specs=[pl.BlockSpec(memory_space=pltpu.HBM)] * 2,
        out_specs=pl.BlockSpec(memory_space=pltpu.VMEM),
        scratch_shapes=scratch,
        compiler_params=pltpu.CompilerParams(
            collective_id=0, has_side_effects=True, vmem_limit_bytes=48 * 1024 * 1024
        ),
    )(
        pltpu.with_memory_space_constraint(density, pltpu.HBM),
        pltpu.with_memory_space_constraint(matrix, pltpu.HBM),
    )


def solution(mesh):
    counts = tuple(mesh.shape[axis] for axis in AXES)
    return jax.shard_map(
        functools.partial(on_device, counts),
        mesh=mesh,
        in_specs=(P("gx", "gy", "gz"),),
        out_specs=P("gx", "gy", "gz"),
        check_vma=False,
    )
```

```python
import functools
import types

import jax
import jax.numpy as jnp
import numpy as np
from jax import lax
from jax.experimental import pallas as pl
from jax.experimental.pallas import tpu as pltpu
from jax.sharding import PartitionSpec as P

LEVELS = 7
CSWEEPS = 4
DENSE = 512
rsd_beta = 0.5
centre = 4.0 + 2.0 * (1.0 + rsd_beta)
along = 1.0 + rsd_beta
inverse = 1.0 / centre
F32 = jnp.float32
BF16 = jnp.bfloat16
LANES = 128
AXES = ("gx", "gy", "gz")
MESH = pl.DeviceIdType.MESH
DIRECTIONS = [
    (dx, dy, dz) for dx in (-1, 0, 1) for dy in (-1, 0, 1) for dz in (-1, 0, 1) if (dx, dy, dz) != (0, 0, 0)
]


ALL, PART, FAR, SWAP, OWN, FIELD, MATRIX = 0, 2, 4, 6, 8, 9, 10


def up_to(value, unit):
    return -(-value // unit) * unit


def iota(shape, dim):
    return lax.broadcasted_iota(jnp.int32, shape, dim)


def pieces(value):
    high = value.astype(BF16)
    rest = value - high.astype(F32)
    middle = rest.astype(BF16)
    return high, middle, (rest - middle.astype(F32)).astype(BF16)


def product(left, right):
    return jnp.dot(left, right, preferred_element_type=F32)


def dot(value, chosen):
    chosen = chosen.astype(BF16)
    parts = [product(part, chosen) for part in pieces(value)]
    return parts[0] + (parts[1] + parts[2])


def local_of(index, length, margin, total):
    return jnp.where(index < total - margin, index, index - total)


def half_down(value):
    return jnp.where(value >= 0, lax.div(value, 2), -lax.div(1 - value, 2))


def parity_of(rows, lanes, step=1):
    return (iota((rows, lanes), 0) + iota((rows, lanes), 1) // step) % 2 == 0


def beside(below, here, above, down, up, even, colour, edge, step):
    lanes = here.shape[1]
    left, right = pltpu.roll(here, step, 1), pltpu.roll(here, lanes - step, 1)
    if edge is not None:
        if edge[1] * step == lanes:
            lane = iota(here.shape, 1)
            left = jnp.where(lane < step, 0.0, left)
            right = jnp.where(lane >= lanes - step, 0.0, right)
    other = jnp.where(even, below, above) if colour == 0 else jnp.where(even, above, below)
    return (here + other) + (down + up) + along * (left + right)


class Grid:
    def __init__(self, block, margins, edge=False, step=1):
        self.block, self.margins, self.step = block, margins, step
        self.inner = block[0] // 2
        self.count = self.inner + 2 * margins[0]
        self.rows = up_to(block[1] + 2 * margins[1], 8)
        self.lanes = up_to(block[2] + 2 * margins[2], LANES)
        self.edge = (block[1], block[2]) if edge else None
        self.tiles = self.lanes // LANES

    def scratch(self):
        field = (self.count + 2, self.rows + 16, LANES)
        source = (self.count, self.rows, self.lanes)
        return dict(
            R=[pltpu.VMEM(field, F32) for _ in range(self.tiles)],
            B=[pltpu.VMEM(field, F32) for _ in range(self.tiles)],
            f=pltpu.VMEM(source, F32),
            g=pltpu.VMEM(source, F32),
            m=pltpu.VMEM((3, self.rows, self.lanes), F32),
        )

    def zone(self, number):
        if number < self.margins[0]:
            return 0
        return 2 if number >= self.count - self.margins[0] else 1

    def guard(self, v):
        empty = jnp.zeros((self.rows + 16, LANES), F32)
        for ref in v.R + v.B:
            ref[0] = empty
            ref[self.count + 1] = empty
            if self.edge:
                ref[:, 0:8] = jnp.zeros((self.count + 2, 8, LANES), F32)
                ref[:, self.rows + 8 :] = jnp.zeros((self.count + 2, 8, LANES), F32)

    def get(self, field, number, shift=0):
        parts = [ref[number, 8 + shift : 8 + shift + self.rows] for ref in field]
        return parts[0] if len(parts) == 1 else jnp.concatenate(parts, axis=1)

    def put(self, field, number, value):
        for tile, ref in enumerate(field):
            piece = value[:, tile * LANES : (tile + 1) * LANES]
            ref[number, 8 : 8 + self.rows] = piece
            if not self.edge:
                ref[number, 0:8] = piece[self.rows - 8 :]
                ref[number, 8 + self.rows :] = piece[0:8]

    def masks(self, v, place, counts):
        inside = None
        shape = (self.rows, self.lanes)
        for dim in (1, 2):
            index = iota(shape, dim - 1)
            size = shape[dim - 1]
            if dim == 2 and self.step > 1:
                inside = inside & (index % self.step == 0) & (index < self.step * self.block[2])
                continue
            margin, length = self.margins[dim], self.block[dim]
            used = (index < length + margin) | (index >= size - margin)
            spot = local_of(index, length, margin, size) + place[dim] * length
            used = used & (spot >= 0) & (spot < length * counts[dim])
            inside = used if inside is None else inside & used
        value = jnp.where(inside, inverse, 0.0).astype(F32)
        v.m[1] = value
        if self.margins[0]:
            low = jnp.where(place[0] > 0, 1.0, 0.0).astype(F32)
            high = jnp.where(place[0] < counts[0] - 1, 1.0, 0.0).astype(F32)
            v.m[0] = value * low
            v.m[2] = value * high

    def first(self, v, begin, end):
        for number in range(begin, end):
            self.put(v.R, number + 1, v.f[number] * v.m[self.zone(number)])

    def totals(self, other, even, colour, begin, end):
        before, here = self.get(other, begin), self.get(other, begin + 1)
        for number in range(begin, end):
            after = self.get(other, number + 2)
            down, up = self.get(other, number + 1, -1), self.get(other, number + 1, 1)
            yield number, beside(before, here, after, down, up, even, colour, self.edge, self.step)
            before, here = here, after

    def half(self, v, colour, even, begin, end):
        target, other = (v.R, v.B) if colour == 0 else (v.B, v.R)
        source = v.f if colour == 0 else v.g
        for number, total in self.totals(other, even, colour, begin, end):
            self.put(target, number + 1, (source[number] + total) * v.m[self.zone(number)])

    def residue(self, v, even, begin, end):
        for number, total in self.totals(v.B, even, 0, begin, end):
            yield number, v.f[number] - centre * self.get(v.R, number + 1) + total

    def planes(self, v, even, plane):
        red, black = self.get(v.R, plane // 2 + 1), self.get(v.B, plane // 2 + 1)
        return jnp.where(even, red, black) if plane % 2 == 0 else jnp.where(even, black, red)


def exists(place, steps, counts):
    found = None
    for which in range(3):
        if steps[which] == 0:
            continue
        other = place[which] + steps[which]
        here = (other >= 0) & (other < counts[which])
        found = here if found is None else found & here
    return found


def device(place, steps):
    return tuple(place[which] + steps[which] for which in range(3))


class Plan:
    def __init__(self, block, counts):
        self.counts, self.block = counts, block
        self.total = counts[0] * counts[1] * counts[2]
        self.block1 = tuple(size // 2 for size in block)
        self.block2 = tuple(size // 4 for size in block)
        self.top = Grid(block, (2, 4, 4))
        self.wide = Grid(block, (4, 8, 8))
        self.next = Grid(self.block1, (3, 8, 8))
        self.width = up_to(block[2], LANES)
        self.tiles = self.top.lanes // LANES
        self.count = self.top.count
        self.high = self.block1[1] + 8
        self.per = LANES // self.block1[2]
        self.side = 8 // self.per
        self.middle = (self.count - 16) // self.per
        self.vectors = 2 * self.side + self.middle + 1
        self.packs = 1 + (self.count > 16)
        self.far_packs = block[0] // 16
        assert block[0] % 16 == 0 and self.block1[1] % 8 == 0 and self.block2[2] <= LANES
        assert self.next.lanes == LANES and (self.count - 16) % self.per == 0 and 64 % self.block1[2] == 0
        self.levels = []
        size = tuple(block[which] * counts[which] // 4 for which in range(3))
        number = 2
        while size[0] * size[1] * size[2] > DENSE:
            self.levels.append(Grid(size, (0, 0, 0), edge=True, step=1 << len(self.levels)))
            assert self.levels[-1].lanes == LANES
            size = tuple(part // 2 for part in size)
            number += 1
        self.dense, self.dense_level = size, number

    def message(self, steps):
        dx, dy, dz = steps
        if dz == 0:
            begin, length = {0: (0, self.vectors), -1: (0, self.side + 1), 1: (self.side, self.side + 1)}[dx]
            if dy == 0:
                return ("part_t", (pl.ds(begin, length),), (length, self.high, LANES))
            return ("part_y", ((dy + 1) // 2, pl.ds(begin, length)), (length, 8, LANES))
        length = self.packs if dx == 0 else 1
        if dy == 0:
            return ("part_z", ((dz + 1) // 2, pl.ds(0, length)), (length, self.high, LANES))
        return (
            "part_zy", ((dz + 1) // 2, (dy + 1) // 2, pl.ds(0, length)), (length, 8, LANES),
        )

    def scratch(self):
        block = self.block
        s = types.SimpleNamespace(
            top=self.top.scratch(), wide=self.wide.scratch(), next=self.next.scratch(),
            levels=[grid.scratch() for grid in self.levels],
        )
        s.own = pltpu.VMEM((block[0], block[1], self.width), F32)
        if block[2] != self.width:
            s.raw = pltpu.VMEM(block, F32)
        s.field = pltpu.VMEM((block[0] + 16, block[1] + 16, self.wide.lanes), F32)
        s.rows = [pltpu.VMEM((self.count, block[1] + 16, LANES), F32) for _ in range(self.tiles)]
        s.part = pltpu.VMEM((self.count, self.high, LANES), F32)
        s.part_t = pltpu.VMEM((self.vectors, self.high, LANES), F32)
        s.part_y = pltpu.VMEM((2, self.vectors, 8, LANES), F32)
        s.part_z = pltpu.VMEM((2, self.packs, self.high, LANES), F32)
        s.part_zy = pltpu.VMEM((2, 2, self.packs, 8, LANES), F32)
        s.land = [pltpu.VMEM(self.message(steps)[2], F32) for steps in DIRECTIONS]
        s.sums, s.sumz = [], []
        wide_rows = self.block1[1] + 16
        for dx in (-1, 0, 1):
            length = self.vectors if dx == 0 else self.side + 1
            packs = self.packs if dx == 0 else 1
            s.sums.append(pltpu.VMEM((length, wide_rows, LANES), F32))
            s.sumz.append(pltpu.VMEM((2, packs, wide_rows, LANES), F32))
        s.far = pltpu.VMEM((2, self.far_packs, block[1], LANES), F32)
        s.far_land = pltpu.VMEM((2, self.far_packs + 2, block[1] + 16, LANES), F32)
        s.swap = pltpu.VMEM((2, self.block1[1], LANES), F32)
        s.swap_land = pltpu.VMEM((self.next.count, self.next.rows, LANES), F32)
        s.swap_side = pltpu.VMEM((2, 3, self.next.rows, LANES), F32)
        first = self.levels[0]
        coarse = [first] + self.levels[1:]
        s.pairs = pltpu.VMEM((max(g.block[0] for g in coarse + [self.next]), 2 * up_to(first.rows, 16), LANES), F32)
        s.solved = pltpu.VMEM((first.block[0] + 6, first.rows, LANES), F32)
        s.spread = pltpu.VMEM((self.next.count, 2 * first.rows + 32, LANES), F32)
        s.whole = pltpu.VMEM((first.block[0], first.rows, LANES), F32)
        s.mine = pltpu.VMEM((8, LANES), F32)
        s.slots = pltpu.VMEM((self.total, 8, LANES), F32)
        size = self.dense[0] * self.dense[1] * self.dense[2]
        s.matrix = pltpu.VMEM((3, size, size), BF16)
        most = max(sum(size(self, steps) for steps in DIRECTIONS) for size in (size_part, size_far, size_swap))
        s.bytes = pltpu.VMEM((max(most, self.total), 8, LANES), F32)
        s.sem = pltpu.SemaphoreType.DMA((MATRIX + 1,))
        return vars(s)


def weights(shape, found, value):
    return jnp.where(found, value, 0.0).astype(F32).reshape(shape)


def pair_sums(s, height, count):
    even = s[0:count, pl.ds(0, height // 2, stride=2), :]
    return even + s[0:count, pl.ds(1, height // 2, stride=2), :]


def named(value):
    if isinstance(value, dict):
        return types.SimpleNamespace(**value)
    return [named(one) for one in value] if isinstance(value, list) else value


def sem(s, number):
    return s.sem.at[number]


def size_part(plan, steps):
    shape = plan.message(steps)[2]
    return shape[0] * shape[1] // 8


def size_far(plan, steps):
    rows = plan.block[1] // 8 if steps[1] == 0 else 1
    if steps[2]:
        return rows * (plan.far_packs if steps[0] == 0 else 1)
    return rows * (plan.block[0] if steps[0] == 0 else 8) * (plan.width // LANES)


def size_swap(plan, steps):
    rows = plan.block1[1] // 8 if steps[1] == 0 else 1
    return rows if steps[2] else rows * (plan.next.inner if steps[0] == 0 else plan.next.margins[0])


def wait_all(plan, s, place, size, name, other):
    counts = plan.counts
    beside_of = [
        jnp.where(place[axis] > 0, 1, 0) + jnp.where(place[axis] < counts[axis] - 1, 1, 0) for axis in range(3)
    ]
    choices = [{1: (0,), 2: (1,)}.get(count, (1, 2)) for count in counts]
    for x in choices[0]:
        for y in choices[1]:
            for z in choices[2]:
                number = 0
                for steps in DIRECTIONS:
                    many = [1 if step == 0 else (have if step > 0 else 0) for step, have in zip(steps, (x, y, z))]
                    if min(steps) >= 0:
                        number += many[0] * many[1] * many[2] * size(plan, steps)
                if number == 0:
                    continue
                found = (beside_of[0] == x) & (beside_of[1] == y) & (beside_of[2] == z)

                @pl.when(found)
                def _():
                    pltpu.make_async_remote_copy(
                        src_ref=s.bytes.at[pl.ds(0, number)],
                        dst_ref=s.bytes.at[pl.ds(0, number)],
                        send_sem=sem(s, name),
                        recv_sem=sem(s, name),
                        device_id=other,
                        device_id_type=MESH,
                    ).wait_recv()


def send_part(plan, s, place, number):
    steps = DIRECTIONS[number]
    name, index, _ = plan.message(steps)
    return pltpu.make_async_remote_copy(
        src_ref=getattr(s, name).at[index],
        dst_ref=s.land[number],
        send_sem=sem(s, PART),
        recv_sem=sem(s, PART + 1),
        device_id=device(place, steps),
        device_id_type=MESH,
    )


def send_far(plan, s, place, number):
    dx, dy, dz = steps = DIRECTIONS[number]
    block = plan.block
    rows = {0: (0, block[1], 0), 1: (block[1] - 8, 8, block[1] + 8), -1: (0, 8, block[1])}[dy]
    if dz == 0:
        planes = {0: (0, block[0], 8), 1: (block[0] - 8, 8, 0), -1: (0, 8, block[0] + 8)}[dx]
        source = s.own.at[pl.ds(planes[0], planes[1]), pl.ds(rows[0], rows[1]), :]
        target = s.field.at[pl.ds(planes[2], planes[1]), pl.ds(rows[2], rows[1]), pl.ds(0, plan.width)]
    else:
        side, last = (dz + 1) // 2, plan.far_packs - 1
        packs = {0: (0, last + 1, 1), 1: (last, 1, 0), -1: (0, 1, last + 2)}[dx]
        source = s.far.at[side, pl.ds(packs[0], packs[1]), pl.ds(rows[0], rows[1]), :]
        target = s.far_land.at[side, pl.ds(packs[2], packs[1]), pl.ds(rows[2], rows[1]), :]
    return pltpu.make_async_remote_copy(
        src_ref=source,
        dst_ref=target,
        send_sem=sem(s, FAR),
        recv_sem=sem(s, FAR + 1),
        device_id=device(place, steps),
        device_id_type=MESH,
    )


def send_swap(plan, s, place, number):
    dx, dy, dz = steps = DIRECTIONS[number]
    high, margin, inner = plan.block1[1], plan.next.margins[0], plan.next.inner
    rows = {0: (0, high, 0), 1: (high - 8, 8, high + 8), -1: (0, 8, high)}[dy]
    if dz == 0:
        planes = {0: (margin, inner, margin), 1: (inner, margin, 0), -1: (margin, margin, margin + inner)}[dx]
        source = s.next.B[0].at[pl.ds(1 + planes[0], planes[1]), pl.ds(8 + rows[0], rows[1]), :]
        target = s.swap_land.at[pl.ds(planes[2], planes[1]), pl.ds(rows[2], rows[1]), :]
    else:
        side = (dz + 1) // 2
        source = s.swap.at[side, pl.ds(rows[0], rows[1]), :]
        target = s.swap_side.at[side, 1 - dx, pl.ds(rows[2], rows[1]), :]
    return pltpu.make_async_remote_copy(
        src_ref=source,
        dst_ref=target,
        send_sem=sem(s, SWAP),
        recv_sem=sem(s, SWAP + 1),
        device_id=device(place, steps),
        device_id_type=MESH,
    )


def pack_swap(plan, s):
    length, margin = plan.block1[2], plan.next.margins[0]
    lane = iota((plan.block1[1], LANES), 1)
    for side in range(2):
        begin = 0 if side == 0 else length - 8
        value = jnp.zeros(lane.shape, F32)
        for slot in range(plan.next.inner):
            plane = s.next.B[0][1 + margin + slot, 8 : 8 + plan.block1[1], :]
            value = jnp.where(lane // 8 == slot, pltpu.roll(plane, (8 * slot - begin) % LANES, 1), value)
        s.swap[side] = value


def swapped(plan, s, number):
    length, rows = plan.block1[2], plan.block1[1]
    margin, inner = plan.next.margins[0], plan.next.inner
    lane = iota((plan.next.rows, LANES), 1)
    which = 0 if number < margin else (2 if number >= margin + inner else 1)
    slot = number - margin + (1 - which) * inner
    value = s.swap_land[number]
    if which == 1:
        value = jnp.concatenate([s.next.B[0][number + 1, 8 : 8 + rows, :], value[rows:]], axis=0)
    high = pltpu.roll(s.swap_side[0, which], (length - 8 * slot) % LANES, 1)
    low = pltpu.roll(s.swap_side[1, which], (LANES - 8 - 8 * slot) % LANES, 1)
    edge = jnp.where(lane < length + 8, high, jnp.where(lane >= LANES - 8, low, 0.0))
    return jnp.where(lane < length, value, edge)


def partners(place, count):
    if count & (count - 1):
        return [(lax.rem(place + off, count), lax.rem(place + count - off, count)) for off in range(count)]
    bits = [lax.rem(lax.div(place, 1 << bit), 2) for bit in range(count.bit_length() - 1)]
    out = []
    for off in range(count):
        value = jnp.int32(0)
        for bit, digit in enumerate(bits):
            value = value + ((1 - digit) if off >> bit & 1 else digit) * (1 << bit)
        out.append((value, value))
    return out


def each(place, counts, send):
    for number, steps in enumerate(DIRECTIONS):
        @pl.when(exists(place, steps, counts))
        def _():
            send(number).start()


def pack_part(plan, s):
    count, per, side, middle, rows = plan.count, plan.per, plan.side, plan.middle, plan.block1[1]
    length = plan.block1[2]
    part = s.part
    shape = (plan.high, LANES)
    lane = iota(shape, 1)
    sub = iota((8, LANES), 0)

    def pair_y(value):
        edge = value[rows:]
        minus = jnp.where(sub >= 6, edge, value[:8])
        return minus, jnp.where(sub < 2, edge, value[rows - 8 : rows])

    groups = [(0, 0, side), (side + 1, count - 8, side), (2 * side + 1, 8, middle)]
    for index, first, number in groups:
        for spot in range(number):
            value = part[first + spot]
            for which in range(1, per):
                moved = pltpu.roll(part[first + spot + which * number], which * length, 1)
                value = jnp.where(lane // length == which, moved, value)
            s.part_t[index + spot] = value
            minus, plus = pair_y(value)
            s.part_y[0, index + spot] = minus
            s.part_y[1, index + spot] = plus
    value = jnp.zeros(shape, F32)
    couple = lane // 2
    for number in range(count):
        low = pltpu.roll(part[number], 2 * number, 1)
        high = low if length == 64 else pltpu.roll(part[number], 64 - length + 2 * number, 1)
        value = jnp.where(couple == ((126 + 2 * number) % LANES) // 2, low, value)
        value = jnp.where(couple == 32 + number, high, value)
    s.part_t[side] = value
    minus, plus = pair_y(value)
    s.part_y[0, side] = minus
    s.part_y[1, side] = plus
    for which in range(2):
        begin = LANES - 2 if which == 0 else length - 6
        for pack in range(plan.packs):
            value = jnp.zeros(shape, F32)
            planes = list(range(8)) + list(range(count - 8, count)) if pack == 0 else list(range(8, count - 8))
            for slot, number in enumerate(planes):
                moved = pltpu.roll(part[number], (8 * slot - begin) % LANES, 1)
                value = jnp.where(lane // 8 == slot, moved, value)
            s.part_z[which, pack] = value
            minus, plus = pair_y(value)
            s.part_zy[which, 0, pack] = minus
            s.part_zy[which, 1, pack] = plus


def gather_part(plan, s):
    side, count, rows, per, length = plan.side, plan.count, plan.block1[1], plan.per, plan.block1[2]
    sub = iota((8, LANES), 0)
    land = {steps: s.land[number] for number, steps in enumerate(DIRECTIONS)}

    def assembled(own, plus, minus):
        edge = own[rows:]
        tiles = [own[8 * number : 8 * number + 8] for number in range(rows // 8)]
        tiles[0] = tiles[0] + jnp.where(sub < 2, minus, 0.0)
        tiles[-1] = tiles[-1] + jnp.where(sub >= 6, plus, 0.0)
        tiles.append(jnp.where(sub < 6, plus, 0.0) + jnp.where(sub < 2, edge, 0.0))
        tiles.append(jnp.where(sub >= 2, minus, 0.0) + jnp.where(sub >= 6, edge, 0.0))
        return jnp.concatenate(tiles, axis=0)

    for dx in (-1, 0, 1):
        own = s.part_t if dx == 0 else land[(dx, 0, 0)]
        for index in range(own.shape[0]):
            s.sums[dx + 1][index] = assembled(own[index], land[(dx, -1, 0)][index], land[(dx, 1, 0)][index])
        for which in range(2):
            dz = 2 * which - 1
            for pack in range(land[(dx, 0, dz)].shape[0]):
                s.sumz[dx + 1][which, pack] = assembled(
                    land[(dx, 0, dz)][pack], land[(dx, -1, dz)][pack], land[(dx, 1, dz)][pack]
                )

    shape = (rows + 16, LANES)
    lane = iota(shape, 1)
    at_low, at_high = lane >= LANES - 2, (lane == length) | (lane == length + 1)
    inner = lane < length
    above = (lane >= length - 2) & (lane < length + 6)
    below = (lane >= LANES - 6) | (lane < 2)
    even = parity_of(*shape)

    def turned(value, shift):
        shift = shift % LANES
        return pltpu.roll(value, shift, 1) if shift else value

    def plane_of(dx, number):
        if number < 8:
            index, slots, size, first = number, number, side, 0
            base = 0
        elif number >= count - 8:
            index, slots, size, first = number - (count - 8), 8 + number - (count - 8), side, count - 8
            base = side + 1
        else:
            index, slots, size, first = number - 8, number - 8, plan.middle, 8
            base = 2 * side + 1
        pack = 0 if number < 8 or number >= count - 8 else 1
        extra = side
        if dx == -1:
            base, extra = 0, side
        if dx == 1:
            base, extra = 1, 0
        total = s.sums[dx + 1]
        main = turned(total[base + index % size], -(index // size) * length)
        low = turned(total[extra], -2 * number)
        high = low if length == 64 else turned(total[extra], length - 64 - 2 * number)
        value = jnp.where(inner, main, jnp.where(at_low, low, jnp.where(at_high, high, 0.0)))
        far = s.sumz[dx + 1]
        from_above = turned(far[0, pack], length - 2 - 8 * slots)
        from_below = turned(far[1, pack], LANES - 6 - 8 * slots)
        return value + (jnp.where(above, from_above, 0.0) + jnp.where(below, from_below, 0.0))

    def plane(number):
        spot = number - 2 * plan.next.margins[0]
        total = None
        for dx, place in ((0, spot), (-1, spot - plan.block1[0]), (1, spot + plan.block1[0])):
            index = place + 2
            allowed = {0: (0, count), -1: (0, 8), 1: (count - 8, count)}[dx]
            if allowed[0] <= index < allowed[1]:
                value = plane_of(dx, index)
                total = value if total is None else total + value
        return total

    for number in range(plan.next.count):
        first, second = plane(2 * number), plane(2 * number + 1)
        s.next.f[number] = jnp.where(even, first, second)
        s.next.g[number] = jnp.where(even, second, first)


def solve(plan, s, number):
    grid, v = plan.levels[number], s.levels[number]
    even = parity_of(grid.rows, LANES, grid.step)
    count, step = grid.count, grid.step
    grid.first(v, 0, count)
    for colour in (1, 0, 1):
        grid.half(v, colour, even, 0, count)
    pairs = s.pairs
    height = max(grid.rows, 16)
    if grid.rows < height:
        pairs[0:count, grid.rows : height] = jnp.zeros((count, height - grid.rows, LANES), F32)
    for spot, value in grid.residue(v, even, 0, count):
        if grid.rows > grid.block[1]:
            value = jnp.where(iota(value.shape, 0) < grid.block[1], value, 0.0)
        pairs[spot, 0 : grid.rows] = value
    sums = pair_sums(pairs, height, count)
    row, column = iota((LANES, LANES), 0), iota((LANES, LANES), 1)
    if number + 1 < len(plan.levels):
        below, under = plan.levels[number + 1], s.levels[number + 1]
        same = parity_of(below.rows, LANES, below.step)
        lane = iota((below.rows, LANES), 1)
        coarse = []
        for spot in range(count):
            value = sums[spot][: below.rows]
            value = 0.5 * (value + pltpu.roll(value, LANES - step, 1))
            coarse.append(jnp.where((lane % below.step == 0) & (lane < step * grid.block[2]), value, 0.0))
        for spot in range(below.count):
            one, two = coarse[2 * spot], coarse[2 * spot + 1]
            under.f[spot] = jnp.where(same, one, two)
            under.g[spot] = jnp.where(same, two, one)
        solve(plan, s, number + 1)
        for spot in range(count):
            plane = below.planes(under, same, spot)
            plane = plane + pltpu.roll(plane, step, 1)
            pairs[spot, pl.ds(0, below.rows, stride=2), :] = plane
            pairs[spot, pl.ds(1, below.rows, stride=2), :] = plane
        for spot in range(count):
            grid.put(v.B, spot + 1, grid.get(v.B, spot + 1) + pairs[spot, 0 : grid.rows])
    else:
        nx, ny, nz = plan.dense
        size = nx * ny * nz
        tall = height // 2
        flat = sums.reshape(count * (height // 2), LANES)
        down = weights((LANES, LANES), (row // (2 * step) == column % nz) & (row < step * grid.block[2]), 0.5)
        many = dot(flat, down).reshape(count, tall, LANES)
        wide = up_to(size, LANES) // LANES
        here, lane = iota((tall, LANES), 0), iota((tall, LANES), 1)
        parts = []
        for vector in range(wide):
            cell = (vector * LANES + lane) // nz
            total = jnp.zeros((tall, LANES), F32)
            for spot in range(nx):
                total = total + jnp.where((cell == spot * ny + here) & (here < ny), many[spot], 0.0)
            parts.append(total)
        left = jnp.concatenate(parts, axis=1)[:, :size]
        high, middle, low = pieces(left)
        stack = jnp.concatenate([high, middle, low], axis=0)
        matrix = s.matrix
        one = product(stack, matrix[0])
        two = product(stack[: 2 * tall], matrix[1])
        three = product(high, matrix[2])
        total = one[:tall] + ((one[tall : 2 * tall] + one[2 * tall :]) + ((two[:tall] + two[tall:]) + three))
        answer = jnp.sum(total, axis=0, keepdims=True)
        here, lane = iota((grid.rows, LANES), 0), iota((grid.rows, LANES), 1)
        planes = []
        for spot in range(nx):
            value = jnp.zeros((grid.rows, LANES), F32)
            for vector in range(wide):
                if (vector + 1) * LANES <= spot * ny * nz or vector * LANES >= (spot + 1) * ny * nz:
                    continue
                piece = jnp.broadcast_to(answer[:, vector * LANES : (vector + 1) * LANES], value.shape)
                cell = (vector * LANES + lane) // nz
                value = jnp.where(cell == spot * ny + here // 2, piece, value)
            planes.append(value)
        spread = weights(
            (LANES, LANES),
            (column // (2 * step) == row % nz) & (column < step * grid.block[2]) & (column % step == 0),
            1.0,
        )
        flat = dot(jnp.concatenate(planes, axis=0), spread).reshape(count, grid.rows, LANES)
        for spot in range(count):
            grid.put(v.B, spot + 1, grid.get(v.B, spot + 1) + flat[spot])
    for colour in (0, 1, 0, 1):
        grid.half(v, colour, even, 0, count)


def first_black(plan, s, even):
    top, high, wide = plan.top, plan.block[1], plan.width
    lane = iota((high, wide), 1)
    none = jnp.zeros((high, LANES), F32)

    def load(number, shift=0, begin=0, size=high):
        parts = [ref[number, 8 + begin + shift : 8 + begin + shift + size] for ref in s.top.R[:-1]]
        return parts[0] if len(parts) == 1 else jnp.concatenate(parts, axis=1)

    for number in range(1, top.count - 1):
        total = jnp.where(even, load(number + 2), load(number))
        edge, side = jnp.zeros((8, wide), F32), none
        if top.zone(number) == 1:
            here = load(number + 1)
            left, right = pltpu.roll(here, 1, 1), pltpu.roll(here, wide - 1, 1)
            beside_z = jnp.where(lane == 0, 0.0, left) + jnp.where(lane == wide - 1, 0.0, right)
            total = (here + total) + (load(number + 1, -1) + load(number + 1, 1)) + along * beside_z
            total = total + s.top.g[number, 0:high, 0:wide]
            edge = load(number + 1, -1, high, 8) + load(number + 1, 1, high, 8)
            first, last = left[:, :LANES], right[:, wide - LANES :]
            spot = lane[:, :LANES]
            side = along * (jnp.where(spot == 0, first, 0.0) + jnp.where(spot == LANES - 1, last, 0.0))
        side = jnp.concatenate([side, none[:8]], axis=0)
        value = jnp.concatenate([jnp.concatenate([total, edge], axis=0), side], axis=1)
        top.put(s.top.B, number + 1, value * s.top.m[top.zone(number)])


def kernel(plan, tree, density, dense, potential, *refs):
    held = jax.tree.unflatten(tree, refs)
    s = types.SimpleNamespace(**{key: named(value) for key, value in held.items()})
    counts, block, total = plan.counts, plan.block, plan.total
    top, wide, next_ = plan.top, plan.wide, plan.next
    place = tuple(lax.axis_index(axis) for axis in AXES)
    me = (place[0] * counts[1] + place[1]) * counts[2] + place[2]
    padded = block[2] != plan.width

    loads = [pltpu.make_async_copy(density, s.raw if padded else s.own, sem(s, OWN))]
    loads[0].start()
    if not padded:
        loads.append(
            pltpu.make_async_copy(
                density,
                s.field.at[pl.ds(8, block[0]), pl.ds(0, block[1]), pl.ds(0, block[2])],
                sem(s, FIELD),
            )
        )
    fill = pltpu.make_async_copy(dense, s.matrix, sem(s, MATRIX))

    for ref in s.land + [s.swap_land, s.swap_side]:
        ref[...] = jnp.zeros(ref.shape, F32)

    axes = [partners(place[axis], counts[axis]) for axis in range(3)]
    offsets = [
        (a, b, c) for a in range(counts[0]) for b in range(counts[1]) for c in range(counts[2]) if (a, b, c) != (0, 0, 0)
    ]
    offsets.sort(key=lambda off: -(off[0] + off[1] + off[2] / 2))

    def peer(off, way):
        target = tuple(axes[axis][off[axis]][way] for axis in range(3))
        return target, (target[0] * counts[1] + target[1]) * counts[2] + target[2]

    other = peer(offsets[0], 0)[0]
    barrier = pltpu.get_barrier_semaphore()
    for off in offsets:
        pl.semaphore_signal(barrier, inc=1, device_id=peer(off, 0)[0], device_id_type=MESH)

    for ref in [s.top.f, s.top.g] + s.top.R + s.top.B:
        ref[...] = jnp.zeros(ref.shape, F32)
    for v, grid in ((s.top, top), (s.wide, wide), (s.next, next_)):
        grid.guard(v)
        grid.masks(v, place, counts)
    for v, grid in zip(s.levels, plan.levels):
        grid.guard(v)
        grid.masks(v, (0, 0, 0), (1, 1, 1))
    loads[0].wait()
    for load in loads[1:] + [fill]:
        load.start()
    own = s.own
    if padded:
        own[...] = jnp.zeros(own.shape, F32)
        own[:, :, 0 : block[2]] = s.raw[...]

    even_own = parity_of(block[1], plan.width)
    for number in range(top.inner):
        one, two = own[2 * number], own[2 * number + 1]
        red = jnp.where(even_own, one, two)
        spot = number + top.margins[0]
        s.top.f[spot, 0 : block[1], 0 : plan.width] = red
        s.top.g[spot, 0 : block[1], 0 : plan.width] = jnp.where(even_own, two, one)
        for tile in range(plan.width // LANES):
            piece = red[:, tile * LANES : (tile + 1) * LANES] * inverse
            s.top.R[tile][spot + 1, 8 : 8 + block[1]] = piece
            s.top.R[tile][spot + 1, 8 + top.rows :] = piece[0:8]
    even_top = parity_of(top.rows, top.lanes)
    count = top.count
    if top.lanes == plan.width + LANES:
        first_black(plan, s, even_own)
    else:
        top.half(s.top, 1, even_top, 1, count - 1)
    top.half(s.top, 0, even_top, 1, count - 1)
    top.half(s.top, 1, even_top, 0, count)
    for number, value in top.residue(s.top, even_top, 0, count):
        for tile in range(plan.tiles):
            piece = value[:, tile * LANES : (tile + 1) * LANES]
            s.rows[tile][number, 0 : top.rows] = piece
            s.rows[tile][number, top.rows : top.rows + 8] = piece[block[1] :]
    flat = jnp.concatenate(
        [
            pair_sums(s.rows[tile], block[1] + 16, count).reshape(count * plan.high, LANES)
            for tile in range(plan.tiles)
        ],
        axis=1,
    )

    def fine_cell(shape, dim):
        index = iota(shape, dim)
        used = (index < block[2] + 4) | (index >= top.lanes - 4)
        cell = half_down(local_of(index, block[2], 4, top.lanes))
        return jnp.where(cell < 0, cell + LANES, cell), used

    shape = (top.lanes, LANES)
    cell, used = fine_cell(shape, 0)
    down = weights(shape, (cell == iota(shape, 1)) & used, 0.5)
    s.part[...] = dot(flat, down).reshape(count, plan.high, LANES)
    pack_part(plan, s)

    pl.semaphore_wait(barrier, total - 1)
    part = functools.partial(send_part, plan, s, place)
    far = functools.partial(send_far, plan, s, place)
    each(place, counts, part)

    lane = iota((block[1], LANES), 1)
    for side in range(2):
        begin = 0 if side == 0 else block[2] - 8
        tile = begin // LANES
        for pack in range(plan.far_packs):
            value = jnp.zeros((block[1], LANES), F32)
            for slot in range(16):
                plane = own[16 * pack + slot, :, tile * LANES : (tile + 1) * LANES]
                moved = pltpu.roll(plane, (8 * slot - begin) % LANES, 1)
                value = jnp.where(lane // 8 == slot, moved, value)
            s.far[side, pack] = value
    each(place, counts, far)
    field, far_land = s.field, s.far_land
    if padded:
        field[8 : 8 + block[0], 0 : block[1], 0 : plan.width] = own[...]
    for dim, step in ((0, -1), (0, 1), (1, -1), (1, 1), (2, -1), (2, 1)):
        steps = tuple(step if which == dim else 0 for which in range(3))

        @pl.when(jnp.logical_not(exists(place, steps, counts)))
        def _():
            if dim == 0:
                begin = 0 if step < 0 else 8 + block[0]
                field[begin : begin + 8] = jnp.zeros((8,) + field.shape[1:], F32)
                pack = 0 if step < 0 else plan.far_packs + 1
                far_land[:, pack] = jnp.zeros((2,) + far_land.shape[2:], F32)
            if dim == 1:
                begin = block[1] if step > 0 else block[1] + 8
                field[:, begin : begin + 8] = jnp.zeros((field.shape[0], 8, field.shape[2]), F32)
                far_land[:, :, begin : begin + 8] = jnp.zeros(far_land.shape[:2] + (8, LANES), F32)
            if dim == 2:
                far_land[(1 - step) // 2] = jnp.zeros(far_land.shape[1:], F32)

    wait_all(plan, s, place, size_part, PART + 1, other)
    gather_part(plan, s)
    even_next = parity_of(next_.rows, LANES)
    n = next_.count
    next_.first(s.next, 0, n)
    next_.half(s.next, 1, even_next, 1, n - 1)
    next_.half(s.next, 0, even_next, 2, n - 2)
    next_.half(s.next, 1, even_next, 2, n - 2)
    pairs = s.pairs
    rows1 = plan.block1[1]
    height = max(rows1, 16)
    if rows1 < height:
        pairs[0 : next_.inner, rows1:height] = jnp.zeros((next_.inner, height - rows1, LANES), F32)
    for number, value in next_.residue(s.next, even_next, 3, n - 3):
        pairs[number - 3, 0:rows1] = value[0:rows1]
    flat = pair_sums(pairs, height, next_.inner).reshape(next_.inner * (height // 2), LANES)
    row, column = iota((LANES, LANES), 0), iota((LANES, LANES), 1)
    down = weights((LANES, LANES), (row // 2 == column) & (row < plan.block1[2]), 0.5)
    below = dot(flat, down).reshape(next_.inner, height // 2, LANES)
    length = plan.block2
    per = LANES // length[2]
    packed = jnp.zeros((8, LANES), F32)
    for plane in range(length[0]):
        moved = below[plane]
        if plane // per:
            moved = pltpu.roll(moved, length[1] * (plane // per), 0)
        if plane % per:
            moved = pltpu.roll(moved, length[2] * (plane % per), 1)
        packed = packed + moved
    s.mine[...] = packed
    slots = s.slots
    slots[me] = packed

    def send(number, slot):
        return pltpu.make_async_remote_copy(
            src_ref=s.mine,
            dst_ref=slots.at[slot],
            send_sem=sem(s, ALL),
            recv_sem=sem(s, ALL + 1),
            device_id=peer(offsets[number], 0)[0],
            device_id_type=MESH,
        )

    def start_sends():
        for number in range(total - 1):
            send(number, me).start()

    start_sends()
    swap = functools.partial(send_swap, plan, s, place)
    pack_swap(plan, s)
    each(place, counts, swap)

    def finish_sends():
        for name in (ALL + 1, ALL):
            pltpu.make_async_remote_copy(
                src_ref=s.bytes.at[pl.ds(0, total - 1)],
                dst_ref=s.bytes.at[pl.ds(0, total - 1)],
                send_sem=sem(s, name),
                recv_sem=sem(s, name),
                device_id=other,
                device_id_type=MESH,
            ).wait_recv()

    wait_all(plan, s, place, size_far, FAR + 1, other)
    if not padded:
        loads[1].wait()
    base = wide.lanes - LANES
    shape = (wide.rows, LANES)
    lane = iota(shape, 1)
    even_wide = parity_of(wide.rows, wide.lanes)
    above = block[2] - base

    def wide_plane(number):
        pack, slot = (number + 8) // 16, (number + 8) % 16
        high = pltpu.roll(far_land[0, pack], (above - 8 * slot) % LANES, 1)
        low = pltpu.roll(far_land[1, pack], (LANES - 8 - 8 * slot) % LANES, 1)
        old = field[number, :, 0:LANES] if base == 0 else 0.0
        value = jnp.where((lane >= above) & (lane < above + 8), high, old)
        value = jnp.where(lane >= LANES - 8, low, value)
        return value if base == 0 else jnp.concatenate([field[number, :, 0:base], value], axis=1)

    for number in range(wide.count):
        one, two = wide_plane(2 * number), wide_plane(2 * number + 1)
        s.wide.f[number] = jnp.where(even_wide, one, two)
        s.wide.g[number] = jnp.where(even_wide, two, one)
    n = wide.count
    wide.first(s.wide, 0, n)
    wide.half(s.wide, 1, even_wide, 1, n - 1)
    wide.half(s.wide, 0, even_wide, 1, n - 1)
    wide.half(s.wide, 1, even_wide, 2, n - 2)
    wider = iota((8, wide.lanes), 0) < 4

    def narrow(value):
        both = jnp.where(wider, value[block[1] : block[1] + 8], value[block[1] + 8 :])
        value = jnp.concatenate([value[: block[1]], both], axis=0)
        if top.lanes != wide.lanes:
            value = jnp.concatenate([value[:, : top.lanes - LANES], value[:, -LANES:]], axis=1)
        return value

    shift = wide.margins[0] - top.margins[0]
    for number in range(count):
        s.top.f[number] = narrow(s.wide.f[number + shift])
        s.top.g[number] = narrow(s.wide.g[number + shift])
        top.put(s.top.B, number + 1, narrow(wide.get(s.wide.B, number + shift + 1)))

    finish_sends()
    fill.wait()
    lane = iota((8, LANES), 1)
    whole = s.whole
    first = plan.levels[0]

    def place_x(which):
        for second in range(counts[1]):
            start = (which * counts[1] + second) * counts[2]
            tiles = [slots[start + third] for third in range(counts[2])]
            for spot in range(per):
                value = jnp.zeros((8, LANES), F32)
                for third in range(counts[2]):
                    turn = (length[2] * (third - spot)) % LANES
                    moved = pltpu.roll(tiles[third], turn, 1) if turn else tiles[third]
                    value = jnp.where(lane // length[2] == third, moved, value)
                for group in range(8 // length[1]):
                    plane = which * length[0] + group * per + spot
                    whole[plane, second * length[1] : (second + 1) * length[1], :] = value[
                        group * length[1] : (group + 1) * length[1]
                    ]

    for which in range(counts[0]):
        place_x(which)
    even_first = parity_of(first.rows, LANES)
    for number in range(first.count):
        one, two = whole[2 * number], whole[2 * number + 1]
        s.levels[0].f[number] = jnp.where(even_first, one, two)
        s.levels[0].g[number] = jnp.where(even_first, two, one)
    solve(plan, s, 0)
    solved = s.solved
    for number in range(3):
        solved[number] = jnp.zeros((first.rows, LANES), F32)
        solved[first.block[0] + 3 + number] = jnp.zeros((first.rows, LANES), F32)
    for plane in range(first.block[0]):
        solved[plane + 3] = first.planes(s.levels[0], even_first, plane)

    wait_all(plan, s, place, size_swap, SWAP + 1, other)
    wait_all(plan, s, place, size_swap, SWAP, other)
    shape = (LANES, LANES)
    index = iota(shape, 1)
    spot = local_of(index, plan.block1[2], 8, LANES)
    used = (index < plan.block1[2] + 8) | (index >= LANES - 8)
    lanes_to = weights(shape, (half_down(spot) + place[2] * length[2] == iota(shape, 0)) & used, 1.0)
    n = next_.count
    flat = jnp.concatenate([solved[place[0] * length[0] + number] for number in range(n)], axis=0)
    flat = dot(flat, lanes_to).reshape(n, first.rows, LANES)
    spread = s.spread
    spread[:, 0:16] = jnp.zeros((n, 16, LANES), F32)
    spread[:, 16 + 2 * first.rows :] = jnp.zeros((n, 16, LANES), F32)
    spread[0:n, pl.ds(16, first.rows, stride=2), :] = flat
    spread[0:n, pl.ds(17, first.rows, stride=2), :] = flat
    start = 16 + place[1] * rows1
    for number in range(n):
        tiles = [
            spread[number, pl.ds(pl.multiple_of(start + shift, 8), size), :]
            for shift, size in ((0, rows1), (rows1, 8), (-8, 8))
        ]
        next_.put(s.next.B, number + 1, swapped(plan, s, number) + jnp.concatenate(tiles, axis=0))
    for colour, skip in ((0, 0), (1, 1), (0, 1), (1, 2)):
        next_.half(s.next, colour, even_next, skip, n - skip)

    pick = iota((8, LANES), 0) < 4
    planes = []
    for number in range(count):
        value = next_.planes(s.next, even_next, number + 2 * next_.margins[0] - top.margins[0])
        edge = jnp.where(pick, value[rows1 : rows1 + 8], value[rows1 + 8 :])
        planes.append(jnp.concatenate([value[:rows1], edge], axis=0))
    shape = (LANES, top.lanes)
    cell, used = fine_cell(shape, 1)
    spreading = weights(shape, (cell == iota(shape, 0)) & used, 1.0)
    flat = dot(jnp.concatenate(planes, axis=0), spreading).reshape(count, plan.high, top.lanes)
    for tile in range(plan.tiles):
        piece = flat[:, :, tile * LANES : (tile + 1) * LANES]
        s.rows[tile][0:count, pl.ds(0, plan.high, stride=2), :] = piece
        s.rows[tile][0:count, pl.ds(1, plan.high, stride=2), :] = piece
    for number in range(count):
        tiles = []
        for tile in range(plan.tiles):
            rows = s.rows[tile]
            edge = jnp.where(pick, rows[number, block[1] : block[1] + 8], rows[number, block[1] + 8 : block[1] + 16])
            tiles.append(jnp.concatenate([rows[number, 0 : block[1]], edge], axis=0))
        top.put(s.top.B, number + 1, top.get(s.top.B, number + 1) + jnp.concatenate(tiles, axis=1))
    top.half(s.top, 0, even_top, 0, count)
    top.half(s.top, 1, even_top, 1, count - 1)
    top.half(s.top, 0, even_top, 1, count - 1)
    red = s.top.R
    even_out = parity_of(block[1], block[2])
    for number, value in top.totals(red, even_top, 1, top.margins[0], count - top.margins[0]):
        black = ((s.top.g[number] + value) * inverse)[0 : block[1], 0 : block[2]]
        old = top.get(red, number + 1)[0 : block[1], 0 : block[2]]
        plane = 2 * (number - top.margins[0])
        potential[plane] = jnp.where(even_out, old, black)
        potential[plane + 1] = jnp.where(even_out, black, old)
    wait_all(plan, s, place, size_part, PART, other)
    wait_all(plan, s, place, size_far, FAR, other)


def cycle_matrix(size, depth):
    def beside_sum(v):
        p = np.pad(v, ((0, 0), (1, 1), (1, 1), (1, 1)))
        total = p[:, 2:, 1:-1, 1:-1] + p[:, :-2, 1:-1, 1:-1] + p[:, 1:-1, 2:, 1:-1] + p[:, 1:-1, :-2, 1:-1]
        return total + along * (p[:, 1:-1, 1:-1, 2:] + p[:, 1:-1, 1:-1, :-2])

    def cycle(g, left):
        parity = np.indices(g.shape[1:]).sum(0) % 2

        def sweeps(v, number):
            for _ in range(number):
                for colour in (0, 1):
                    v = np.where(parity == colour, (g + beside_sum(v)) / centre, v)
            return v

        v = np.zeros_like(g)
        if left == 0:
            return sweeps(v, CSWEEPS)
        v = sweeps(v, 2)
        r = g - centre * v + beside_sum(v)
        x, y, z = (part // 2 for part in g.shape[1:])
        coarse = 4 * r.reshape(-1, x, 2, y, 2, z, 2).mean((2, 4, 6))
        e = cycle(coarse, left - 1)
        for dim in (1, 2, 3):
            e = np.repeat(e, 2, dim)
        return sweeps(v + e, 2)

    cells = size[0] * size[1] * size[2]
    found = cycle(np.eye(cells).reshape((cells,) + size), depth).reshape(cells, cells)
    parts = []
    for _ in range(3):
        parts.append(found.astype(np.float32).astype(jnp.bfloat16))
        found = found - parts[-1].astype(np.float64)
    return np.stack(parts)


def on_device(counts, density):
    plan = Plan(density.shape, counts)
    scratch, tree = jax.tree.flatten(plan.scratch())
    matrix = jnp.asarray(cycle_matrix(plan.dense, LEVELS - 1 - plan.dense_level))
    return pl.pallas_call(
        functools.partial(kernel, plan, tree),
        out_shape=jax.ShapeDtypeStruct(density.shape, F32),
        in_specs=[pl.BlockSpec(memory_space=pltpu.HBM)] * 2,
        out_specs=pl.BlockSpec(memory_space=pltpu.VMEM),
        scratch_shapes=scratch,
        compiler_params=pltpu.CompilerParams(
            collective_id=0, has_side_effects=True, vmem_limit_bytes=48 * 1024 * 1024
        ),
    )(
        pltpu.with_memory_space_constraint(density, pltpu.HBM),
        pltpu.with_memory_space_constraint(matrix, pltpu.HBM),
    )


def solution(mesh):
    counts = tuple(mesh.shape[axis] for axis in AXES)
    return jax.shard_map(
        functools.partial(on_device, counts),
        mesh=mesh,
        in_specs=(P("gx", "gy", "gz"),),
        out_specs=P("gx", "gy", "gz"),
        check_vma=False,
    )
```

```python
import functools
import types

import jax
import jax.numpy as jnp
import numpy as np
from jax import lax
from jax.experimental import pallas as pl
from jax.experimental.pallas import tpu as pltpu
from jax.sharding import PartitionSpec as P

LEVELS = 7
CSWEEPS = 4
DENSE = 512
rsd_beta = 0.5
centre = 4.0 + 2.0 * (1.0 + rsd_beta)
along = 1.0 + rsd_beta
inverse = 1.0 / centre
F32 = jnp.float32
BF16 = jnp.bfloat16
LANES = 128
AXES = ("gx", "gy", "gz")
MESH = pl.DeviceIdType.MESH
DIRECTIONS = [
    (dx, dy, dz) for dx in (-1, 0, 1) for dy in (-1, 0, 1) for dz in (-1, 0, 1) if (dx, dy, dz) != (0, 0, 0)
]


ALL, PART, FAR, SWAP, OWN, FIELD, MATRIX, PAIR = 0, 2, 4, 6, 8, 9, 10, 11


def up_to(value, unit):
    return -(-value // unit) * unit


def iota(shape, dim):
    return lax.broadcasted_iota(jnp.int32, shape, dim)


def pieces(value):
    high = value.astype(BF16)
    rest = value - high.astype(F32)
    middle = rest.astype(BF16)
    return high, middle, (rest - middle.astype(F32)).astype(BF16)


def product(left, right):
    return jnp.dot(left, right, preferred_element_type=F32)


def dot(value, chosen):
    chosen = chosen.astype(BF16)
    parts = [product(part, chosen) for part in pieces(value)]
    return parts[0] + (parts[1] + parts[2])


def local_of(index, length, margin, total):
    return jnp.where(index < total - margin, index, index - total)


def half_down(value):
    return jnp.where(value >= 0, lax.div(value, 2), -lax.div(1 - value, 2))


def parity_of(rows, lanes, step=1):
    return (iota((rows, lanes), 0) + iota((rows, lanes), 1) // step) % 2 == 0


def beside(below, here, above, down, up, even, colour, edge, step):
    lanes = here.shape[1]
    left, right = pltpu.roll(here, step, 1), pltpu.roll(here, lanes - step, 1)
    if edge is not None:
        if edge[1] * step == lanes:
            lane = iota(here.shape, 1)
            left = jnp.where(lane < step, 0.0, left)
            right = jnp.where(lane >= lanes - step, 0.0, right)
    other = jnp.where(even, below, above) if colour == 0 else jnp.where(even, above, below)
    return (here + other) + (down + up) + along * (left + right)


class Grid:
    def __init__(self, block, margins, edge=False, step=1):
        self.block, self.margins, self.step = block, margins, step
        self.inner = block[0] // 2
        self.count = self.inner + 2 * margins[0]
        self.rows = up_to(block[1] + 2 * margins[1], 8)
        self.lanes = up_to(block[2] + 2 * margins[2], LANES)
        self.edge = (block[1], block[2]) if edge else None
        self.tiles = self.lanes // LANES

    def scratch(self):
        field = (self.count + 2, self.rows + 16, LANES)
        source = (self.count, self.rows, self.lanes)
        return dict(
            R=[pltpu.VMEM(field, F32) for _ in range(self.tiles)],
            B=[pltpu.VMEM(field, F32) for _ in range(self.tiles)],
            f=pltpu.VMEM(source, F32),
            g=pltpu.VMEM(source, F32),
            m=pltpu.VMEM((3, self.rows, self.lanes), F32),
        )

    def zone(self, number):
        if number < self.margins[0]:
            return 0
        return 2 if number >= self.count - self.margins[0] else 1

    def guard(self, v):
        empty = jnp.zeros((self.rows + 16, LANES), F32)
        for ref in v.R + v.B:
            ref[0] = empty
            ref[self.count + 1] = empty
            if self.edge:
                ref[:, 0:8] = jnp.zeros((self.count + 2, 8, LANES), F32)
                ref[:, self.rows + 8 :] = jnp.zeros((self.count + 2, 8, LANES), F32)

    def get(self, field, number, shift=0):
        parts = [ref[number, 8 + shift : 8 + shift + self.rows] for ref in field]
        return parts[0] if len(parts) == 1 else jnp.concatenate(parts, axis=1)

    def put(self, field, number, value):
        for tile, ref in enumerate(field):
            piece = value[:, tile * LANES : (tile + 1) * LANES]
            ref[number, 8 : 8 + self.rows] = piece
            if not self.edge:
                ref[number, 0:8] = piece[self.rows - 8 :]
                ref[number, 8 + self.rows :] = piece[0:8]

    def masks(self, v, place, counts):
        inside = None
        shape = (self.rows, self.lanes)
        for dim in (1, 2):
            index = iota(shape, dim - 1)
            size = shape[dim - 1]
            if dim == 2 and self.step > 1:
                inside = inside & (index % self.step == 0) & (index < self.step * self.block[2])
                continue
            margin, length = self.margins[dim], self.block[dim]
            used = (index < length + margin) | (index >= size - margin)
            spot = local_of(index, length, margin, size) + place[dim] * length
            used = used & (spot >= 0) & (spot < length * counts[dim])
            inside = used if inside is None else inside & used
        value = jnp.where(inside, inverse, 0.0).astype(F32)
        v.m[1] = value
        if self.edge:
            for zone, shift in ((0, -self.step), (2, self.step)):
                spot = iota(shape, 1) + shift
                kept = (spot >= 0) & (spot < self.step * self.block[2]) & (iota(shape, 1) % self.step == 0)
                v.m[zone] = jnp.where(kept & (iota(shape, 0) < self.block[1]), inverse, 0.0).astype(F32)
        if self.margins[0]:
            low = jnp.where(place[0] > 0, 1.0, 0.0).astype(F32)
            high = jnp.where(place[0] < counts[0] - 1, 1.0, 0.0).astype(F32)
            v.m[0] = value * low
            v.m[2] = value * high

    def first(self, v, begin, end):
        for number in range(begin, end):
            self.put(v.R, number + 1, v.f[number] * v.m[self.zone(number)])

    def totals(self, other, even, colour, begin, end):
        before, here = self.get(other, begin), self.get(other, begin + 1)
        for number in range(begin, end):
            after = self.get(other, number + 2)
            down, up = self.get(other, number + 1, -1), self.get(other, number + 1, 1)
            yield number, beside(before, here, after, down, up, even, colour, self.edge, self.step)
            before, here = here, after

    def half(self, v, colour, even, begin, end):
        target, other = (v.R, v.B) if colour == 0 else (v.B, v.R)
        source = v.f if colour == 0 else v.g
        for number, total in self.totals(other, even, colour, begin, end):
            self.put(target, number + 1, (source[number] + total) * v.m[self.zone(number)])

    def pair(self, v, even):
        step, lanes = self.step, self.lanes
        lane = iota((self.rows, lanes), 1)
        sides = []
        for number in range(self.count):
            here = self.get(v.B, number + 1)
            other = jnp.where(even, self.get(v.B, number), self.get(v.B, number + 2))
            rows = self.get(v.B, number + 1, -1) + self.get(v.B, number + 1, 1)
            total = v.f[number] + ((here + other) + rows)
            left = jnp.where(lane < step, 0.0, pltpu.roll(here, step, 1))
            right = jnp.where(lane >= lanes - step, 0.0, pltpu.roll(here, lanes - step, 1))
            second = jnp.where(lane < 2 * step, 0.0, pltpu.roll(here, 2 * step, 1))
            third = jnp.where(lane >= lanes - 2 * step, 0.0, pltpu.roll(here, lanes - 2 * step, 1))
            self.put(v.R, number + 1, (total + along * (left + right)) * v.m[1])
            before = (pltpu.roll(total, step, 1) + along * (second + here)) * v.m[0]
            after = (pltpu.roll(total, lanes - step, 1) + along * (here + third)) * v.m[2]
            sides.append(before + after)
        for number in range(self.count):
            here = self.get(v.R, number + 1)
            other = jnp.where(even, self.get(v.R, number + 2), self.get(v.R, number))
            rows = self.get(v.R, number + 1, -1) + self.get(v.R, number + 1, 1)
            total = v.g[number] + ((here + other) + rows)
            self.put(v.B, number + 1, (total + along * sides[number]) * v.m[1])

    def residue(self, v, even, begin, end):
        for number, total in self.totals(v.B, even, 0, begin, end):
            yield number, v.f[number] - centre * self.get(v.R, number + 1) + total

    def planes(self, v, even, plane):
        red, black = self.get(v.R, plane // 2 + 1), self.get(v.B, plane // 2 + 1)
        return jnp.where(even, red, black) if plane % 2 == 0 else jnp.where(even, black, red)


def exists(place, steps, counts):
    found = None
    for which in range(3):
        if steps[which] == 0:
            continue
        other = place[which] + steps[which]
        here = (other >= 0) & (other < counts[which])
        found = here if found is None else found & here
    return found


def device(place, steps):
    return tuple(place[which] + steps[which] for which in range(3))


class Plan:
    def __init__(self, block, counts):
        self.counts, self.block = counts, block
        self.total = counts[0] * counts[1] * counts[2]
        self.block1 = tuple(size // 2 for size in block)
        self.block2 = tuple(size // 4 for size in block)
        self.top = Grid(block, (2, 4, 4))
        self.wide = Grid(block, (4, 8, 8))
        self.next = Grid(self.block1, (3, 8, 8))
        self.width = up_to(block[2], LANES)
        self.tiles = self.top.lanes // LANES
        self.count = self.top.count
        self.high = self.block1[1] + 8
        self.per = LANES // self.block1[2]
        self.side = 8 // self.per
        self.middle = (self.count - 16) // self.per
        self.vectors = 2 * self.side + self.middle + 1
        self.packs = 1 + (self.count > 16)
        self.far_packs = block[0] // 16
        assert block[0] % 16 == 0 and self.block1[1] % 8 == 0 and self.block2[2] <= LANES
        assert self.next.lanes == LANES and (self.count - 16) % self.per == 0 and 64 % self.block1[2] == 0
        self.levels = []
        size = tuple(block[which] * counts[which] // 4 for which in range(3))
        number = 2
        while size[0] * size[1] * size[2] > DENSE:
            self.levels.append(Grid(size, (0, 0, 0), edge=True, step=1 << len(self.levels)))
            assert self.levels[-1].lanes == LANES
            size = tuple(part // 2 for part in size)
            number += 1
        self.dense, self.dense_level = size, number

    def message(self, steps):
        dx, dy, dz = steps
        if dz == 0:
            begin, length = {0: (0, self.vectors), -1: (0, self.side + 1), 1: (self.side, self.side + 1)}[dx]
            if dy == 0:
                return ("part_t", (pl.ds(begin, length),), (length, self.high, LANES))
            return ("part_y", ((dy + 1) // 2, pl.ds(begin, length)), (length, 8, LANES))
        length = self.packs if dx == 0 else 1
        if dy == 0:
            return ("part_z", ((dz + 1) // 2, pl.ds(0, length)), (length, self.high, LANES))
        return (
            "part_zy", ((dz + 1) // 2, (dy + 1) // 2, pl.ds(0, length)), (length, 8, LANES),
        )

    def scratch(self):
        block = self.block
        s = types.SimpleNamespace(
            top=self.top.scratch(), wide=self.wide.scratch(), next=self.next.scratch(),
            levels=[grid.scratch() for grid in self.levels],
        )
        s.own = pltpu.VMEM((block[0], block[1], self.width), F32)
        if block[2] != self.width:
            s.raw = pltpu.VMEM(block, F32)
        s.field = pltpu.VMEM((block[0] + 16, block[1] + 16, self.wide.lanes), F32)
        s.rows = [pltpu.VMEM((self.count, block[1] + 16, LANES), F32) for _ in range(self.tiles)]
        s.part = pltpu.VMEM((self.count, self.high, LANES), F32)
        s.part_t = pltpu.VMEM((self.vectors, self.high, LANES), F32)
        s.part_y = pltpu.VMEM((2, self.vectors, 8, LANES), F32)
        s.part_z = pltpu.VMEM((2, self.packs, self.high, LANES), F32)
        s.part_zy = pltpu.VMEM((2, 2, self.packs, 8, LANES), F32)
        s.land = [pltpu.VMEM(self.message(steps)[2], F32) for steps in DIRECTIONS]
        s.sums, s.sumz = [], []
        wide_rows = self.block1[1] + 16
        for dx in (-1, 0, 1):
            length = self.vectors if dx == 0 else self.side + 1
            packs = self.packs if dx == 0 else 1
            s.sums.append(pltpu.VMEM((length, wide_rows, LANES), F32))
            s.sumz.append(pltpu.VMEM((2, packs, wide_rows, LANES), F32))
        s.far = pltpu.VMEM((2, self.far_packs, block[1], LANES), F32)
        s.far_land = pltpu.VMEM((2, self.far_packs + 2, block[1] + 16, LANES), F32)
        s.swap = pltpu.VMEM((2, self.block1[1], LANES), F32)
        s.swap_land = pltpu.VMEM((self.next.count, self.next.rows, LANES), F32)
        s.swap_side = pltpu.VMEM((2, 3, self.next.rows, LANES), F32)
        first = self.levels[0]
        coarse = [first] + self.levels[1:]
        s.pairs = pltpu.VMEM((max(g.block[0] for g in coarse + [self.next]), 2 * up_to(first.rows, 16), LANES), F32)
        s.solved = pltpu.VMEM((first.block[0] + 6, first.rows, LANES), F32)
        s.spread = pltpu.VMEM((self.next.count, 2 * first.rows + 32, LANES), F32)
        s.whole = pltpu.VMEM((first.block[0], first.rows, LANES), F32)
        s.mine = pltpu.VMEM((8, LANES), F32)
        s.slots = pltpu.VMEM((self.total, 8, LANES), F32)
        size = self.dense[0] * self.dense[1] * self.dense[2]
        s.matrix = pltpu.VMEM((3, size, size), BF16)
        most = max(sum(size(self, steps) for steps in DIRECTIONS) for size in (size_part, size_far, size_swap))
        s.bytes = pltpu.VMEM((max(most, self.total), 8, LANES), F32)
        s.sem = pltpu.SemaphoreType.DMA((PAIR + 2,))
        return vars(s)


def weights(shape, found, value):
    return jnp.where(found, value, 0.0).astype(F32).reshape(shape)


def pair_sums(s, height, count):
    even = s[0:count, pl.ds(0, height // 2, stride=2), :]
    return even + s[0:count, pl.ds(1, height // 2, stride=2), :]


def named(value):
    if isinstance(value, dict):
        return types.SimpleNamespace(**value)
    return [named(one) for one in value] if isinstance(value, list) else value


def sem(s, number):
    return s.sem.at[number]


def size_part(plan, steps):
    shape = plan.message(steps)[2]
    return shape[0] * shape[1] // 8


def size_far(plan, steps):
    rows = plan.block[1] // 8 if steps[1] == 0 else 1
    if steps[2]:
        return rows * (plan.far_packs if steps[0] == 0 else 1)
    return rows * (plan.block[0] if steps[0] == 0 else 8) * (plan.width // LANES)


def size_swap(plan, steps):
    rows = plan.block1[1] // 8 if steps[1] == 0 else 1
    return rows if steps[2] else rows * (plan.next.inner if steps[0] == 0 else plan.next.margins[0])


def wait_all(plan, s, place, size, name, other):
    counts = plan.counts
    beside_of = [
        jnp.where(place[axis] > 0, 1, 0) + jnp.where(place[axis] < counts[axis] - 1, 1, 0) for axis in range(3)
    ]
    choices = [{1: (0,), 2: (1,)}.get(count, (1, 2)) for count in counts]
    for x in choices[0]:
        for y in choices[1]:
            for z in choices[2]:
                number = 0
                for steps in DIRECTIONS:
                    many = [1 if step == 0 else (have if step > 0 else 0) for step, have in zip(steps, (x, y, z))]
                    if min(steps) >= 0:
                        number += many[0] * many[1] * many[2] * size(plan, steps)
                if number == 0:
                    continue
                found = (beside_of[0] == x) & (beside_of[1] == y) & (beside_of[2] == z)

                @pl.when(found)
                def _():
                    pltpu.make_async_remote_copy(
                        src_ref=s.bytes.at[pl.ds(0, number)],
                        dst_ref=s.bytes.at[pl.ds(0, number)],
                        send_sem=sem(s, name),
                        recv_sem=sem(s, name),
                        device_id=other,
                        device_id_type=MESH,
                    ).wait_recv()


def send_part(plan, s, place, number):
    steps = DIRECTIONS[number]
    name, index, _ = plan.message(steps)
    return pltpu.make_async_remote_copy(
        src_ref=getattr(s, name).at[index],
        dst_ref=s.land[number],
        send_sem=sem(s, PART),
        recv_sem=sem(s, PART + 1),
        device_id=device(place, steps),
        device_id_type=MESH,
    )


def send_far(plan, s, place, number):
    dx, dy, dz = steps = DIRECTIONS[number]
    block = plan.block
    rows = {0: (0, block[1], 0), 1: (block[1] - 8, 8, block[1] + 8), -1: (0, 8, block[1])}[dy]
    if dz == 0:
        planes = {0: (0, block[0], 8), 1: (block[0] - 8, 8, 0), -1: (0, 8, block[0] + 8)}[dx]
        source = s.own.at[pl.ds(planes[0], planes[1]), pl.ds(rows[0], rows[1]), :]
        target = s.field.at[pl.ds(planes[2], planes[1]), pl.ds(rows[2], rows[1]), pl.ds(0, plan.width)]
    else:
        side, last = (dz + 1) // 2, plan.far_packs - 1
        packs = {0: (0, last + 1, 1), 1: (last, 1, 0), -1: (0, 1, last + 2)}[dx]
        source = s.far.at[side, pl.ds(packs[0], packs[1]), pl.ds(rows[0], rows[1]), :]
        target = s.far_land.at[side, pl.ds(packs[2], packs[1]), pl.ds(rows[2], rows[1]), :]
    return pltpu.make_async_remote_copy(
        src_ref=source,
        dst_ref=target,
        send_sem=sem(s, FAR),
        recv_sem=sem(s, FAR + 1),
        device_id=device(place, steps),
        device_id_type=MESH,
    )


def send_swap(plan, s, place, number):
    dx, dy, dz = steps = DIRECTIONS[number]
    high, margin, inner = plan.block1[1], plan.next.margins[0], plan.next.inner
    rows = {0: (0, high, 0), 1: (high - 8, 8, high + 8), -1: (0, 8, high)}[dy]
    if dz == 0:
        planes = {0: (margin, inner, margin), 1: (inner, margin, 0), -1: (margin, margin, margin + inner)}[dx]
        source = s.next.B[0].at[pl.ds(1 + planes[0], planes[1]), pl.ds(8 + rows[0], rows[1]), :]
        target = s.swap_land.at[pl.ds(planes[2], planes[1]), pl.ds(rows[2], rows[1]), :]
    else:
        side = (dz + 1) // 2
        source = s.swap.at[side, pl.ds(rows[0], rows[1]), :]
        target = s.swap_side.at[side, 1 - dx, pl.ds(rows[2], rows[1]), :]
    return pltpu.make_async_remote_copy(
        src_ref=source,
        dst_ref=target,
        send_sem=sem(s, SWAP),
        recv_sem=sem(s, SWAP + 1),
        device_id=device(place, steps),
        device_id_type=MESH,
    )


def pack_swap(plan, s):
    length, margin = plan.block1[2], plan.next.margins[0]
    lane = iota((plan.block1[1], LANES), 1)
    for side in range(2):
        begin = 0 if side == 0 else length - 8
        value = jnp.zeros(lane.shape, F32)
        for slot in range(plan.next.inner):
            plane = s.next.B[0][1 + margin + slot, 8 : 8 + plan.block1[1], :]
            value = jnp.where(lane // 8 == slot, pltpu.roll(plane, (8 * slot - begin) % LANES, 1), value)
        s.swap[side] = value


def swapped(plan, s, number):
    length, rows = plan.block1[2], plan.block1[1]
    margin, inner = plan.next.margins[0], plan.next.inner
    lane = iota((plan.next.rows, LANES), 1)
    which = 0 if number < margin else (2 if number >= margin + inner else 1)
    slot = number - margin + (1 - which) * inner
    value = s.swap_land[number]
    if which == 1:
        value = jnp.concatenate([s.next.B[0][number + 1, 8 : 8 + rows, :], value[rows:]], axis=0)
    high = pltpu.roll(s.swap_side[0, which], (length - 8 * slot) % LANES, 1)
    low = pltpu.roll(s.swap_side[1, which], (LANES - 8 - 8 * slot) % LANES, 1)
    edge = jnp.where(lane < length + 8, high, jnp.where(lane >= LANES - 8, low, 0.0))
    return jnp.where(lane < length, value, edge)


def partners(place, count):
    if count & (count - 1):
        return [(lax.rem(place + off, count), lax.rem(place + count - off, count)) for off in range(count)]
    bits = [lax.rem(lax.div(place, 1 << bit), 2) for bit in range(count.bit_length() - 1)]
    out = []
    for off in range(count):
        value = jnp.int32(0)
        for bit, digit in enumerate(bits):
            value = value + ((1 - digit) if off >> bit & 1 else digit) * (1 << bit)
        out.append((value, value))
    return out


def each(place, counts, send):
    for number, steps in enumerate(DIRECTIONS):
        @pl.when(exists(place, steps, counts))
        def _():
            send(number).start()


def pack_part(plan, s):
    count, per, side, middle, rows = plan.count, plan.per, plan.side, plan.middle, plan.block1[1]
    length = plan.block1[2]
    part = s.part
    shape = (plan.high, LANES)
    lane = iota(shape, 1)
    sub = iota((8, LANES), 0)

    def pair_y(value):
        edge = value[rows:]
        minus = jnp.where(sub >= 6, edge, value[:8])
        return minus, jnp.where(sub < 2, edge, value[rows - 8 : rows])

    groups = [(0, 0, side), (side + 1, count - 8, side), (2 * side + 1, 8, middle)]
    for index, first, number in groups:
        for spot in range(number):
            value = part[first + spot]
            for which in range(1, per):
                moved = pltpu.roll(part[first + spot + which * number], which * length, 1)
                value = jnp.where(lane // length == which, moved, value)
            s.part_t[index + spot] = value
            minus, plus = pair_y(value)
            s.part_y[0, index + spot] = minus
            s.part_y[1, index + spot] = plus
    value = jnp.zeros(shape, F32)
    couple = lane // 2
    for number in range(count):
        low = pltpu.roll(part[number], 2 * number, 1)
        high = low if length == 64 else pltpu.roll(part[number], 64 - length + 2 * number, 1)
        value = jnp.where(couple == ((126 + 2 * number) % LANES) // 2, low, value)
        value = jnp.where(couple == 32 + number, high, value)
    s.part_t[side] = value
    minus, plus = pair_y(value)
    s.part_y[0, side] = minus
    s.part_y[1, side] = plus
    for which in range(2):
        begin = LANES - 2 if which == 0 else length - 6
        for pack in range(plan.packs):
            value = jnp.zeros(shape, F32)
            planes = list(range(8)) + list(range(count - 8, count)) if pack == 0 else list(range(8, count - 8))
            for slot, number in enumerate(planes):
                moved = pltpu.roll(part[number], (8 * slot - begin) % LANES, 1)
                value = jnp.where(lane // 8 == slot, moved, value)
            s.part_z[which, pack] = value
            minus, plus = pair_y(value)
            s.part_zy[which, 0, pack] = minus
            s.part_zy[which, 1, pack] = plus


def gather_part(plan, s):
    side, count, rows, per, length = plan.side, plan.count, plan.block1[1], plan.per, plan.block1[2]
    sub = iota((8, LANES), 0)
    land = {steps: s.land[number] for number, steps in enumerate(DIRECTIONS)}

    def assembled(own, plus, minus):
        edge = own[rows:]
        tiles = [own[8 * number : 8 * number + 8] for number in range(rows // 8)]
        tiles[0] = tiles[0] + jnp.where(sub < 2, minus, 0.0)
        tiles[-1] = tiles[-1] + jnp.where(sub >= 6, plus, 0.0)
        tiles.append(jnp.where(sub < 6, plus, 0.0) + jnp.where(sub < 2, edge, 0.0))
        tiles.append(jnp.where(sub >= 2, minus, 0.0) + jnp.where(sub >= 6, edge, 0.0))
        return jnp.concatenate(tiles, axis=0)

    for dx in (-1, 0, 1):
        own = s.part_t if dx == 0 else land[(dx, 0, 0)]
        for index in range(own.shape[0]):
            s.sums[dx + 1][index] = assembled(own[index], land[(dx, -1, 0)][index], land[(dx, 1, 0)][index])
        for which in range(2):
            dz = 2 * which - 1
            for pack in range(land[(dx, 0, dz)].shape[0]):
                s.sumz[dx + 1][which, pack] = assembled(
                    land[(dx, 0, dz)][pack], land[(dx, -1, dz)][pack], land[(dx, 1, dz)][pack]
                )

    shape = (rows + 16, LANES)
    lane = iota(shape, 1)
    at_low, at_high = lane >= LANES - 2, (lane == length) | (lane == length + 1)
    inner = lane < length
    above = (lane >= length - 2) & (lane < length + 6)
    below = (lane >= LANES - 6) | (lane < 2)
    even = parity_of(*shape)

    def turned(value, shift):
        shift = shift % LANES
        return pltpu.roll(value, shift, 1) if shift else value

    def plane_of(dx, number):
        if number < 8:
            index, slots, size, first = number, number, side, 0
            base = 0
        elif number >= count - 8:
            index, slots, size, first = number - (count - 8), 8 + number - (count - 8), side, count - 8
            base = side + 1
        else:
            index, slots, size, first = number - 8, number - 8, plan.middle, 8
            base = 2 * side + 1
        pack = 0 if number < 8 or number >= count - 8 else 1
        extra = side
        if dx == -1:
            base, extra = 0, side
        if dx == 1:
            base, extra = 1, 0
        total = s.sums[dx + 1]
        main = turned(total[base + index % size], -(index // size) * length)
        low = turned(total[extra], -2 * number)
        high = low if length == 64 else turned(total[extra], length - 64 - 2 * number)
        value = jnp.where(inner, main, jnp.where(at_low, low, jnp.where(at_high, high, 0.0)))
        far = s.sumz[dx + 1]
        from_above = turned(far[0, pack], length - 2 - 8 * slots)
        from_below = turned(far[1, pack], LANES - 6 - 8 * slots)
        return value + (jnp.where(above, from_above, 0.0) + jnp.where(below, from_below, 0.0))

    def plane(number):
        spot = number - 2 * plan.next.margins[0]
        total = None
        for dx, place in ((0, spot), (-1, spot - plan.block1[0]), (1, spot + plan.block1[0])):
            index = place + 2
            allowed = {0: (0, count), -1: (0, 8), 1: (count - 8, count)}[dx]
            if allowed[0] <= index < allowed[1]:
                value = plane_of(dx, index)
                total = value if total is None else total + value
        return total

    for number in range(plan.next.count):
        first, second = plane(2 * number), plane(2 * number + 1)
        s.next.f[number] = jnp.where(even, first, second)
        s.next.g[number] = jnp.where(even, second, first)


def solve(plan, s, number):
    grid, v = plan.levels[number], s.levels[number]
    even = parity_of(grid.rows, LANES, grid.step)
    count, step = grid.count, grid.step
    grid.first(v, 0, count)
    small = count * grid.rows <= 64

    def sweep():
        if small:
            grid.pair(v, even)
            return
        grid.half(v, 0, even, 0, count)
        grid.half(v, 1, even, 0, count)

    grid.half(v, 1, even, 0, count)
    sweep()
    pairs = s.pairs
    height = max(grid.rows, 16)
    if grid.rows < height:
        pairs[0:count, grid.rows : height] = jnp.zeros((count, height - grid.rows, LANES), F32)
    for spot, value in grid.residue(v, even, 0, count):
        if grid.rows > grid.block[1]:
            value = jnp.where(iota(value.shape, 0) < grid.block[1], value, 0.0)
        pairs[spot, 0 : grid.rows] = value
    sums = pair_sums(pairs, height, count)
    row, column = iota((LANES, LANES), 0), iota((LANES, LANES), 1)
    if number + 1 < len(plan.levels):
        below, under = plan.levels[number + 1], s.levels[number + 1]
        same = parity_of(below.rows, LANES, below.step)
        lane = iota((below.rows, LANES), 1)
        coarse = []
        for spot in range(count):
            value = sums[spot][: below.rows]
            value = 0.5 * (value + pltpu.roll(value, LANES - step, 1))
            coarse.append(jnp.where((lane % below.step == 0) & (lane < step * grid.block[2]), value, 0.0))
        for spot in range(below.count):
            one, two = coarse[2 * spot], coarse[2 * spot + 1]
            under.f[spot] = jnp.where(same, one, two)
            under.g[spot] = jnp.where(same, two, one)
        solve(plan, s, number + 1)
        for spot in range(count):
            plane = below.planes(under, same, spot)
            plane = plane + pltpu.roll(plane, step, 1)
            pairs[spot, pl.ds(0, below.rows, stride=2), :] = plane
            pairs[spot, pl.ds(1, below.rows, stride=2), :] = plane
        for spot in range(count):
            grid.put(v.B, spot + 1, grid.get(v.B, spot + 1) + pairs[spot, 0 : grid.rows])
    else:
        nx, ny, nz = plan.dense
        size = nx * ny * nz
        tall = height // 2
        flat = sums.reshape(count * (height // 2), LANES)
        down = weights((LANES, LANES), (row // (2 * step) == column % nz) & (row < step * grid.block[2]), 0.5)
        many = dot(flat, down).reshape(count, tall, LANES)
        wide = up_to(size, LANES) // LANES
        here, lane = iota((tall, LANES), 0), iota((tall, LANES), 1)
        parts = []
        for vector in range(wide):
            cell = (vector * LANES + lane) // nz
            total = jnp.zeros((tall, LANES), F32)
            for spot in range(nx):
                total = total + jnp.where((cell == spot * ny + here) & (here < ny), many[spot], 0.0)
            parts.append(total)
        left = jnp.concatenate(parts, axis=1)[:, :size]
        high, middle, low = pieces(left)
        stack = jnp.concatenate([high, middle, low], axis=0)
        matrix = s.matrix
        one = product(stack, matrix[0])
        two = product(stack[: 2 * tall], matrix[1])
        three = product(high, matrix[2])
        total = one[:tall] + ((one[tall : 2 * tall] + one[2 * tall :]) + ((two[:tall] + two[tall:]) + three))
        answer = jnp.sum(total, axis=0, keepdims=True)
        here, lane = iota((grid.rows, LANES), 0), iota((grid.rows, LANES), 1)
        planes = []
        for spot in range(nx):
            value = jnp.zeros((grid.rows, LANES), F32)
            for vector in range(wide):
                if (vector + 1) * LANES <= spot * ny * nz or vector * LANES >= (spot + 1) * ny * nz:
                    continue
                piece = jnp.broadcast_to(answer[:, vector * LANES : (vector + 1) * LANES], value.shape)
                cell = (vector * LANES + lane) // nz
                value = jnp.where(cell == spot * ny + here // 2, piece, value)
            planes.append(value)
        spread = weights(
            (LANES, LANES),
            (column // (2 * step) == row % nz) & (column < step * grid.block[2]) & (column % step == 0),
            1.0,
        )
        flat = dot(jnp.concatenate(planes, axis=0), spread).reshape(count, grid.rows, LANES)
        for spot in range(count):
            grid.put(v.B, spot + 1, grid.get(v.B, spot + 1) + flat[spot])
    sweep()
    sweep()


def first_black(plan, s, even):
    top, high, wide = plan.top, plan.block[1], plan.width
    lane = iota((high, wide), 1)
    none = jnp.zeros((high, LANES), F32)

    def load(number, shift=0, begin=0, size=high):
        parts = [ref[number, 8 + begin + shift : 8 + begin + shift + size] for ref in s.top.R[:-1]]
        return parts[0] if len(parts) == 1 else jnp.concatenate(parts, axis=1)

    for number in range(1, top.count - 1):
        total = jnp.where(even, load(number + 2), load(number))
        edge, side = jnp.zeros((8, wide), F32), none
        if top.zone(number) == 1:
            here = load(number + 1)
            left, right = pltpu.roll(here, 1, 1), pltpu.roll(here, wide - 1, 1)
            beside_z = jnp.where(lane == 0, 0.0, left) + jnp.where(lane == wide - 1, 0.0, right)
            total = (here + total) + (load(number + 1, -1) + load(number + 1, 1)) + along * beside_z
            total = total + s.top.g[number, 0:high, 0:wide]
            edge = load(number + 1, -1, high, 8) + load(number + 1, 1, high, 8)
            first, last = left[:, :LANES], right[:, wide - LANES :]
            spot = lane[:, :LANES]
            side = along * (jnp.where(spot == 0, first, 0.0) + jnp.where(spot == LANES - 1, last, 0.0))
        side = jnp.concatenate([side, none[:8]], axis=0)
        value = jnp.concatenate([jnp.concatenate([total, edge], axis=0), side], axis=1)
        top.put(s.top.B, number + 1, value * s.top.m[top.zone(number)])


def kernel(plan, tree, density, dense, potential, *refs):
    held = jax.tree.unflatten(tree, refs)
    s = types.SimpleNamespace(**{key: named(value) for key, value in held.items()})
    counts, block, total = plan.counts, plan.block, plan.total
    top, wide, next_ = plan.top, plan.wide, plan.next
    place = tuple(lax.axis_index(axis) for axis in AXES)
    paired = counts[2] % 2 == 0
    kinds = 2 if paired else 1

    def slot_of(x, y, z):
        kind, rest = (lax.rem(z, 2), lax.div(z, 2)) if paired and not isinstance(z, int) else (z % kinds, z // kinds)
        return kind * (total // kinds) + (x * counts[1] + y) * (counts[2] // kinds) + rest

    me = slot_of(*place)
    padded = block[2] != plan.width

    loads = [pltpu.make_async_copy(density, s.raw if padded else s.own, sem(s, OWN))]
    loads[0].start()
    if not padded:
        loads.append(
            pltpu.make_async_copy(
                density,
                s.field.at[pl.ds(8, block[0]), pl.ds(0, block[1]), pl.ds(0, block[2])],
                sem(s, FIELD),
            )
        )
    fill = pltpu.make_async_copy(dense, s.matrix, sem(s, MATRIX))

    for ref in s.land + [s.swap_land, s.swap_side]:
        ref[...] = jnp.zeros(ref.shape, F32)

    axes = [partners(place[axis], counts[axis]) for axis in range(3)]
    offsets = [
        (a, b, c) for a in range(counts[0]) for b in range(counts[1]) for c in range(counts[2]) if (a, b, c) != (0, 0, 0)
    ]
    offsets.sort(key=lambda off: -(off[0] + off[1] + off[2] / 2))

    def peer(off, way):
        target = tuple(axes[axis][off[axis]][way] for axis in range(3))
        return target, slot_of(*target)

    other = peer(offsets[0], 0)[0]
    barrier = pltpu.get_barrier_semaphore()
    for off in offsets:
        pl.semaphore_signal(barrier, inc=1, device_id=peer(off, 0)[0], device_id_type=MESH)

    for ref in [s.top.f, s.top.g] + s.top.R + s.top.B:
        ref[...] = jnp.zeros(ref.shape, F32)
    for v, grid in ((s.top, top), (s.wide, wide), (s.next, next_)):
        grid.guard(v)
        grid.masks(v, place, counts)
    for v, grid in zip(s.levels, plan.levels):
        grid.guard(v)
        grid.masks(v, (0, 0, 0), (1, 1, 1))
    loads[0].wait()
    for load in loads[1:] + [fill]:
        load.start()
    own = s.own
    if padded:
        own[...] = jnp.zeros(own.shape, F32)
        own[:, :, 0 : block[2]] = s.raw[...]

    even_own = parity_of(block[1], plan.width)
    for number in range(top.inner):
        one, two = own[2 * number], own[2 * number + 1]
        red = jnp.where(even_own, one, two)
        spot = number + top.margins[0]
        s.top.f[spot, 0 : block[1], 0 : plan.width] = red
        s.top.g[spot, 0 : block[1], 0 : plan.width] = jnp.where(even_own, two, one)
        for tile in range(plan.width // LANES):
            piece = red[:, tile * LANES : (tile + 1) * LANES] * inverse
            s.top.R[tile][spot + 1, 8 : 8 + block[1]] = piece
            s.top.R[tile][spot + 1, 8 + top.rows :] = piece[0:8]
    even_top = parity_of(top.rows, top.lanes)
    count = top.count
    if top.lanes == plan.width + LANES:
        first_black(plan, s, even_own)
    else:
        top.half(s.top, 1, even_top, 1, count - 1)
    top.half(s.top, 0, even_top, 1, count - 1)
    top.half(s.top, 1, even_top, 0, count)
    for number, value in top.residue(s.top, even_top, 0, count):
        for tile in range(plan.tiles):
            piece = value[:, tile * LANES : (tile + 1) * LANES]
            s.rows[tile][number, 0 : top.rows] = piece
            s.rows[tile][number, top.rows : top.rows + 8] = piece[block[1] :]
    flat = jnp.concatenate(
        [
            pair_sums(s.rows[tile], block[1] + 16, count).reshape(count * plan.high, LANES)
            for tile in range(plan.tiles)
        ],
        axis=1,
    )

    def fine_cell(shape, dim):
        index = iota(shape, dim)
        used = (index < block[2] + 4) | (index >= top.lanes - 4)
        cell = half_down(local_of(index, block[2], 4, top.lanes))
        return jnp.where(cell < 0, cell + LANES, cell), used

    shape = (top.lanes, LANES)
    cell, used = fine_cell(shape, 0)
    down = weights(shape, (cell == iota(shape, 1)) & used, 0.5)
    s.part[...] = dot(flat, down).reshape(count, plan.high, LANES)
    pack_part(plan, s)

    pl.semaphore_wait(barrier, total - 1)
    part = functools.partial(send_part, plan, s, place)
    far = functools.partial(send_far, plan, s, place)
    each(place, counts, part)

    lane = iota((block[1], LANES), 1)
    for side in range(2):
        begin = 0 if side == 0 else block[2] - 8
        tile = begin // LANES
        for pack in range(plan.far_packs):
            value = jnp.zeros((block[1], LANES), F32)
            for slot in range(16):
                plane = own[16 * pack + slot, :, tile * LANES : (tile + 1) * LANES]
                moved = pltpu.roll(plane, (8 * slot - begin) % LANES, 1)
                value = jnp.where(lane // 8 == slot, moved, value)
            s.far[side, pack] = value
    each(place, counts, far)
    field, far_land = s.field, s.far_land
    if padded:
        field[8 : 8 + block[0], 0 : block[1], 0 : plan.width] = own[...]
    for dim, step in ((0, -1), (0, 1), (1, -1), (1, 1), (2, -1), (2, 1)):
        steps = tuple(step if which == dim else 0 for which in range(3))

        @pl.when(jnp.logical_not(exists(place, steps, counts)))
        def _():
            if dim == 0:
                begin = 0 if step < 0 else 8 + block[0]
                field[begin : begin + 8] = jnp.zeros((8,) + field.shape[1:], F32)
                pack = 0 if step < 0 else plan.far_packs + 1
                far_land[:, pack] = jnp.zeros((2,) + far_land.shape[2:], F32)
            if dim == 1:
                begin = block[1] if step > 0 else block[1] + 8
                field[:, begin : begin + 8] = jnp.zeros((field.shape[0], 8, field.shape[2]), F32)
                far_land[:, :, begin : begin + 8] = jnp.zeros(far_land.shape[:2] + (8, LANES), F32)
            if dim == 2:
                far_land[(1 - step) // 2] = jnp.zeros(far_land.shape[1:], F32)

    wait_all(plan, s, place, size_part, PART + 1, other)
    gather_part(plan, s)
    even_next = parity_of(next_.rows, LANES)
    n = next_.count
    next_.first(s.next, 0, n)
    next_.half(s.next, 1, even_next, 1, n - 1)
    next_.half(s.next, 0, even_next, 2, n - 2)
    next_.half(s.next, 1, even_next, 2, n - 2)
    pairs = s.pairs
    rows1 = plan.block1[1]
    height = max(rows1, 16)
    if rows1 < height:
        pairs[0 : next_.inner, rows1:height] = jnp.zeros((next_.inner, height - rows1, LANES), F32)
    for number, value in next_.residue(s.next, even_next, 3, n - 3):
        pairs[number - 3, 0:rows1] = value[0:rows1]
    flat = pair_sums(pairs, height, next_.inner).reshape(next_.inner * (height // 2), LANES)
    row, column = iota((LANES, LANES), 0), iota((LANES, LANES), 1)
    down = weights((LANES, LANES), (row // 2 == column) & (row < plan.block1[2]), 0.5)
    below = dot(flat, down).reshape(next_.inner, height // 2, LANES)
    length = plan.block2
    per = LANES // length[2]
    packed = jnp.zeros((8, LANES), F32)
    for plane in range(length[0]):
        moved = below[plane]
        if plane // per:
            moved = pltpu.roll(moved, length[1] * (plane // per), 0)
        if plane % per:
            moved = pltpu.roll(moved, length[2] * (plane % per), 1)
        packed = packed + moved
    s.mine[...] = packed
    slots = s.slots
    slots[me] = packed

    def send(number, slot):
        return pltpu.make_async_remote_copy(
            src_ref=s.mine,
            dst_ref=slots.at[slot],
            send_sem=sem(s, ALL),
            recv_sem=sem(s, ALL + 1),
            device_id=peer(offsets[number], 0)[0],
            device_id_type=MESH,
        )

    chosen = [number for number, off in enumerate(offsets) if off[2] % kinds == 0]

    def start_sends():
        for number in chosen:
            send(number, me).start()

    def forward():
        half = total // 2
        kind = lax.rem(place[2], 2) * half
        return pltpu.make_async_remote_copy(
            src_ref=slots.at[pl.ds(kind, half)],
            dst_ref=slots.at[pl.ds(kind, half)],
            send_sem=sem(s, PAIR),
            recv_sem=sem(s, PAIR + 1),
            device_id=peer((0, 0, 1), 0)[0],
            device_id_type=MESH,
        )

    start_sends()
    swap = functools.partial(send_swap, plan, s, place)
    pack_swap(plan, s)
    each(place, counts, swap)

    def finish_sends():
        for name in (ALL + 1, ALL):
            pltpu.make_async_remote_copy(
                src_ref=s.bytes.at[pl.ds(0, len(chosen))],
                dst_ref=s.bytes.at[pl.ds(0, len(chosen))],
                send_sem=sem(s, name),
                recv_sem=sem(s, name),
                device_id=other,
                device_id_type=MESH,
            ).wait_recv()

    wait_all(plan, s, place, size_far, FAR + 1, other)
    if not padded:
        loads[1].wait()
    base = wide.lanes - LANES
    shape = (wide.rows, LANES)
    lane = iota(shape, 1)
    even_wide = parity_of(wide.rows, wide.lanes)
    above = block[2] - base

    def wide_plane(number):
        pack, slot = (number + 8) // 16, (number + 8) % 16
        high = pltpu.roll(far_land[0, pack], (above - 8 * slot) % LANES, 1)
        low = pltpu.roll(far_land[1, pack], (LANES - 8 - 8 * slot) % LANES, 1)
        old = field[number, :, 0:LANES] if base == 0 else 0.0
        value = jnp.where((lane >= above) & (lane < above + 8), high, old)
        value = jnp.where(lane >= LANES - 8, low, value)
        return value if base == 0 else jnp.concatenate([field[number, :, 0:base], value], axis=1)

    for number in range(wide.count):
        one, two = wide_plane(2 * number), wide_plane(2 * number + 1)
        s.wide.f[number] = jnp.where(even_wide, one, two)
        s.wide.g[number] = jnp.where(even_wide, two, one)
    n = wide.count
    wide.first(s.wide, 0, n)
    wide.half(s.wide, 1, even_wide, 1, n - 1)
    wide.half(s.wide, 0, even_wide, 1, n - 1)
    wide.half(s.wide, 1, even_wide, 2, n - 2)
    wider = iota((8, wide.lanes), 0) < 4

    def narrow(value):
        both = jnp.where(wider, value[block[1] : block[1] + 8], value[block[1] + 8 :])
        value = jnp.concatenate([value[: block[1]], both], axis=0)
        if top.lanes != wide.lanes:
            value = jnp.concatenate([value[:, : top.lanes - LANES], value[:, -LANES:]], axis=1)
        return value

    shift = wide.margins[0] - top.margins[0]
    for number in range(count):
        s.top.f[number] = narrow(s.wide.f[number + shift])
        s.top.g[number] = narrow(s.wide.g[number + shift])
        top.put(s.top.B, number + 1, narrow(wide.get(s.wide.B, number + shift + 1)))

    finish_sends()
    if paired:
        forward().start()
        forward().wait()
    fill.wait()
    lane = iota((8, LANES), 1)
    whole = s.whole
    first = plan.levels[0]

    def place_x(which):
        for second in range(counts[1]):
            tiles = [slots[slot_of(which, second, third)] for third in range(counts[2])]
            for spot in range(per):
                value = jnp.zeros((8, LANES), F32)
                for third in range(counts[2]):
                    turn = (length[2] * (third - spot)) % LANES
                    moved = pltpu.roll(tiles[third], turn, 1) if turn else tiles[third]
                    value = jnp.where(lane // length[2] == third, moved, value)
                for group in range(8 // length[1]):
                    plane = which * length[0] + group * per + spot
                    whole[plane, second * length[1] : (second + 1) * length[1], :] = value[
                        group * length[1] : (group + 1) * length[1]
                    ]

    for which in range(counts[0]):
        place_x(which)
    even_first = parity_of(first.rows, LANES)
    for number in range(first.count):
        one, two = whole[2 * number], whole[2 * number + 1]
        s.levels[0].f[number] = jnp.where(even_first, one, two)
        s.levels[0].g[number] = jnp.where(even_first, two, one)
    solve(plan, s, 0)
    solved = s.solved
    for number in range(3):
        solved[number] = jnp.zeros((first.rows, LANES), F32)
        solved[first.block[0] + 3 + number] = jnp.zeros((first.rows, LANES), F32)
    for plane in range(first.block[0]):
        solved[plane + 3] = first.planes(s.levels[0], even_first, plane)

    wait_all(plan, s, place, size_swap, SWAP + 1, other)
    wait_all(plan, s, place, size_swap, SWAP, other)
    shape = (LANES, LANES)
    index = iota(shape, 1)
    spot = local_of(index, plan.block1[2], 8, LANES)
    used = (index < plan.block1[2] + 8) | (index >= LANES - 8)
    lanes_to = weights(shape, (half_down(spot) + place[2] * length[2] == iota(shape, 0)) & used, 1.0)
    n = next_.count
    flat = jnp.concatenate([solved[place[0] * length[0] + number] for number in range(n)], axis=0)
    flat = dot(flat, lanes_to).reshape(n, first.rows, LANES)
    spread = s.spread
    spread[:, 0:16] = jnp.zeros((n, 16, LANES), F32)
    spread[:, 16 + 2 * first.rows :] = jnp.zeros((n, 16, LANES), F32)
    spread[0:n, pl.ds(16, first.rows, stride=2), :] = flat
    spread[0:n, pl.ds(17, first.rows, stride=2), :] = flat
    start = 16 + place[1] * rows1
    for number in range(n):
        tiles = [
            spread[number, pl.ds(pl.multiple_of(start + shift, 8), size), :]
            for shift, size in ((0, rows1), (rows1, 8), (-8, 8))
        ]
        next_.put(s.next.B, number + 1, swapped(plan, s, number) + jnp.concatenate(tiles, axis=0))
    for colour, skip in ((0, 0), (1, 1), (0, 1), (1, 2)):
        next_.half(s.next, colour, even_next, skip, n - skip)

    pick = iota((8, LANES), 0) < 4
    planes = []
    for number in range(count):
        value = next_.planes(s.next, even_next, number + 2 * next_.margins[0] - top.margins[0])
        edge = jnp.where(pick, value[rows1 : rows1 + 8], value[rows1 + 8 :])
        planes.append(jnp.concatenate([value[:rows1], edge], axis=0))
    shape = (LANES, top.lanes)
    cell, used = fine_cell(shape, 1)
    spreading = weights(shape, (cell == iota(shape, 0)) & used, 1.0)
    flat = dot(jnp.concatenate(planes, axis=0), spreading).reshape(count, plan.high, top.lanes)
    for tile in range(plan.tiles):
        piece = flat[:, :, tile * LANES : (tile + 1) * LANES]
        s.rows[tile][0:count, pl.ds(0, plan.high, stride=2), :] = piece
        s.rows[tile][0:count, pl.ds(1, plan.high, stride=2), :] = piece
    for number in range(count):
        tiles = []
        for tile in range(plan.tiles):
            rows = s.rows[tile]
            edge = jnp.where(pick, rows[number, block[1] : block[1] + 8], rows[number, block[1] + 8 : block[1] + 16])
            tiles.append(jnp.concatenate([rows[number, 0 : block[1]], edge], axis=0))
        top.put(s.top.B, number + 1, top.get(s.top.B, number + 1) + jnp.concatenate(tiles, axis=1))
    top.half(s.top, 0, even_top, 0, count)
    top.half(s.top, 1, even_top, 1, count - 1)
    top.half(s.top, 0, even_top, 1, count - 1)
    red = s.top.R
    even_out = parity_of(block[1], block[2])
    for number, value in top.totals(red, even_top, 1, top.margins[0], count - top.margins[0]):
        black = ((s.top.g[number] + value) * inverse)[0 : block[1], 0 : block[2]]
        old = top.get(red, number + 1)[0 : block[1], 0 : block[2]]
        plane = 2 * (number - top.margins[0])
        potential[plane] = jnp.where(even_out, old, black)
        potential[plane + 1] = jnp.where(even_out, black, old)
    wait_all(plan, s, place, size_part, PART, other)
    wait_all(plan, s, place, size_far, FAR, other)


def cycle_matrix(size, depth):
    def beside_sum(v):
        p = np.pad(v, ((0, 0), (1, 1), (1, 1), (1, 1)))
        total = p[:, 2:, 1:-1, 1:-1] + p[:, :-2, 1:-1, 1:-1] + p[:, 1:-1, 2:, 1:-1] + p[:, 1:-1, :-2, 1:-1]
        return total + along * (p[:, 1:-1, 1:-1, 2:] + p[:, 1:-1, 1:-1, :-2])

    def cycle(g, left):
        parity = np.indices(g.shape[1:]).sum(0) % 2

        def sweeps(v, number):
            for _ in range(number):
                for colour in (0, 1):
                    v = np.where(parity == colour, (g + beside_sum(v)) / centre, v)
            return v

        v = np.zeros_like(g)
        if left == 0:
            return sweeps(v, CSWEEPS)
        v = sweeps(v, 2)
        r = g - centre * v + beside_sum(v)
        x, y, z = (part // 2 for part in g.shape[1:])
        coarse = 4 * r.reshape(-1, x, 2, y, 2, z, 2).mean((2, 4, 6))
        e = cycle(coarse, left - 1)
        for dim in (1, 2, 3):
            e = np.repeat(e, 2, dim)
        return sweeps(v + e, 2)

    cells = size[0] * size[1] * size[2]
    found = cycle(np.eye(cells).reshape((cells,) + size), depth).reshape(cells, cells)
    parts = []
    for _ in range(3):
        parts.append(found.astype(np.float32).astype(jnp.bfloat16))
        found = found - parts[-1].astype(np.float64)
    return np.stack(parts)


def on_device(counts, density):
    plan = Plan(density.shape, counts)
    scratch, tree = jax.tree.flatten(plan.scratch())
    matrix = jnp.asarray(cycle_matrix(plan.dense, LEVELS - 1 - plan.dense_level))
    return pl.pallas_call(
        functools.partial(kernel, plan, tree),
        out_shape=jax.ShapeDtypeStruct(density.shape, F32),
        in_specs=[pl.BlockSpec(memory_space=pltpu.HBM)] * 2,
        out_specs=pl.BlockSpec(memory_space=pltpu.VMEM),
        scratch_shapes=scratch,
        compiler_params=pltpu.CompilerParams(
            collective_id=0, has_side_effects=True, vmem_limit_bytes=48 * 1024 * 1024
        ),
    )(
        pltpu.with_memory_space_constraint(density, pltpu.HBM),
        pltpu.with_memory_space_constraint(matrix, pltpu.HBM),
    )


def solution(mesh):
    counts = tuple(mesh.shape[axis] for axis in AXES)
    return jax.shard_map(
        functools.partial(on_device, counts),
        mesh=mesh,
        in_specs=(P("gx", "gy", "gz"),),
        out_specs=P("gx", "gy", "gz"),
        check_vma=False,
    )
```

```python
import functools
import types

import jax
import jax.numpy as jnp
import numpy as np
from jax import lax
from jax.experimental import pallas as pl
from jax.experimental.pallas import tpu as pltpu
from jax.sharding import PartitionSpec as P

LEVELS = 7
CSWEEPS = 4
DENSE = 512
rsd_beta = 0.5
centre = 4.0 + 2.0 * (1.0 + rsd_beta)
along = 1.0 + rsd_beta
inverse = 1.0 / centre
F32 = jnp.float32
BF16 = jnp.bfloat16
LANES = 128
AXES = ("gx", "gy", "gz")
MESH = pl.DeviceIdType.MESH
DIRECTIONS = [
    (dx, dy, dz) for dx in (-1, 0, 1) for dy in (-1, 0, 1) for dz in (-1, 0, 1) if (dx, dy, dz) != (0, 0, 0)
]


ALL, PART, FAR, SWAP, OWN, FIELD, MATRIX, PAIR = 0, 2, 4, 6, 8, 9, 10, 11


def up_to(value, unit):
    return -(-value // unit) * unit


def iota(shape, dim):
    return lax.broadcasted_iota(jnp.int32, shape, dim)


def pieces(value):
    high = value.astype(BF16)
    rest = value - high.astype(F32)
    middle = rest.astype(BF16)
    return high, middle, (rest - middle.astype(F32)).astype(BF16)


def product(left, right):
    return jnp.dot(left, right, preferred_element_type=F32)


def dot(value, chosen):
    chosen = chosen.astype(BF16)
    parts = [product(part, chosen) for part in pieces(value)]
    return parts[0] + (parts[1] + parts[2])


def local_of(index, length, margin, total):
    return jnp.where(index < total - margin, index, index - total)


def half_down(value):
    return jnp.where(value >= 0, lax.div(value, 2), -lax.div(1 - value, 2))


def parity_of(rows, lanes, step=1):
    return (iota((rows, lanes), 0) + iota((rows, lanes), 1) // step) % 2 == 0


def beside(below, here, above, down, up, even, colour, edge, step):
    lanes = here.shape[1]
    left, right = pltpu.roll(here, step, 1), pltpu.roll(here, lanes - step, 1)
    if edge is not None:
        if edge[1] * step == lanes:
            lane = iota(here.shape, 1)
            left = jnp.where(lane < step, 0.0, left)
            right = jnp.where(lane >= lanes - step, 0.0, right)
    other = jnp.where(even, below, above) if colour == 0 else jnp.where(even, above, below)
    return (here + other) + (down + up) + along * (left + right)


class Grid:
    def __init__(self, block, margins, edge=False, step=1):
        self.block, self.margins, self.step = block, margins, step
        self.inner = block[0] // 2
        self.count = self.inner + 2 * margins[0]
        self.rows = up_to(block[1] + 2 * margins[1], 8)
        self.lanes = up_to(block[2] + 2 * margins[2], LANES)
        self.edge = (block[1], block[2]) if edge else None
        self.tiles = self.lanes // LANES

    def scratch(self):
        field = (self.count + 2, self.rows + 16, LANES)
        source = (self.count, self.rows, self.lanes)
        return dict(
            R=[pltpu.VMEM(field, F32) for _ in range(self.tiles)],
            B=[pltpu.VMEM(field, F32) for _ in range(self.tiles)],
            f=pltpu.VMEM(source, F32),
            g=pltpu.VMEM(source, F32),
            m=pltpu.VMEM((3, self.rows, self.lanes), F32),
        )

    def zone(self, number):
        if number < self.margins[0]:
            return 0
        return 2 if number >= self.count - self.margins[0] else 1

    def guard(self, v):
        empty = jnp.zeros((self.rows + 16, LANES), F32)
        for ref in v.R + v.B:
            ref[0] = empty
            ref[self.count + 1] = empty
            if self.edge:
                ref[:, 0:8] = jnp.zeros((self.count + 2, 8, LANES), F32)
                ref[:, self.rows + 8 :] = jnp.zeros((self.count + 2, 8, LANES), F32)

    def get(self, field, number, shift=0):
        parts = [ref[number, 8 + shift : 8 + shift + self.rows] for ref in field]
        return parts[0] if len(parts) == 1 else jnp.concatenate(parts, axis=1)

    def put(self, field, number, value):
        for tile, ref in enumerate(field):
            piece = value[:, tile * LANES : (tile + 1) * LANES]
            ref[number, 8 : 8 + self.rows] = piece
            if not self.edge:
                ref[number, 0:8] = piece[self.rows - 8 :]
                ref[number, 8 + self.rows :] = piece[0:8]

    def masks(self, v, place, counts):
        inside = None
        shape = (self.rows, self.lanes)
        for dim in (1, 2):
            index = iota(shape, dim - 1)
            size = shape[dim - 1]
            if dim == 2 and self.step > 1:
                inside = inside & (index % self.step == 0) & (index < self.step * self.block[2])
                continue
            margin, length = self.margins[dim], self.block[dim]
            used = (index < length + margin) | (index >= size - margin)
            spot = local_of(index, length, margin, size) + place[dim] * length
            used = used & (spot >= 0) & (spot < length * counts[dim])
            inside = used if inside is None else inside & used
        value = jnp.where(inside, inverse, 0.0).astype(F32)
        v.m[1] = value
        if self.edge:
            for zone, shift in ((0, -self.step), (2, self.step)):
                spot = iota(shape, 1) + shift
                kept = (spot >= 0) & (spot < self.step * self.block[2]) & (iota(shape, 1) % self.step == 0)
                v.m[zone] = jnp.where(kept & (iota(shape, 0) < self.block[1]), inverse, 0.0).astype(F32)
        if self.margins[0]:
            low = jnp.where(place[0] > 0, 1.0, 0.0).astype(F32)
            high = jnp.where(place[0] < counts[0] - 1, 1.0, 0.0).astype(F32)
            v.m[0] = value * low
            v.m[2] = value * high

    def first(self, v, begin, end):
        for number in range(begin, end):
            self.put(v.R, number + 1, v.f[number] * v.m[self.zone(number)])

    def totals(self, other, even, colour, begin, end):
        before, here = self.get(other, begin), self.get(other, begin + 1)
        for number in range(begin, end):
            after = self.get(other, number + 2)
            down, up = self.get(other, number + 1, -1), self.get(other, number + 1, 1)
            yield number, beside(before, here, after, down, up, even, colour, self.edge, self.step)
            before, here = here, after

    def half(self, v, colour, even, begin, end):
        target, other = (v.R, v.B) if colour == 0 else (v.B, v.R)
        source = v.f if colour == 0 else v.g
        for number, total in self.totals(other, even, colour, begin, end):
            self.put(target, number + 1, (source[number] + total) * v.m[self.zone(number)])

    def pair(self, v, even):
        step, lanes = self.step, self.lanes
        lane = iota((self.rows, lanes), 1)
        sides = []
        for number in range(self.count):
            here = self.get(v.B, number + 1)
            other = jnp.where(even, self.get(v.B, number), self.get(v.B, number + 2))
            rows = self.get(v.B, number + 1, -1) + self.get(v.B, number + 1, 1)
            total = v.f[number] + ((here + other) + rows)
            left = jnp.where(lane < step, 0.0, pltpu.roll(here, step, 1))
            right = jnp.where(lane >= lanes - step, 0.0, pltpu.roll(here, lanes - step, 1))
            second = jnp.where(lane < 2 * step, 0.0, pltpu.roll(here, 2 * step, 1))
            third = jnp.where(lane >= lanes - 2 * step, 0.0, pltpu.roll(here, lanes - 2 * step, 1))
            self.put(v.R, number + 1, (total + along * (left + right)) * v.m[1])
            before = (pltpu.roll(total, step, 1) + along * (second + here)) * v.m[0]
            after = (pltpu.roll(total, lanes - step, 1) + along * (here + third)) * v.m[2]
            sides.append(before + after)
        for number in range(self.count):
            here = self.get(v.R, number + 1)
            other = jnp.where(even, self.get(v.R, number + 2), self.get(v.R, number))
            rows = self.get(v.R, number + 1, -1) + self.get(v.R, number + 1, 1)
            total = v.g[number] + ((here + other) + rows)
            self.put(v.B, number + 1, (total + along * sides[number]) * v.m[1])

    def residue(self, v, even, begin, end):
        for number, total in self.totals(v.B, even, 0, begin, end):
            yield number, v.f[number] - centre * self.get(v.R, number + 1) + total

    def planes(self, v, even, plane):
        red, black = self.get(v.R, plane // 2 + 1), self.get(v.B, plane // 2 + 1)
        return jnp.where(even, red, black) if plane % 2 == 0 else jnp.where(even, black, red)


def exists(place, steps, counts):
    found = None
    for which in range(3):
        if steps[which] == 0:
            continue
        other = place[which] + steps[which]
        here = (other >= 0) & (other < counts[which])
        found = here if found is None else found & here
    return found


def device(place, steps):
    return tuple(place[which] + steps[which] for which in range(3))


class Plan:
    def __init__(self, block, counts):
        self.counts, self.block = counts, block
        self.total = counts[0] * counts[1] * counts[2]
        self.block1 = tuple(size // 2 for size in block)
        self.block2 = tuple(size // 4 for size in block)
        self.top = Grid(block, (2, 4, 4))
        self.wide = Grid(block, (4, 8, 8))
        self.next = Grid(self.block1, (3, 8, 8))
        self.width = up_to(block[2], LANES)
        self.tiles = self.top.lanes // LANES
        self.count = self.top.count
        self.high = self.block1[1] + 8
        self.per = LANES // self.block1[2]
        self.side = 8 // self.per
        self.middle = (self.count - 16) // self.per
        self.vectors = 2 * self.side + self.middle + 1
        self.packs = 1 + (self.count > 16)
        self.far_packs = block[0] // 16
        assert block[0] % 16 == 0 and self.block1[1] % 8 == 0 and self.block2[2] <= LANES
        assert self.next.lanes == LANES and (self.count - 16) % self.per == 0 and 64 % self.block1[2] == 0
        self.levels = []
        size = tuple(block[which] * counts[which] // 4 for which in range(3))
        number = 2
        while size[0] * size[1] * size[2] > DENSE:
            self.levels.append(Grid(size, (0, 0, 0), edge=True, step=1 << len(self.levels)))
            assert self.levels[-1].lanes == LANES
            size = tuple(part // 2 for part in size)
            number += 1
        self.dense, self.dense_level = size, number

    def message(self, steps):
        dx, dy, dz = steps
        if dz == 0:
            begin, length = {0: (0, self.vectors), -1: (0, self.side + 1), 1: (self.side, self.side + 1)}[dx]
            if dy == 0:
                return ("part_t", (pl.ds(begin, length),), (length, self.high, LANES))
            return ("part_y", ((dy + 1) // 2, pl.ds(begin, length)), (length, 8, LANES))
        length = self.packs if dx == 0 else 1
        if dy == 0:
            return ("part_z", ((dz + 1) // 2, pl.ds(0, length)), (length, self.high, LANES))
        return (
            "part_zy", ((dz + 1) // 2, (dy + 1) // 2, pl.ds(0, length)), (length, 8, LANES),
        )

    def scratch(self):
        block = self.block
        s = types.SimpleNamespace(
            top=self.top.scratch(), wide=self.wide.scratch(), next=self.next.scratch(),
            levels=[grid.scratch() for grid in self.levels],
        )
        s.own = pltpu.VMEM((block[0], block[1], self.width), F32)
        if block[2] != self.width:
            s.raw = pltpu.VMEM(block, F32)
        s.field = pltpu.VMEM((block[0] + 16, block[1] + 16, self.wide.lanes), F32)
        s.rows = [pltpu.VMEM((self.count, block[1] + 16, LANES), F32) for _ in range(self.tiles)]
        s.part = pltpu.VMEM((self.count, self.high, LANES), F32)
        s.part_t = pltpu.VMEM((self.vectors, self.high, LANES), F32)
        s.part_y = pltpu.VMEM((2, self.vectors, 8, LANES), F32)
        s.part_z = pltpu.VMEM((2, self.packs, self.high, LANES), F32)
        s.part_zy = pltpu.VMEM((2, 2, self.packs, 8, LANES), F32)
        s.land = [pltpu.VMEM(self.message(steps)[2], F32) for steps in DIRECTIONS]
        s.sums, s.sumz = [], []
        wide_rows = self.block1[1] + 16
        for dx in (-1, 0, 1):
            length = self.vectors if dx == 0 else self.side + 1
            packs = self.packs if dx == 0 else 1
            s.sums.append(pltpu.VMEM((length, wide_rows, LANES), F32))
            s.sumz.append(pltpu.VMEM((2, packs, wide_rows, LANES), F32))
        s.far = pltpu.VMEM((2, self.far_packs, block[1], LANES), F32)
        s.far_land = pltpu.VMEM((2, self.far_packs + 2, block[1] + 16, LANES), F32)
        s.swap = pltpu.VMEM((2, self.block1[1], LANES), F32)
        s.swap_land = pltpu.VMEM((self.next.count, self.next.rows, LANES), F32)
        s.swap_side = pltpu.VMEM((2, 3, self.next.rows, LANES), F32)
        first = self.levels[0]
        coarse = [first] + self.levels[1:]
        s.pairs = pltpu.VMEM((max(g.block[0] for g in coarse + [self.next]), 2 * up_to(first.rows, 16), LANES), F32)
        s.solved = pltpu.VMEM((first.block[0] + 6, first.rows, LANES), F32)
        s.spread = pltpu.VMEM((self.next.count, 2 * first.rows + 32, LANES), F32)
        s.whole = pltpu.VMEM((first.block[0], first.rows, LANES), F32)
        s.mine = pltpu.VMEM((8, LANES), F32)
        s.slots = pltpu.VMEM((self.total, 8, LANES), F32)
        size = self.dense[0] * self.dense[1] * self.dense[2]
        s.matrix = pltpu.VMEM((3, size, size), BF16)
        most = max(sum(size(self, steps) for steps in DIRECTIONS) for size in (size_part, size_far, size_swap))
        s.bytes = pltpu.VMEM((max(most, self.total), 8, LANES), F32)
        s.sem = pltpu.SemaphoreType.DMA((PAIR + 2,))
        return vars(s)


def weights(shape, found, value):
    return jnp.where(found, value, 0.0).astype(F32).reshape(shape)


def pair_sums(s, height, count):
    even = s[0:count, pl.ds(0, height // 2, stride=2), :]
    return even + s[0:count, pl.ds(1, height // 2, stride=2), :]


def named(value):
    if isinstance(value, dict):
        return types.SimpleNamespace(**value)
    return [named(one) for one in value] if isinstance(value, list) else value


def sem(s, number):
    return s.sem.at[number]


def size_part(plan, steps):
    shape = plan.message(steps)[2]
    return shape[0] * shape[1] // 8


def size_far(plan, steps):
    rows = plan.block[1] // 8 if steps[1] == 0 else 1
    if steps[2]:
        return rows * (plan.far_packs if steps[0] == 0 else 1)
    return rows * (plan.block[0] if steps[0] == 0 else 8) * (plan.width // LANES)


def size_swap(plan, steps):
    rows = plan.block1[1] // 8 if steps[1] == 0 else 1
    return rows if steps[2] else rows * (plan.next.inner if steps[0] == 0 else plan.next.margins[0])


def wait_all(plan, s, place, size, name, other):
    counts = plan.counts
    beside_of = [
        jnp.where(place[axis] > 0, 1, 0) + jnp.where(place[axis] < counts[axis] - 1, 1, 0) for axis in range(3)
    ]
    choices = [{1: (0,), 2: (1,)}.get(count, (1, 2)) for count in counts]
    for x in choices[0]:
        for y in choices[1]:
            for z in choices[2]:
                number = 0
                for steps in DIRECTIONS:
                    many = [1 if step == 0 else (have if step > 0 else 0) for step, have in zip(steps, (x, y, z))]
                    if min(steps) >= 0:
                        number += many[0] * many[1] * many[2] * size(plan, steps)
                if number == 0:
                    continue
                found = (beside_of[0] == x) & (beside_of[1] == y) & (beside_of[2] == z)

                @pl.when(found)
                def _():
                    pltpu.make_async_remote_copy(
                        src_ref=s.bytes.at[pl.ds(0, number)],
                        dst_ref=s.bytes.at[pl.ds(0, number)],
                        send_sem=sem(s, name),
                        recv_sem=sem(s, name),
                        device_id=other,
                        device_id_type=MESH,
                    ).wait_recv()


def send_part(plan, s, place, number):
    steps = DIRECTIONS[number]
    name, index, _ = plan.message(steps)
    return pltpu.make_async_remote_copy(
        src_ref=getattr(s, name).at[index],
        dst_ref=s.land[number],
        send_sem=sem(s, PART),
        recv_sem=sem(s, PART + 1),
        device_id=device(place, steps),
        device_id_type=MESH,
    )


def send_far(plan, s, place, number):
    dx, dy, dz = steps = DIRECTIONS[number]
    block = plan.block
    rows = {0: (0, block[1], 0), 1: (block[1] - 8, 8, block[1] + 8), -1: (0, 8, block[1])}[dy]
    if dz == 0:
        planes = {0: (0, block[0], 8), 1: (block[0] - 8, 8, 0), -1: (0, 8, block[0] + 8)}[dx]
        source = s.own.at[pl.ds(planes[0], planes[1]), pl.ds(rows[0], rows[1]), :]
        target = s.field.at[pl.ds(planes[2], planes[1]), pl.ds(rows[2], rows[1]), pl.ds(0, plan.width)]
    else:
        side, last = (dz + 1) // 2, plan.far_packs - 1
        packs = {0: (0, last + 1, 1), 1: (last, 1, 0), -1: (0, 1, last + 2)}[dx]
        source = s.far.at[side, pl.ds(packs[0], packs[1]), pl.ds(rows[0], rows[1]), :]
        target = s.far_land.at[side, pl.ds(packs[2], packs[1]), pl.ds(rows[2], rows[1]), :]
    return pltpu.make_async_remote_copy(
        src_ref=source,
        dst_ref=target,
        send_sem=sem(s, FAR),
        recv_sem=sem(s, FAR + 1),
        device_id=device(place, steps),
        device_id_type=MESH,
    )


def send_swap(plan, s, place, number):
    dx, dy, dz = steps = DIRECTIONS[number]
    high, margin, inner = plan.block1[1], plan.next.margins[0], plan.next.inner
    rows = {0: (0, high, 0), 1: (high - 8, 8, high + 8), -1: (0, 8, high)}[dy]
    if dz == 0:
        planes = {0: (margin, inner, margin), 1: (inner, margin, 0), -1: (margin, margin, margin + inner)}[dx]
        source = s.next.B[0].at[pl.ds(1 + planes[0], planes[1]), pl.ds(8 + rows[0], rows[1]), :]
        target = s.swap_land.at[pl.ds(planes[2], planes[1]), pl.ds(rows[2], rows[1]), :]
    else:
        side = (dz + 1) // 2
        source = s.swap.at[side, pl.ds(rows[0], rows[1]), :]
        target = s.swap_side.at[side, 1 - dx, pl.ds(rows[2], rows[1]), :]
    return pltpu.make_async_remote_copy(
        src_ref=source,
        dst_ref=target,
        send_sem=sem(s, SWAP),
        recv_sem=sem(s, SWAP + 1),
        device_id=device(place, steps),
        device_id_type=MESH,
    )


def pack_swap(plan, s):
    length, margin = plan.block1[2], plan.next.margins[0]
    lane = iota((plan.block1[1], LANES), 1)
    for side in range(2):
        begin = 0 if side == 0 else length - 8
        value = jnp.zeros(lane.shape, F32)
        for slot in range(plan.next.inner):
            plane = s.next.B[0][1 + margin + slot, 8 : 8 + plan.block1[1], :]
            value = jnp.where(lane // 8 == slot, pltpu.roll(plane, (8 * slot - begin) % LANES, 1), value)
        s.swap[side] = value


def swapped(plan, s, number):
    length, rows = plan.block1[2], plan.block1[1]
    margin, inner = plan.next.margins[0], plan.next.inner
    lane = iota((plan.next.rows, LANES), 1)
    which = 0 if number < margin else (2 if number >= margin + inner else 1)
    slot = number - margin + (1 - which) * inner
    value = s.swap_land[number]
    if which == 1:
        value = jnp.concatenate([s.next.B[0][number + 1, 8 : 8 + rows, :], value[rows:]], axis=0)
    high = pltpu.roll(s.swap_side[0, which], (length - 8 * slot) % LANES, 1)
    low = pltpu.roll(s.swap_side[1, which], (LANES - 8 - 8 * slot) % LANES, 1)
    edge = jnp.where(lane < length + 8, high, jnp.where(lane >= LANES - 8, low, 0.0))
    return jnp.where(lane < length, value, edge)


def partners(place, count):
    if count & (count - 1):
        return [(lax.rem(place + off, count), lax.rem(place + count - off, count)) for off in range(count)]
    bits = [lax.rem(lax.div(place, 1 << bit), 2) for bit in range(count.bit_length() - 1)]
    out = []
    for off in range(count):
        value = jnp.int32(0)
        for bit, digit in enumerate(bits):
            value = value + ((1 - digit) if off >> bit & 1 else digit) * (1 << bit)
        out.append((value, value))
    return out


def each(place, counts, send):
    for number, steps in enumerate(DIRECTIONS):
        @pl.when(exists(place, steps, counts))
        def _():
            send(number).start()


def pack_part(plan, s):
    count, per, side, middle, rows = plan.count, plan.per, plan.side, plan.middle, plan.block1[1]
    length = plan.block1[2]
    part = s.part
    shape = (plan.high, LANES)
    lane = iota(shape, 1)
    sub = iota((8, LANES), 0)

    def pair_y(value):
        edge = value[rows:]
        minus = jnp.where(sub >= 6, edge, value[:8])
        return minus, jnp.where(sub < 2, edge, value[rows - 8 : rows])

    groups = [(0, 0, side), (side + 1, count - 8, side), (2 * side + 1, 8, middle)]
    for index, first, number in groups:
        for spot in range(number):
            value = part[first + spot]
            for which in range(1, per):
                moved = pltpu.roll(part[first + spot + which * number], which * length, 1)
                value = jnp.where(lane // length == which, moved, value)
            s.part_t[index + spot] = value
            minus, plus = pair_y(value)
            s.part_y[0, index + spot] = minus
            s.part_y[1, index + spot] = plus
    value = jnp.zeros(shape, F32)
    couple = lane // 2
    for number in range(count):
        low = pltpu.roll(part[number], 2 * number, 1)
        high = low if length == 64 else pltpu.roll(part[number], 64 - length + 2 * number, 1)
        value = jnp.where(couple == ((126 + 2 * number) % LANES) // 2, low, value)
        value = jnp.where(couple == 32 + number, high, value)
    s.part_t[side] = value
    minus, plus = pair_y(value)
    s.part_y[0, side] = minus
    s.part_y[1, side] = plus
    for which in range(2):
        begin = LANES - 2 if which == 0 else length - 6
        for pack in range(plan.packs):
            value = jnp.zeros(shape, F32)
            planes = list(range(8)) + list(range(count - 8, count)) if pack == 0 else list(range(8, count - 8))
            for slot, number in enumerate(planes):
                moved = pltpu.roll(part[number], (8 * slot - begin) % LANES, 1)
                value = jnp.where(lane // 8 == slot, moved, value)
            s.part_z[which, pack] = value
            minus, plus = pair_y(value)
            s.part_zy[which, 0, pack] = minus
            s.part_zy[which, 1, pack] = plus


def gather_part(plan, s):
    side, count, rows, per, length = plan.side, plan.count, plan.block1[1], plan.per, plan.block1[2]
    sub = iota((8, LANES), 0)
    land = {steps: s.land[number] for number, steps in enumerate(DIRECTIONS)}

    def assembled(own, plus, minus):
        edge = own[rows:]
        tiles = [own[8 * number : 8 * number + 8] for number in range(rows // 8)]
        tiles[0] = tiles[0] + jnp.where(sub < 2, minus, 0.0)
        tiles[-1] = tiles[-1] + jnp.where(sub >= 6, plus, 0.0)
        tiles.append(jnp.where(sub < 6, plus, 0.0) + jnp.where(sub < 2, edge, 0.0))
        tiles.append(jnp.where(sub >= 2, minus, 0.0) + jnp.where(sub >= 6, edge, 0.0))
        return jnp.concatenate(tiles, axis=0)

    for dx in (-1, 0, 1):
        own = s.part_t if dx == 0 else land[(dx, 0, 0)]
        for index in range(own.shape[0]):
            s.sums[dx + 1][index] = assembled(own[index], land[(dx, -1, 0)][index], land[(dx, 1, 0)][index])
        for which in range(2):
            dz = 2 * which - 1
            for pack in range(land[(dx, 0, dz)].shape[0]):
                s.sumz[dx + 1][which, pack] = assembled(
                    land[(dx, 0, dz)][pack], land[(dx, -1, dz)][pack], land[(dx, 1, dz)][pack]
                )

    shape = (rows + 16, LANES)
    lane = iota(shape, 1)
    at_low, at_high = lane >= LANES - 2, (lane == length) | (lane == length + 1)
    inner = lane < length
    above = (lane >= length - 2) & (lane < length + 6)
    below = (lane >= LANES - 6) | (lane < 2)
    even = parity_of(*shape)

    def turned(value, shift):
        shift = shift % LANES
        return pltpu.roll(value, shift, 1) if shift else value

    def plane_of(dx, number):
        if number < 8:
            index, slots, size, first = number, number, side, 0
            base = 0
        elif number >= count - 8:
            index, slots, size, first = number - (count - 8), 8 + number - (count - 8), side, count - 8
            base = side + 1
        else:
            index, slots, size, first = number - 8, number - 8, plan.middle, 8
            base = 2 * side + 1
        pack = 0 if number < 8 or number >= count - 8 else 1
        extra = side
        if dx == -1:
            base, extra = 0, side
        if dx == 1:
            base, extra = 1, 0
        total = s.sums[dx + 1]
        main = turned(total[base + index % size], -(index // size) * length)
        low = turned(total[extra], -2 * number)
        high = low if length == 64 else turned(total[extra], length - 64 - 2 * number)
        value = jnp.where(inner, main, jnp.where(at_low, low, jnp.where(at_high, high, 0.0)))
        far = s.sumz[dx + 1]
        from_above = turned(far[0, pack], length - 2 - 8 * slots)
        from_below = turned(far[1, pack], LANES - 6 - 8 * slots)
        return value + (jnp.where(above, from_above, 0.0) + jnp.where(below, from_below, 0.0))

    def plane(number):
        spot = number - 2 * plan.next.margins[0]
        total = None
        for dx, place in ((0, spot), (-1, spot - plan.block1[0]), (1, spot + plan.block1[0])):
            index = place + 2
            allowed = {0: (0, count), -1: (0, 8), 1: (count - 8, count)}[dx]
            if allowed[0] <= index < allowed[1]:
                value = plane_of(dx, index)
                total = value if total is None else total + value
        return total

    for number in range(plan.next.count):
        first, second = plane(2 * number), plane(2 * number + 1)
        s.next.f[number] = jnp.where(even, first, second)
        s.next.g[number] = jnp.where(even, second, first)


def solve(plan, s, number):
    grid, v = plan.levels[number], s.levels[number]
    even = parity_of(grid.rows, LANES, grid.step)
    count, step = grid.count, grid.step
    grid.first(v, 0, count)
    small = count * grid.rows <= 64

    def sweep():
        if small:
            grid.pair(v, even)
            return
        grid.half(v, 0, even, 0, count)
        grid.half(v, 1, even, 0, count)

    grid.half(v, 1, even, 0, count)
    sweep()
    pairs = s.pairs
    height = max(grid.rows, 16)
    if grid.rows < height:
        pairs[0:count, grid.rows : height] = jnp.zeros((count, height - grid.rows, LANES), F32)
    for spot, value in grid.residue(v, even, 0, count):
        if grid.rows > grid.block[1]:
            value = jnp.where(iota(value.shape, 0) < grid.block[1], value, 0.0)
        pairs[spot, 0 : grid.rows] = value
    sums = pair_sums(pairs, height, count)
    row, column = iota((LANES, LANES), 0), iota((LANES, LANES), 1)
    if number + 1 < len(plan.levels):
        below, under = plan.levels[number + 1], s.levels[number + 1]
        same = parity_of(below.rows, LANES, below.step)
        lane = iota((below.rows, LANES), 1)
        coarse = []
        for spot in range(count):
            value = sums[spot][: below.rows]
            value = 0.5 * (value + pltpu.roll(value, LANES - step, 1))
            coarse.append(jnp.where((lane % below.step == 0) & (lane < step * grid.block[2]), value, 0.0))
        for spot in range(below.count):
            one, two = coarse[2 * spot], coarse[2 * spot + 1]
            under.f[spot] = jnp.where(same, one, two)
            under.g[spot] = jnp.where(same, two, one)
        solve(plan, s, number + 1)
        for spot in range(count):
            plane = below.planes(under, same, spot)
            plane = plane + pltpu.roll(plane, step, 1)
            pairs[spot, pl.ds(0, below.rows, stride=2), :] = plane
            pairs[spot, pl.ds(1, below.rows, stride=2), :] = plane
        for spot in range(count):
            grid.put(v.B, spot + 1, grid.get(v.B, spot + 1) + pairs[spot, 0 : grid.rows])
    else:
        nx, ny, nz = plan.dense
        size = nx * ny * nz
        tall = height // 2
        flat = sums.reshape(count * (height // 2), LANES)
        down = weights((LANES, LANES), (row // (2 * step) == column % nz) & (row < step * grid.block[2]), 0.5)
        many = dot(flat, down).reshape(count, tall, LANES)
        wide = up_to(size, LANES) // LANES
        here, lane = iota((tall, LANES), 0), iota((tall, LANES), 1)
        parts = []
        for vector in range(wide):
            cell = (vector * LANES + lane) // nz
            total = jnp.zeros((tall, LANES), F32)
            for spot in range(nx):
                total = total + jnp.where((cell == spot * ny + here) & (here < ny), many[spot], 0.0)
            parts.append(total)
        left = jnp.concatenate(parts, axis=1)[:, :size]
        high, middle, low = pieces(left)
        stack = jnp.concatenate([high, middle, low], axis=0)
        matrix = s.matrix
        one = product(stack, matrix[0])
        two = product(stack[: 2 * tall], matrix[1])
        three = product(high, matrix[2])
        total = one[:tall] + ((one[tall : 2 * tall] + one[2 * tall :]) + ((two[:tall] + two[tall:]) + three))
        answer = jnp.sum(total, axis=0, keepdims=True)
        here, lane = iota((grid.rows, LANES), 0), iota((grid.rows, LANES), 1)
        planes = []
        for spot in range(nx):
            value = jnp.zeros((grid.rows, LANES), F32)
            for vector in range(wide):
                if (vector + 1) * LANES <= spot * ny * nz or vector * LANES >= (spot + 1) * ny * nz:
                    continue
                piece = jnp.broadcast_to(answer[:, vector * LANES : (vector + 1) * LANES], value.shape)
                cell = (vector * LANES + lane) // nz
                value = jnp.where(cell == spot * ny + here // 2, piece, value)
            planes.append(value)
        spread = weights(
            (LANES, LANES),
            (column // (2 * step) == row % nz) & (column < step * grid.block[2]) & (column % step == 0),
            1.0,
        )
        flat = dot(jnp.concatenate(planes, axis=0), spread).reshape(count, grid.rows, LANES)
        for spot in range(count):
            grid.put(v.B, spot + 1, grid.get(v.B, spot + 1) + flat[spot])
    sweep()
    sweep()


def first_black(plan, s, even):
    top, high, wide = plan.top, plan.block[1], plan.width
    lane = iota((high, wide), 1)
    none = jnp.zeros((high, LANES), F32)

    def load(number, shift=0, begin=0, size=high):
        parts = [ref[number, 8 + begin + shift : 8 + begin + shift + size] for ref in s.top.R[:-1]]
        return parts[0] if len(parts) == 1 else jnp.concatenate(parts, axis=1)

    for number in range(1, top.count - 1):
        total = jnp.where(even, load(number + 2), load(number))
        edge, side = jnp.zeros((8, wide), F32), none
        if top.zone(number) == 1:
            here = load(number + 1)
            left, right = pltpu.roll(here, 1, 1), pltpu.roll(here, wide - 1, 1)
            beside_z = jnp.where(lane == 0, 0.0, left) + jnp.where(lane == wide - 1, 0.0, right)
            total = (here + total) + (load(number + 1, -1) + load(number + 1, 1)) + along * beside_z
            total = total + s.top.g[number, 0:high, 0:wide]
            edge = load(number + 1, -1, high, 8) + load(number + 1, 1, high, 8)
            first, last = left[:, :LANES], right[:, wide - LANES :]
            spot = lane[:, :LANES]
            side = along * (jnp.where(spot == 0, first, 0.0) + jnp.where(spot == LANES - 1, last, 0.0))
        side = jnp.concatenate([side, none[:8]], axis=0)
        value = jnp.concatenate([jnp.concatenate([total, edge], axis=0), side], axis=1)
        top.put(s.top.B, number + 1, value * s.top.m[top.zone(number)])


def kernel(plan, tree, density, dense, potential, *refs):
    held = jax.tree.unflatten(tree, refs)
    s = types.SimpleNamespace(**{key: named(value) for key, value in held.items()})
    counts, block, total = plan.counts, plan.block, plan.total
    top, wide, next_ = plan.top, plan.wide, plan.next
    place = tuple(lax.axis_index(axis) for axis in AXES)
    paired = counts[2] % 2 == 0
    kinds = 2 if paired else 1

    def slot_of(x, y, z):
        kind, rest = (lax.rem(z, 2), lax.div(z, 2)) if paired and not isinstance(z, int) else (z % kinds, z // kinds)
        return kind * (total // kinds) + (x * counts[1] + y) * (counts[2] // kinds) + rest

    me = slot_of(*place)
    padded = block[2] != plan.width

    loads = [pltpu.make_async_copy(density, s.raw if padded else s.own, sem(s, OWN))]
    loads[0].start()
    if not padded:
        loads.append(
            pltpu.make_async_copy(
                density,
                s.field.at[pl.ds(8, block[0]), pl.ds(0, block[1]), pl.ds(0, block[2])],
                sem(s, FIELD),
            )
        )
    fill = pltpu.make_async_copy(dense, s.matrix, sem(s, MATRIX))

    for ref in s.land + [s.swap_land, s.swap_side]:
        ref[...] = jnp.zeros(ref.shape, F32)

    axes = [partners(place[axis], counts[axis]) for axis in range(3)]
    offsets = [
        (a, b, c) for a in range(counts[0]) for b in range(counts[1]) for c in range(counts[2]) if (a, b, c) != (0, 0, 0)
    ]
    offsets.sort(key=lambda off: -(off[0] + off[1] + off[2] / 2))

    def peer(off, way):
        target = tuple(axes[axis][off[axis]][way] for axis in range(3))
        return target, slot_of(*target)

    other = peer(offsets[0], 0)[0]
    barrier = pltpu.get_barrier_semaphore()
    close = max(counts) <= 4
    waited = total - 1
    if close:
        waited = 1
        for axis in range(3):
            waited = waited * (1 + jnp.minimum(place[axis], 2) + jnp.minimum(counts[axis] - 1 - place[axis], 2))
        waited = waited - 1
    for off in offsets:
        target = peer(off, 0)[0]
        apart = [target[axis] - place[axis] for axis in range(3) if off[axis] and counts[axis] > 3]
        near = None
        for step in apart if close else []:
            here = (step <= 2) & (step >= -2)
            near = here if near is None else near & here
        if near is None:
            pl.semaphore_signal(barrier, inc=1, device_id=target, device_id_type=MESH)
            continue

        @pl.when(near)
        def _():
            pl.semaphore_signal(barrier, inc=1, device_id=target, device_id_type=MESH)

    for ref in [s.top.f, s.top.g] + s.top.R + s.top.B:
        ref[...] = jnp.zeros(ref.shape, F32)
    for v, grid in ((s.top, top), (s.wide, wide), (s.next, next_)):
        grid.guard(v)
        grid.masks(v, place, counts)
    for v, grid in zip(s.levels, plan.levels):
        grid.guard(v)
        grid.masks(v, (0, 0, 0), (1, 1, 1))
    loads[0].wait()
    for load in loads[1:] + [fill]:
        load.start()
    own = s.own
    if padded:
        own[...] = jnp.zeros(own.shape, F32)
        own[:, :, 0 : block[2]] = s.raw[...]

    even_own = parity_of(block[1], plan.width)
    for number in range(top.inner):
        one, two = own[2 * number], own[2 * number + 1]
        red = jnp.where(even_own, one, two)
        spot = number + top.margins[0]
        s.top.f[spot, 0 : block[1], 0 : plan.width] = red
        s.top.g[spot, 0 : block[1], 0 : plan.width] = jnp.where(even_own, two, one)
        for tile in range(plan.width // LANES):
            piece = red[:, tile * LANES : (tile + 1) * LANES] * inverse
            s.top.R[tile][spot + 1, 8 : 8 + block[1]] = piece
            s.top.R[tile][spot + 1, 8 + top.rows :] = piece[0:8]
    even_top = parity_of(top.rows, top.lanes)
    count = top.count
    if top.lanes == plan.width + LANES:
        first_black(plan, s, even_own)
    else:
        top.half(s.top, 1, even_top, 1, count - 1)
    top.half(s.top, 0, even_top, 1, count - 1)
    top.half(s.top, 1, even_top, 0, count)
    for number, value in top.residue(s.top, even_top, 0, count):
        for tile in range(plan.tiles):
            piece = value[:, tile * LANES : (tile + 1) * LANES]
            s.rows[tile][number, 0 : top.rows] = piece
            s.rows[tile][number, top.rows : top.rows + 8] = piece[block[1] :]
    flat = jnp.concatenate(
        [
            pair_sums(s.rows[tile], block[1] + 16, count).reshape(count * plan.high, LANES)
            for tile in range(plan.tiles)
        ],
        axis=1,
    )

    def fine_cell(shape, dim):
        index = iota(shape, dim)
        used = (index < block[2] + 4) | (index >= top.lanes - 4)
        cell = half_down(local_of(index, block[2], 4, top.lanes))
        return jnp.where(cell < 0, cell + LANES, cell), used

    shape = (top.lanes, LANES)
    cell, used = fine_cell(shape, 0)
    down = weights(shape, (cell == iota(shape, 1)) & used, 0.5)
    s.part[...] = dot(flat, down).reshape(count, plan.high, LANES)
    pack_part(plan, s)

    pl.semaphore_wait(barrier, waited)
    part = functools.partial(send_part, plan, s, place)
    far = functools.partial(send_far, plan, s, place)
    each(place, counts, part)

    lane = iota((block[1], LANES), 1)
    for side in range(2):
        begin = 0 if side == 0 else block[2] - 8
        tile = begin // LANES
        for pack in range(plan.far_packs):
            value = jnp.zeros((block[1], LANES), F32)
            for slot in range(16):
                plane = own[16 * pack + slot, :, tile * LANES : (tile + 1) * LANES]
                moved = pltpu.roll(plane, (8 * slot - begin) % LANES, 1)
                value = jnp.where(lane // 8 == slot, moved, value)
            s.far[side, pack] = value
    each(place, counts, far)
    field, far_land = s.field, s.far_land
    if padded:
        field[8 : 8 + block[0], 0 : block[1], 0 : plan.width] = own[...]
    for dim, step in ((0, -1), (0, 1), (1, -1), (1, 1), (2, -1), (2, 1)):
        steps = tuple(step if which == dim else 0 for which in range(3))

        @pl.when(jnp.logical_not(exists(place, steps, counts)))
        def _():
            if dim == 0:
                begin = 0 if step < 0 else 8 + block[0]
                field[begin : begin + 8] = jnp.zeros((8,) + field.shape[1:], F32)
                pack = 0 if step < 0 else plan.far_packs + 1
                far_land[:, pack] = jnp.zeros((2,) + far_land.shape[2:], F32)
            if dim == 1:
                begin = block[1] if step > 0 else block[1] + 8
                field[:, begin : begin + 8] = jnp.zeros((field.shape[0], 8, field.shape[2]), F32)
                far_land[:, :, begin : begin + 8] = jnp.zeros(far_land.shape[:2] + (8, LANES), F32)
            if dim == 2:
                far_land[(1 - step) // 2] = jnp.zeros(far_land.shape[1:], F32)

    wait_all(plan, s, place, size_part, PART + 1, other)
    gather_part(plan, s)
    even_next = parity_of(next_.rows, LANES)
    n = next_.count
    next_.first(s.next, 0, n)
    next_.half(s.next, 1, even_next, 1, n - 1)
    next_.half(s.next, 0, even_next, 2, n - 2)
    next_.half(s.next, 1, even_next, 2, n - 2)
    pairs = s.pairs
    rows1 = plan.block1[1]
    height = max(rows1, 16)
    if rows1 < height:
        pairs[0 : next_.inner, rows1:height] = jnp.zeros((next_.inner, height - rows1, LANES), F32)
    for number, value in next_.residue(s.next, even_next, 3, n - 3):
        pairs[number - 3, 0:rows1] = value[0:rows1]
    flat = pair_sums(pairs, height, next_.inner).reshape(next_.inner * (height // 2), LANES)
    row, column = iota((LANES, LANES), 0), iota((LANES, LANES), 1)
    down = weights((LANES, LANES), (row // 2 == column) & (row < plan.block1[2]), 0.5)
    below = dot(flat, down).reshape(next_.inner, height // 2, LANES)
    length = plan.block2
    per = LANES // length[2]
    packed = jnp.zeros((8, LANES), F32)
    for plane in range(length[0]):
        moved = below[plane]
        if plane // per:
            moved = pltpu.roll(moved, length[1] * (plane // per), 0)
        if plane % per:
            moved = pltpu.roll(moved, length[2] * (plane % per), 1)
        packed = packed + moved
    s.mine[...] = packed
    slots = s.slots
    slots[me] = packed

    def send(number, slot):
        return pltpu.make_async_remote_copy(
            src_ref=s.mine,
            dst_ref=slots.at[slot],
            send_sem=sem(s, ALL),
            recv_sem=sem(s, ALL + 1),
            device_id=peer(offsets[number], 0)[0],
            device_id_type=MESH,
        )

    chosen = [number for number, off in enumerate(offsets) if off[2] % kinds == 0]

    def start_sends():
        for number in chosen:
            send(number, me).start()

    def forward():
        half = total // 2
        kind = lax.rem(place[2], 2) * half
        return pltpu.make_async_remote_copy(
            src_ref=slots.at[pl.ds(kind, half)],
            dst_ref=slots.at[pl.ds(kind, half)],
            send_sem=sem(s, PAIR),
            recv_sem=sem(s, PAIR + 1),
            device_id=peer((0, 0, 1), 0)[0],
            device_id_type=MESH,
        )

    start_sends()
    swap = functools.partial(send_swap, plan, s, place)
    pack_swap(plan, s)
    each(place, counts, swap)

    def finish_sends():
        for name in (ALL + 1, ALL):
            pltpu.make_async_remote_copy(
                src_ref=s.bytes.at[pl.ds(0, len(chosen))],
                dst_ref=s.bytes.at[pl.ds(0, len(chosen))],
                send_sem=sem(s, name),
                recv_sem=sem(s, name),
                device_id=other,
                device_id_type=MESH,
            ).wait_recv()

    wait_all(plan, s, place, size_far, FAR + 1, other)
    if not padded:
        loads[1].wait()
    base = wide.lanes - LANES
    shape = (wide.rows, LANES)
    lane = iota(shape, 1)
    even_wide = parity_of(wide.rows, wide.lanes)
    above = block[2] - base

    def wide_plane(number):
        pack, slot = (number + 8) // 16, (number + 8) % 16
        high = pltpu.roll(far_land[0, pack], (above - 8 * slot) % LANES, 1)
        low = pltpu.roll(far_land[1, pack], (LANES - 8 - 8 * slot) % LANES, 1)
        old = field[number, :, 0:LANES] if base == 0 else 0.0
        value = jnp.where((lane >= above) & (lane < above + 8), high, old)
        value = jnp.where(lane >= LANES - 8, low, value)
        return value if base == 0 else jnp.concatenate([field[number, :, 0:base], value], axis=1)

    for number in range(wide.count):
        one, two = wide_plane(2 * number), wide_plane(2 * number + 1)
        s.wide.f[number] = jnp.where(even_wide, one, two)
        s.wide.g[number] = jnp.where(even_wide, two, one)
    n = wide.count
    wide.first(s.wide, 0, n)
    wide.half(s.wide, 1, even_wide, 1, n - 1)
    wide.half(s.wide, 0, even_wide, 1, n - 1)
    wide.half(s.wide, 1, even_wide, 2, n - 2)
    wider = iota((8, wide.lanes), 0) < 4

    def narrow(value):
        both = jnp.where(wider, value[block[1] : block[1] + 8], value[block[1] + 8 :])
        value = jnp.concatenate([value[: block[1]], both], axis=0)
        if top.lanes != wide.lanes:
            value = jnp.concatenate([value[:, : top.lanes - LANES], value[:, -LANES:]], axis=1)
        return value

    shift = wide.margins[0] - top.margins[0]
    for number in range(count):
        s.top.f[number] = narrow(s.wide.f[number + shift])
        s.top.g[number] = narrow(s.wide.g[number + shift])
        top.put(s.top.B, number + 1, narrow(wide.get(s.wide.B, number + shift + 1)))

    finish_sends()
    if paired:
        forward().start()
        forward().wait()
    fill.wait()
    lane = iota((8, LANES), 1)
    whole = s.whole
    first = plan.levels[0]

    def place_x(which):
        for second in range(counts[1]):
            tiles = [slots[slot_of(which, second, third)] for third in range(counts[2])]
            for spot in range(per):
                value = jnp.zeros((8, LANES), F32)
                for third in range(counts[2]):
                    turn = (length[2] * (third - spot)) % LANES
                    moved = pltpu.roll(tiles[third], turn, 1) if turn else tiles[third]
                    value = jnp.where(lane // length[2] == third, moved, value)
                for group in range(8 // length[1]):
                    plane = which * length[0] + group * per + spot
                    whole[plane, second * length[1] : (second + 1) * length[1], :] = value[
                        group * length[1] : (group + 1) * length[1]
                    ]

    for which in range(counts[0]):
        place_x(which)
    even_first = parity_of(first.rows, LANES)
    for number in range(first.count):
        one, two = whole[2 * number], whole[2 * number + 1]
        s.levels[0].f[number] = jnp.where(even_first, one, two)
        s.levels[0].g[number] = jnp.where(even_first, two, one)
    solve(plan, s, 0)
    solved = s.solved
    for number in range(3):
        solved[number] = jnp.zeros((first.rows, LANES), F32)
        solved[first.block[0] + 3 + number] = jnp.zeros((first.rows, LANES), F32)
    for plane in range(first.block[0]):
        solved[plane + 3] = first.planes(s.levels[0], even_first, plane)

    wait_all(plan, s, place, size_swap, SWAP + 1, other)
    wait_all(plan, s, place, size_swap, SWAP, other)
    shape = (LANES, LANES)
    index = iota(shape, 1)
    spot = local_of(index, plan.block1[2], 8, LANES)
    used = (index < plan.block1[2] + 8) | (index >= LANES - 8)
    lanes_to = weights(shape, (half_down(spot) + place[2] * length[2] == iota(shape, 0)) & used, 1.0)
    n = next_.count
    flat = jnp.concatenate([solved[place[0] * length[0] + number] for number in range(n)], axis=0)
    flat = dot(flat, lanes_to).reshape(n, first.rows, LANES)
    spread = s.spread
    spread[:, 0:16] = jnp.zeros((n, 16, LANES), F32)
    spread[:, 16 + 2 * first.rows :] = jnp.zeros((n, 16, LANES), F32)
    spread[0:n, pl.ds(16, first.rows, stride=2), :] = flat
    spread[0:n, pl.ds(17, first.rows, stride=2), :] = flat
    start = 16 + place[1] * rows1
    for number in range(n):
        tiles = [
            spread[number, pl.ds(pl.multiple_of(start + shift, 8), size), :]
            for shift, size in ((0, rows1), (rows1, 8), (-8, 8))
        ]
        next_.put(s.next.B, number + 1, swapped(plan, s, number) + jnp.concatenate(tiles, axis=0))
    for colour, skip in ((0, 0), (1, 1), (0, 1), (1, 2)):
        next_.half(s.next, colour, even_next, skip, n - skip)

    pick = iota((8, LANES), 0) < 4
    planes = []
    for number in range(count):
        value = next_.planes(s.next, even_next, number + 2 * next_.margins[0] - top.margins[0])
        edge = jnp.where(pick, value[rows1 : rows1 + 8], value[rows1 + 8 :])
        planes.append(jnp.concatenate([value[:rows1], edge], axis=0))
    shape = (LANES, top.lanes)
    cell, used = fine_cell(shape, 1)
    spreading = weights(shape, (cell == iota(shape, 0)) & used, 1.0)
    flat = dot(jnp.concatenate(planes, axis=0), spreading).reshape(count, plan.high, top.lanes)
    for tile in range(plan.tiles):
        piece = flat[:, :, tile * LANES : (tile + 1) * LANES]
        s.rows[tile][0:count, pl.ds(0, plan.high, stride=2), :] = piece
        s.rows[tile][0:count, pl.ds(1, plan.high, stride=2), :] = piece
    for number in range(count):
        tiles = []
        for tile in range(plan.tiles):
            rows = s.rows[tile]
            edge = jnp.where(pick, rows[number, block[1] : block[1] + 8], rows[number, block[1] + 8 : block[1] + 16])
            tiles.append(jnp.concatenate([rows[number, 0 : block[1]], edge], axis=0))
        top.put(s.top.B, number + 1, top.get(s.top.B, number + 1) + jnp.concatenate(tiles, axis=1))
    top.half(s.top, 0, even_top, 0, count)
    top.half(s.top, 1, even_top, 1, count - 1)
    top.half(s.top, 0, even_top, 1, count - 1)
    red = s.top.R
    even_out = parity_of(block[1], block[2])
    for number, value in top.totals(red, even_top, 1, top.margins[0], count - top.margins[0]):
        black = ((s.top.g[number] + value) * inverse)[0 : block[1], 0 : block[2]]
        old = top.get(red, number + 1)[0 : block[1], 0 : block[2]]
        plane = 2 * (number - top.margins[0])
        potential[plane] = jnp.where(even_out, old, black)
        potential[plane + 1] = jnp.where(even_out, black, old)
    wait_all(plan, s, place, size_part, PART, other)
    wait_all(plan, s, place, size_far, FAR, other)


def cycle_matrix(size, depth):
    def beside_sum(v):
        p = np.pad(v, ((0, 0), (1, 1), (1, 1), (1, 1)))
        total = p[:, 2:, 1:-1, 1:-1] + p[:, :-2, 1:-1, 1:-1] + p[:, 1:-1, 2:, 1:-1] + p[:, 1:-1, :-2, 1:-1]
        return total + along * (p[:, 1:-1, 1:-1, 2:] + p[:, 1:-1, 1:-1, :-2])

    def cycle(g, left):
        parity = np.indices(g.shape[1:]).sum(0) % 2

        def sweeps(v, number):
            for _ in range(number):
                for colour in (0, 1):
                    v = np.where(parity == colour, (g + beside_sum(v)) / centre, v)
            return v

        v = np.zeros_like(g)
        if left == 0:
            return sweeps(v, CSWEEPS)
        v = sweeps(v, 2)
        r = g - centre * v + beside_sum(v)
        x, y, z = (part // 2 for part in g.shape[1:])
        coarse = 4 * r.reshape(-1, x, 2, y, 2, z, 2).mean((2, 4, 6))
        e = cycle(coarse, left - 1)
        for dim in (1, 2, 3):
            e = np.repeat(e, 2, dim)
        return sweeps(v + e, 2)

    cells = size[0] * size[1] * size[2]
    found = cycle(np.eye(cells).reshape((cells,) + size), depth).reshape(cells, cells)
    parts = []
    for _ in range(3):
        parts.append(found.astype(np.float32).astype(jnp.bfloat16))
        found = found - parts[-1].astype(np.float64)
    return np.stack(parts)


def on_device(counts, density):
    plan = Plan(density.shape, counts)
    scratch, tree = jax.tree.flatten(plan.scratch())
    matrix = jnp.asarray(cycle_matrix(plan.dense, LEVELS - 1 - plan.dense_level))
    return pl.pallas_call(
        functools.partial(kernel, plan, tree),
        out_shape=jax.ShapeDtypeStruct(density.shape, F32),
        in_specs=[pl.BlockSpec(memory_space=pltpu.HBM)] * 2,
        out_specs=pl.BlockSpec(memory_space=pltpu.VMEM),
        scratch_shapes=scratch,
        compiler_params=pltpu.CompilerParams(
            collective_id=0, has_side_effects=True, vmem_limit_bytes=48 * 1024 * 1024
        ),
    )(
        pltpu.with_memory_space_constraint(density, pltpu.HBM),
        pltpu.with_memory_space_constraint(matrix, pltpu.HBM),
    )


def solution(mesh):
    counts = tuple(mesh.shape[axis] for axis in AXES)
    return jax.shard_map(
        functools.partial(on_device, counts),
        mesh=mesh,
        in_specs=(P("gx", "gy", "gz"),),
        out_specs=P("gx", "gy", "gz"),
        check_vma=False,
    )
```

```python
import functools
import types

import jax
import jax.numpy as jnp
import numpy as np
from jax import lax
from jax.experimental import pallas as pl
from jax.experimental.pallas import tpu as pltpu
from jax.sharding import PartitionSpec as P

LEVELS = 7
CSWEEPS = 4
DENSE = 512
rsd_beta = 0.5
centre = 4.0 + 2.0 * (1.0 + rsd_beta)
along = 1.0 + rsd_beta
inverse = 1.0 / centre
F32 = jnp.float32
BF16 = jnp.bfloat16
LANES = 128
AXES = ("gx", "gy", "gz")
MESH = pl.DeviceIdType.MESH
DIRECTIONS = [
    (dx, dy, dz) for dx in (-1, 0, 1) for dy in (-1, 0, 1) for dz in (-1, 0, 1) if (dx, dy, dz) != (0, 0, 0)
]


ALL, PART, FAR, SWAP, OWN, FIELD, MATRIX, PAIR = 0, 2, 4, 6, 8, 9, 10, 11


def up_to(value, unit):
    return -(-value // unit) * unit


def iota(shape, dim):
    return lax.broadcasted_iota(jnp.int32, shape, dim)


def pieces(value):
    high = value.astype(BF16)
    rest = value - high.astype(F32)
    middle = rest.astype(BF16)
    return high, middle, (rest - middle.astype(F32)).astype(BF16)


def product(left, right):
    return jnp.dot(left, right, preferred_element_type=F32)


def dot(value, chosen):
    chosen = chosen.astype(BF16)
    parts = [product(part, chosen) for part in pieces(value)]
    return parts[0] + (parts[1] + parts[2])


def local_of(index, length, margin, total):
    return jnp.where(index < total - margin, index, index - total)


def half_down(value):
    return jnp.where(value >= 0, lax.div(value, 2), -lax.div(1 - value, 2))


def parity_of(rows, lanes, step=1):
    return (iota((rows, lanes), 0) + iota((rows, lanes), 1) // step) % 2 == 0


def beside(below, here, above, down, up, even, colour, edge, step):
    lanes = here.shape[1]
    left, right = pltpu.roll(here, step, 1), pltpu.roll(here, lanes - step, 1)
    if edge is not None:
        if edge[1] * step == lanes:
            lane = iota(here.shape, 1)
            left = jnp.where(lane < step, 0.0, left)
            right = jnp.where(lane >= lanes - step, 0.0, right)
    other = jnp.where(even, below, above) if colour == 0 else jnp.where(even, above, below)
    return (here + other) + (down + up) + along * (left + right)


class Grid:
    def __init__(self, block, margins, edge=False, step=1):
        self.block, self.margins, self.step = block, margins, step
        self.inner = block[0] // 2
        self.count = self.inner + 2 * margins[0]
        self.rows = up_to(block[1] + 2 * margins[1], 8)
        self.lanes = up_to(block[2] + 2 * margins[2], LANES)
        self.edge = (block[1], block[2]) if edge else None
        self.tiles = self.lanes // LANES

    def scratch(self):
        field = (self.count + 2, self.rows + 16, LANES)
        source = (self.count, self.rows, self.lanes)
        return dict(
            R=[pltpu.VMEM(field, F32) for _ in range(self.tiles)],
            B=[pltpu.VMEM(field, F32) for _ in range(self.tiles)],
            f=pltpu.VMEM(source, F32),
            g=pltpu.VMEM(source, F32),
            m=pltpu.VMEM((3, self.rows, self.lanes), F32),
        )

    def zone(self, number):
        if number < self.margins[0]:
            return 0
        return 2 if number >= self.count - self.margins[0] else 1

    def guard(self, v):
        empty = jnp.zeros((self.rows + 16, LANES), F32)
        for ref in v.R + v.B:
            ref[0] = empty
            ref[self.count + 1] = empty
            if self.edge:
                ref[:, 0:8] = jnp.zeros((self.count + 2, 8, LANES), F32)
                ref[:, self.rows + 8 :] = jnp.zeros((self.count + 2, 8, LANES), F32)

    def get(self, field, number, shift=0):
        parts = [ref[number, 8 + shift : 8 + shift + self.rows] for ref in field]
        return parts[0] if len(parts) == 1 else jnp.concatenate(parts, axis=1)

    def put(self, field, number, value):
        for tile, ref in enumerate(field):
            piece = value[:, tile * LANES : (tile + 1) * LANES]
            ref[number, 8 : 8 + self.rows] = piece
            if not self.edge:
                ref[number, 0:8] = piece[self.rows - 8 :]
                ref[number, 8 + self.rows :] = piece[0:8]

    def masks(self, v, place, counts):
        inside = None
        shape = (self.rows, self.lanes)
        for dim in (1, 2):
            index = iota(shape, dim - 1)
            size = shape[dim - 1]
            if dim == 2 and self.step > 1:
                inside = inside & (index % self.step == 0) & (index < self.step * self.block[2])
                continue
            margin, length = self.margins[dim], self.block[dim]
            used = (index < length + margin) | (index >= size - margin)
            spot = local_of(index, length, margin, size) + place[dim] * length
            used = used & (spot >= 0) & (spot < length * counts[dim])
            inside = used if inside is None else inside & used
        value = jnp.where(inside, inverse, 0.0).astype(F32)
        v.m[1] = value
        if self.edge:
            for zone, shift in ((0, -self.step), (2, self.step)):
                spot = iota(shape, 1) + shift
                kept = (spot >= 0) & (spot < self.step * self.block[2]) & (iota(shape, 1) % self.step == 0)
                v.m[zone] = jnp.where(kept & (iota(shape, 0) < self.block[1]), inverse, 0.0).astype(F32)
        if self.margins[0]:
            low = jnp.where(place[0] > 0, 1.0, 0.0).astype(F32)
            high = jnp.where(place[0] < counts[0] - 1, 1.0, 0.0).astype(F32)
            v.m[0] = value * low
            v.m[2] = value * high

    def first(self, v, begin, end):
        for number in range(begin, end):
            self.put(v.R, number + 1, v.f[number] * v.m[self.zone(number)])

    def totals(self, other, even, colour, begin, end):
        before, here = self.get(other, begin), self.get(other, begin + 1)
        for number in range(begin, end):
            after = self.get(other, number + 2)
            down, up = self.get(other, number + 1, -1), self.get(other, number + 1, 1)
            yield number, beside(before, here, after, down, up, even, colour, self.edge, self.step)
            before, here = here, after

    def half(self, v, colour, even, begin, end):
        target, other = (v.R, v.B) if colour == 0 else (v.B, v.R)
        source = v.f if colour == 0 else v.g
        for number, total in self.totals(other, even, colour, begin, end):
            self.put(target, number + 1, (source[number] + total) * v.m[self.zone(number)])

    def pair(self, v, even):
        step, lanes = self.step, self.lanes
        lane = iota((self.rows, lanes), 1)
        sides = []
        for number in range(self.count):
            here = self.get(v.B, number + 1)
            other = jnp.where(even, self.get(v.B, number), self.get(v.B, number + 2))
            rows = self.get(v.B, number + 1, -1) + self.get(v.B, number + 1, 1)
            total = v.f[number] + ((here + other) + rows)
            left = jnp.where(lane < step, 0.0, pltpu.roll(here, step, 1))
            right = jnp.where(lane >= lanes - step, 0.0, pltpu.roll(here, lanes - step, 1))
            second = jnp.where(lane < 2 * step, 0.0, pltpu.roll(here, 2 * step, 1))
            third = jnp.where(lane >= lanes - 2 * step, 0.0, pltpu.roll(here, lanes - 2 * step, 1))
            self.put(v.R, number + 1, (total + along * (left + right)) * v.m[1])
            before = (pltpu.roll(total, step, 1) + along * (second + here)) * v.m[0]
            after = (pltpu.roll(total, lanes - step, 1) + along * (here + third)) * v.m[2]
            sides.append(before + after)
        for number in range(self.count):
            here = self.get(v.R, number + 1)
            other = jnp.where(even, self.get(v.R, number + 2), self.get(v.R, number))
            rows = self.get(v.R, number + 1, -1) + self.get(v.R, number + 1, 1)
            total = v.g[number] + ((here + other) + rows)
            self.put(v.B, number + 1, (total + along * sides[number]) * v.m[1])

    def residue(self, v, even, begin, end):
        for number, total in self.totals(v.B, even, 0, begin, end):
            yield number, v.f[number] - centre * self.get(v.R, number + 1) + total

    def planes(self, v, even, plane):
        red, black = self.get(v.R, plane // 2 + 1), self.get(v.B, plane // 2 + 1)
        return jnp.where(even, red, black) if plane % 2 == 0 else jnp.where(even, black, red)


def exists(place, steps, counts):
    found = None
    for which in range(3):
        if steps[which] == 0:
            continue
        other = place[which] + steps[which]
        here = (other >= 0) & (other < counts[which])
        found = here if found is None else found & here
    return found


def device(place, steps):
    return tuple(place[which] + steps[which] for which in range(3))


class Plan:
    def __init__(self, block, counts):
        self.counts, self.block = counts, block
        self.total = counts[0] * counts[1] * counts[2]
        self.block1 = tuple(size // 2 for size in block)
        self.block2 = tuple(size // 4 for size in block)
        self.top = Grid(block, (2, 4, 4))
        self.wide = Grid(block, (4, 8, 8))
        self.next = Grid(self.block1, (3, 8, 8))
        self.width = up_to(block[2], LANES)
        self.tiles = self.top.lanes // LANES
        self.count = self.top.count
        self.high = self.block1[1] + 8
        self.per = LANES // self.block1[2]
        self.side = 8 // self.per
        self.middle = (self.count - 16) // self.per
        self.vectors = 2 * self.side + self.middle + 1
        self.packs = 1 + (self.count > 16)
        self.far_packs = block[0] // 16
        assert block[0] % 16 == 0 and self.block1[1] % 8 == 0 and self.block2[2] <= LANES
        assert self.next.lanes == LANES and (self.count - 16) % self.per == 0 and 64 % self.block1[2] == 0
        self.levels = []
        size = tuple(block[which] * counts[which] // 4 for which in range(3))
        number = 2
        while size[0] * size[1] * size[2] > DENSE:
            self.levels.append(Grid(size, (0, 0, 0), edge=True, step=1 << len(self.levels)))
            assert self.levels[-1].lanes == LANES
            size = tuple(part // 2 for part in size)
            number += 1
        self.dense, self.dense_level = size, number

    def message(self, steps):
        dx, dy, dz = steps
        if dz == 0:
            begin, length = {0: (0, self.vectors), -1: (0, self.side + 1), 1: (self.side, self.side + 1)}[dx]
            if dy == 0:
                return ("part_t", (pl.ds(begin, length),), (length, self.high, LANES))
            return ("part_y", ((dy + 1) // 2, pl.ds(begin, length)), (length, 8, LANES))
        length = self.packs if dx == 0 else 1
        if dy == 0:
            return ("part_z", ((dz + 1) // 2, pl.ds(0, length)), (length, self.high, LANES))
        return (
            "part_zy", ((dz + 1) // 2, (dy + 1) // 2, pl.ds(0, length)), (length, 8, LANES),
        )

    def scratch(self):
        block = self.block
        s = types.SimpleNamespace(
            top=self.top.scratch(), wide=self.wide.scratch(), next=self.next.scratch(),
            levels=[grid.scratch() for grid in self.levels],
        )
        s.own = pltpu.VMEM((block[0], block[1], self.width), F32)
        if block[2] != self.width:
            s.raw = pltpu.VMEM(block, F32)
        s.field = pltpu.VMEM((block[0] + 16, block[1] + 16, self.wide.lanes), F32)
        s.rows = [pltpu.VMEM((self.count, block[1] + 16, LANES), F32) for _ in range(self.tiles)]
        s.part = pltpu.VMEM((self.count, self.high, LANES), F32)
        s.part_t = pltpu.VMEM((self.vectors, self.high, LANES), F32)
        s.part_y = pltpu.VMEM((2, self.vectors, 8, LANES), F32)
        s.part_z = pltpu.VMEM((2, self.packs, self.high, LANES), F32)
        s.part_zy = pltpu.VMEM((2, 2, self.packs, 8, LANES), F32)
        s.land = [pltpu.VMEM(self.message(steps)[2], F32) for steps in DIRECTIONS]
        s.sums, s.sumz = [], []
        wide_rows = self.block1[1] + 16
        for dx in (-1, 0, 1):
            length = self.vectors if dx == 0 else self.side + 1
            packs = self.packs if dx == 0 else 1
            s.sums.append(pltpu.VMEM((length, wide_rows, LANES), F32))
            s.sumz.append(pltpu.VMEM((2, packs, wide_rows, LANES), F32))
        s.far = pltpu.VMEM((2, self.far_packs, block[1], LANES), F32)
        s.far_land = pltpu.VMEM((2, self.far_packs + 2, block[1] + 16, LANES), F32)
        s.swap = pltpu.VMEM((2, self.block1[1], LANES), F32)
        s.swap_land = pltpu.VMEM((self.next.count, self.next.rows, LANES), F32)
        s.swap_side = pltpu.VMEM((2, 3, self.next.rows, LANES), F32)
        first = self.levels[0]
        coarse = [first] + self.levels[1:]
        s.pairs = pltpu.VMEM((max(g.block[0] for g in coarse + [self.next]), 2 * up_to(first.rows, 16), LANES), F32)
        s.solved = pltpu.VMEM((first.block[0] + 6, first.rows, LANES), F32)
        s.spread = pltpu.VMEM((self.next.count, 2 * first.rows + 32, LANES), F32)
        s.whole = pltpu.VMEM((first.block[0], first.rows, LANES), F32)
        s.mine = pltpu.VMEM((8, LANES), F32)
        s.slots = pltpu.VMEM((self.total, 8, LANES), F32)
        size = self.dense[0] * self.dense[1] * self.dense[2]
        s.matrix = pltpu.VMEM((3, size, size), BF16)
        most = max(sum(size(self, steps) for steps in DIRECTIONS) for size in (size_part, size_far, size_swap))
        s.bytes = pltpu.VMEM((max(most, self.total), 8, LANES), F32)
        s.sem = pltpu.SemaphoreType.DMA((PAIR + 2,))
        return vars(s)


def weights(shape, found, value):
    return jnp.where(found, value, 0.0).astype(F32).reshape(shape)


def pair_sums(s, height, count):
    even = s[0:count, pl.ds(0, height // 2, stride=2), :]
    return even + s[0:count, pl.ds(1, height // 2, stride=2), :]


def named(value):
    if isinstance(value, dict):
        return types.SimpleNamespace(**value)
    return [named(one) for one in value] if isinstance(value, list) else value


def sem(s, number):
    return s.sem.at[number]


def size_part(plan, steps):
    shape = plan.message(steps)[2]
    return shape[0] * shape[1] // 8


def size_far(plan, steps):
    rows = plan.block[1] // 8 if steps[1] == 0 else 1
    if steps[2]:
        return rows * (plan.far_packs if steps[0] == 0 else 1)
    return rows * (plan.block[0] if steps[0] == 0 else 8) * (plan.width // LANES)


def size_swap(plan, steps):
    rows = plan.block1[1] // 8 if steps[1] == 0 else 1
    return rows if steps[2] else rows * (plan.next.inner if steps[0] == 0 else plan.next.margins[0])


def wait_all(plan, s, place, size, name, other):
    counts = plan.counts
    beside_of = [
        jnp.where(place[axis] > 0, 1, 0) + jnp.where(place[axis] < counts[axis] - 1, 1, 0) for axis in range(3)
    ]
    choices = [{1: (0,), 2: (1,)}.get(count, (1, 2)) for count in counts]
    for x in choices[0]:
        for y in choices[1]:
            for z in choices[2]:
                number = 0
                for steps in DIRECTIONS:
                    many = [1 if step == 0 else (have if step > 0 else 0) for step, have in zip(steps, (x, y, z))]
                    if min(steps) >= 0:
                        number += many[0] * many[1] * many[2] * size(plan, steps)
                if number == 0:
                    continue
                found = (beside_of[0] == x) & (beside_of[1] == y) & (beside_of[2] == z)

                @pl.when(found)
                def _():
                    pltpu.make_async_remote_copy(
                        src_ref=s.bytes.at[pl.ds(0, number)],
                        dst_ref=s.bytes.at[pl.ds(0, number)],
                        send_sem=sem(s, name),
                        recv_sem=sem(s, name),
                        device_id=other,
                        device_id_type=MESH,
                    ).wait_recv()


def send_part(plan, s, place, number):
    steps = DIRECTIONS[number]
    name, index, _ = plan.message(steps)
    return pltpu.make_async_remote_copy(
        src_ref=getattr(s, name).at[index],
        dst_ref=s.land[number],
        send_sem=sem(s, PART),
        recv_sem=sem(s, PART + 1),
        device_id=device(place, steps),
        device_id_type=MESH,
    )


def send_far(plan, s, place, number):
    dx, dy, dz = steps = DIRECTIONS[number]
    block = plan.block
    rows = {0: (0, block[1], 0), 1: (block[1] - 8, 8, block[1] + 8), -1: (0, 8, block[1])}[dy]
    if dz == 0:
        planes = {0: (0, block[0], 8), 1: (block[0] - 8, 8, 0), -1: (0, 8, block[0] + 8)}[dx]
        source = s.own.at[pl.ds(planes[0], planes[1]), pl.ds(rows[0], rows[1]), :]
        target = s.field.at[pl.ds(planes[2], planes[1]), pl.ds(rows[2], rows[1]), pl.ds(0, plan.width)]
    else:
        side, last = (dz + 1) // 2, plan.far_packs - 1
        packs = {0: (0, last + 1, 1), 1: (last, 1, 0), -1: (0, 1, last + 2)}[dx]
        source = s.far.at[side, pl.ds(packs[0], packs[1]), pl.ds(rows[0], rows[1]), :]
        target = s.far_land.at[side, pl.ds(packs[2], packs[1]), pl.ds(rows[2], rows[1]), :]
    return pltpu.make_async_remote_copy(
        src_ref=source,
        dst_ref=target,
        send_sem=sem(s, FAR),
        recv_sem=sem(s, FAR + 1),
        device_id=device(place, steps),
        device_id_type=MESH,
    )


def send_swap(plan, s, place, number):
    dx, dy, dz = steps = DIRECTIONS[number]
    high, margin, inner = plan.block1[1], plan.next.margins[0], plan.next.inner
    rows = {0: (0, high, 0), 1: (high - 8, 8, high + 8), -1: (0, 8, high)}[dy]
    if dz == 0:
        planes = {0: (margin, inner, margin), 1: (inner, margin, 0), -1: (margin, margin, margin + inner)}[dx]
        source = s.next.B[0].at[pl.ds(1 + planes[0], planes[1]), pl.ds(8 + rows[0], rows[1]), :]
        target = s.swap_land.at[pl.ds(planes[2], planes[1]), pl.ds(rows[2], rows[1]), :]
    else:
        side = (dz + 1) // 2
        source = s.swap.at[side, pl.ds(rows[0], rows[1]), :]
        target = s.swap_side.at[side, 1 - dx, pl.ds(rows[2], rows[1]), :]
    return pltpu.make_async_remote_copy(
        src_ref=source,
        dst_ref=target,
        send_sem=sem(s, SWAP),
        recv_sem=sem(s, SWAP + 1),
        device_id=device(place, steps),
        device_id_type=MESH,
    )


def pack_swap(plan, s):
    length, margin = plan.block1[2], plan.next.margins[0]
    lane = iota((plan.block1[1], LANES), 1)
    for side in range(2):
        begin = 0 if side == 0 else length - 8
        value = jnp.zeros(lane.shape, F32)
        for slot in range(plan.next.inner):
            plane = s.next.B[0][1 + margin + slot, 8 : 8 + plan.block1[1], :]
            value = jnp.where(lane // 8 == slot, pltpu.roll(plane, (8 * slot - begin) % LANES, 1), value)
        s.swap[side] = value


def swapped(plan, s, number):
    length, rows = plan.block1[2], plan.block1[1]
    margin, inner = plan.next.margins[0], plan.next.inner
    lane = iota((plan.next.rows, LANES), 1)
    which = 0 if number < margin else (2 if number >= margin + inner else 1)
    slot = number - margin + (1 - which) * inner
    value = s.swap_land[number]
    if which == 1:
        value = jnp.concatenate([s.next.B[0][number + 1, 8 : 8 + rows, :], value[rows:]], axis=0)
    high = pltpu.roll(s.swap_side[0, which], (length - 8 * slot) % LANES, 1)
    low = pltpu.roll(s.swap_side[1, which], (LANES - 8 - 8 * slot) % LANES, 1)
    edge = jnp.where(lane < length + 8, high, jnp.where(lane >= LANES - 8, low, 0.0))
    return jnp.where(lane < length, value, edge)


def partners(place, count):
    if count & (count - 1):
        return [(lax.rem(place + off, count), lax.rem(place + count - off, count)) for off in range(count)]
    bits = [lax.rem(lax.div(place, 1 << bit), 2) for bit in range(count.bit_length() - 1)]
    out = []
    for off in range(count):
        value = jnp.int32(0)
        for bit, digit in enumerate(bits):
            value = value + ((1 - digit) if off >> bit & 1 else digit) * (1 << bit)
        out.append((value, value))
    return out


def each(place, counts, send):
    for number, steps in enumerate(DIRECTIONS):
        @pl.when(exists(place, steps, counts))
        def _():
            send(number).start()


def pack_part(plan, s):
    count, per, side, middle, rows = plan.count, plan.per, plan.side, plan.middle, plan.block1[1]
    length = plan.block1[2]
    part = s.part
    shape = (plan.high, LANES)
    lane = iota(shape, 1)
    sub = iota((8, LANES), 0)

    def pair_y(value):
        edge = value[rows:]
        minus = jnp.where(sub >= 6, edge, value[:8])
        return minus, jnp.where(sub < 2, edge, value[rows - 8 : rows])

    groups = [(0, 0, side), (side + 1, count - 8, side), (2 * side + 1, 8, middle)]
    for index, first, number in groups:
        for spot in range(number):
            value = part[first + spot]
            for which in range(1, per):
                moved = pltpu.roll(part[first + spot + which * number], which * length, 1)
                value = jnp.where(lane // length == which, moved, value)
            s.part_t[index + spot] = value
            minus, plus = pair_y(value)
            s.part_y[0, index + spot] = minus
            s.part_y[1, index + spot] = plus
    value = jnp.zeros(shape, F32)
    couple = lane // 2
    for number in range(count):
        low = pltpu.roll(part[number], 2 * number, 1)
        high = low if length == 64 else pltpu.roll(part[number], 64 - length + 2 * number, 1)
        value = jnp.where(couple == ((126 + 2 * number) % LANES) // 2, low, value)
        value = jnp.where(couple == 32 + number, high, value)
    s.part_t[side] = value
    minus, plus = pair_y(value)
    s.part_y[0, side] = minus
    s.part_y[1, side] = plus
    for which in range(2):
        begin = LANES - 2 if which == 0 else length - 6
        for pack in range(plan.packs):
            value = jnp.zeros(shape, F32)
            planes = list(range(8)) + list(range(count - 8, count)) if pack == 0 else list(range(8, count - 8))
            for slot, number in enumerate(planes):
                moved = pltpu.roll(part[number], (8 * slot - begin) % LANES, 1)
                value = jnp.where(lane // 8 == slot, moved, value)
            s.part_z[which, pack] = value
            minus, plus = pair_y(value)
            s.part_zy[which, 0, pack] = minus
            s.part_zy[which, 1, pack] = plus


def gather_part(plan, s):
    side, count, rows, per, length = plan.side, plan.count, plan.block1[1], plan.per, plan.block1[2]
    sub = iota((8, LANES), 0)
    land = {steps: s.land[number] for number, steps in enumerate(DIRECTIONS)}

    def assembled(own, plus, minus):
        edge = own[rows:]
        tiles = [own[8 * number : 8 * number + 8] for number in range(rows // 8)]
        tiles[0] = tiles[0] + jnp.where(sub < 2, minus, 0.0)
        tiles[-1] = tiles[-1] + jnp.where(sub >= 6, plus, 0.0)
        tiles.append(jnp.where(sub < 6, plus, 0.0) + jnp.where(sub < 2, edge, 0.0))
        tiles.append(jnp.where(sub >= 2, minus, 0.0) + jnp.where(sub >= 6, edge, 0.0))
        return jnp.concatenate(tiles, axis=0)

    for dx in (-1, 0, 1):
        own = s.part_t if dx == 0 else land[(dx, 0, 0)]
        for index in range(own.shape[0]):
            s.sums[dx + 1][index] = assembled(own[index], land[(dx, -1, 0)][index], land[(dx, 1, 0)][index])
        for which in range(2):
            dz = 2 * which - 1
            for pack in range(land[(dx, 0, dz)].shape[0]):
                s.sumz[dx + 1][which, pack] = assembled(
                    land[(dx, 0, dz)][pack], land[(dx, -1, dz)][pack], land[(dx, 1, dz)][pack]
                )

    shape = (rows + 16, LANES)
    lane = iota(shape, 1)
    at_low, at_high = lane >= LANES - 2, (lane == length) | (lane == length + 1)
    inner = lane < length
    above = (lane >= length - 2) & (lane < length + 6)
    below = (lane >= LANES - 6) | (lane < 2)
    even = parity_of(*shape)

    def turned(value, shift):
        shift = shift % LANES
        return pltpu.roll(value, shift, 1) if shift else value

    def plane_of(dx, number):
        if number < 8:
            index, slots, size, first = number, number, side, 0
            base = 0
        elif number >= count - 8:
            index, slots, size, first = number - (count - 8), 8 + number - (count - 8), side, count - 8
            base = side + 1
        else:
            index, slots, size, first = number - 8, number - 8, plan.middle, 8
            base = 2 * side + 1
        pack = 0 if number < 8 or number >= count - 8 else 1
        extra = side
        if dx == -1:
            base, extra = 0, side
        if dx == 1:
            base, extra = 1, 0
        total = s.sums[dx + 1]
        main = turned(total[base + index % size], -(index // size) * length)
        low = turned(total[extra], -2 * number)
        high = low if length == 64 else turned(total[extra], length - 64 - 2 * number)
        value = jnp.where(inner, main, jnp.where(at_low, low, jnp.where(at_high, high, 0.0)))
        far = s.sumz[dx + 1]
        from_above = turned(far[0, pack], length - 2 - 8 * slots)
        from_below = turned(far[1, pack], LANES - 6 - 8 * slots)
        return value + (jnp.where(above, from_above, 0.0) + jnp.where(below, from_below, 0.0))

    def plane(number):
        spot = number - 2 * plan.next.margins[0]
        total = None
        for dx, place in ((0, spot), (-1, spot - plan.block1[0]), (1, spot + plan.block1[0])):
            index = place + 2
            allowed = {0: (0, count), -1: (0, 8), 1: (count - 8, count)}[dx]
            if allowed[0] <= index < allowed[1]:
                value = plane_of(dx, index)
                total = value if total is None else total + value
        return total

    for number in range(plan.next.count):
        first, second = plane(2 * number), plane(2 * number + 1)
        s.next.f[number] = jnp.where(even, first, second)
        s.next.g[number] = jnp.where(even, second, first)


def solve(plan, s, number):
    grid, v = plan.levels[number], s.levels[number]
    even = parity_of(grid.rows, LANES, grid.step)
    count, step = grid.count, grid.step
    grid.first(v, 0, count)
    small = count * grid.rows <= 64

    def sweep():
        if small:
            grid.pair(v, even)
            return
        grid.half(v, 0, even, 0, count)
        grid.half(v, 1, even, 0, count)

    grid.half(v, 1, even, 0, count)
    sweep()
    pairs = s.pairs
    height = max(grid.rows, 16)
    if grid.rows < height:
        pairs[0:count, grid.rows : height] = jnp.zeros((count, height - grid.rows, LANES), F32)
    for spot, value in grid.residue(v, even, 0, count):
        if grid.rows > grid.block[1]:
            value = jnp.where(iota(value.shape, 0) < grid.block[1], value, 0.0)
        pairs[spot, 0 : grid.rows] = value
    sums = pair_sums(pairs, height, count)
    row, column = iota((LANES, LANES), 0), iota((LANES, LANES), 1)
    if number + 1 < len(plan.levels):
        below, under = plan.levels[number + 1], s.levels[number + 1]
        same = parity_of(below.rows, LANES, below.step)
        lane = iota((below.rows, LANES), 1)
        coarse = []
        for spot in range(count):
            value = sums[spot][: below.rows]
            value = 0.5 * (value + pltpu.roll(value, LANES - step, 1))
            coarse.append(jnp.where((lane % below.step == 0) & (lane < step * grid.block[2]), value, 0.0))
        for spot in range(below.count):
            one, two = coarse[2 * spot], coarse[2 * spot + 1]
            under.f[spot] = jnp.where(same, one, two)
            under.g[spot] = jnp.where(same, two, one)
        solve(plan, s, number + 1)
        for spot in range(count):
            plane = below.planes(under, same, spot)
            plane = plane + pltpu.roll(plane, step, 1)
            pairs[spot, pl.ds(0, below.rows, stride=2), :] = plane
            pairs[spot, pl.ds(1, below.rows, stride=2), :] = plane
        for spot in range(count):
            grid.put(v.B, spot + 1, grid.get(v.B, spot + 1) + pairs[spot, 0 : grid.rows])
    else:
        nx, ny, nz = plan.dense
        size = nx * ny * nz
        tall = height // 2
        flat = sums.reshape(count * (height // 2), LANES)
        down = weights((LANES, LANES), (row // (2 * step) == column % nz) & (row < step * grid.block[2]), 0.5)
        many = dot(flat, down).reshape(count, tall, LANES)
        wide = up_to(size, LANES) // LANES
        here, lane = iota((tall, LANES), 0), iota((tall, LANES), 1)
        parts = []
        for vector in range(wide):
            cell = (vector * LANES + lane) // nz
            total = jnp.zeros((tall, LANES), F32)
            for spot in range(nx):
                total = total + jnp.where((cell == spot * ny + here) & (here < ny), many[spot], 0.0)
            parts.append(total)
        left = jnp.concatenate(parts, axis=1)[:, :size]
        high, middle, low = pieces(left)
        stack = jnp.concatenate([high, middle, low], axis=0)
        matrix = s.matrix
        one = product(stack, matrix[0])
        two = product(stack[: 2 * tall], matrix[1])
        three = product(high, matrix[2])
        total = one[:tall] + ((one[tall : 2 * tall] + one[2 * tall :]) + ((two[:tall] + two[tall:]) + three))
        answer = jnp.sum(total, axis=0, keepdims=True)
        here, lane = iota((grid.rows, LANES), 0), iota((grid.rows, LANES), 1)
        planes = []
        for spot in range(nx):
            value = jnp.zeros((grid.rows, LANES), F32)
            for vector in range(wide):
                if (vector + 1) * LANES <= spot * ny * nz or vector * LANES >= (spot + 1) * ny * nz:
                    continue
                piece = jnp.broadcast_to(answer[:, vector * LANES : (vector + 1) * LANES], value.shape)
                cell = (vector * LANES + lane) // nz
                value = jnp.where(cell == spot * ny + here // 2, piece, value)
            planes.append(value)
        spread = weights(
            (LANES, LANES),
            (column // (2 * step) == row % nz) & (column < step * grid.block[2]) & (column % step == 0),
            1.0,
        )
        flat = dot(jnp.concatenate(planes, axis=0), spread).reshape(count, grid.rows, LANES)
        for spot in range(count):
            grid.put(v.B, spot + 1, grid.get(v.B, spot + 1) + flat[spot])
    sweep()
    sweep()


def first_black(plan, s, even):
    top, high, wide = plan.top, plan.block[1], plan.width
    lane = iota((high, wide), 1)
    none = jnp.zeros((high, LANES), F32)

    def load(number, shift=0, begin=0, size=high):
        parts = [ref[number, 8 + begin + shift : 8 + begin + shift + size] for ref in s.top.R[:-1]]
        return parts[0] if len(parts) == 1 else jnp.concatenate(parts, axis=1)

    for number in range(1, top.count - 1):
        total = jnp.where(even, load(number + 2), load(number))
        edge, side = jnp.zeros((8, wide), F32), none
        if top.zone(number) == 1:
            here = load(number + 1)
            left, right = pltpu.roll(here, 1, 1), pltpu.roll(here, wide - 1, 1)
            beside_z = jnp.where(lane == 0, 0.0, left) + jnp.where(lane == wide - 1, 0.0, right)
            total = (here + total) + (load(number + 1, -1) + load(number + 1, 1)) + along * beside_z
            total = total + s.top.g[number, 0:high, 0:wide]
            edge = load(number + 1, -1, high, 8) + load(number + 1, 1, high, 8)
            first, last = left[:, :LANES], right[:, wide - LANES :]
            spot = lane[:, :LANES]
            side = along * (jnp.where(spot == 0, first, 0.0) + jnp.where(spot == LANES - 1, last, 0.0))
        side = jnp.concatenate([side, none[:8]], axis=0)
        value = jnp.concatenate([jnp.concatenate([total, edge], axis=0), side], axis=1)
        top.put(s.top.B, number + 1, value * s.top.m[top.zone(number)])


def kernel(plan, tree, density, dense, potential, *refs):
    held = jax.tree.unflatten(tree, refs)
    s = types.SimpleNamespace(**{key: named(value) for key, value in held.items()})
    counts, block, total = plan.counts, plan.block, plan.total
    top, wide, next_ = plan.top, plan.wide, plan.next
    place = tuple(lax.axis_index(axis) for axis in AXES)
    paired = counts[2] % 2 == 0
    kinds = 2 if paired else 1

    def slot_of(x, y, z):
        kind, rest = (lax.rem(z, 2), lax.div(z, 2)) if paired and not isinstance(z, int) else (z % kinds, z // kinds)
        return kind * (total // kinds) + (x * counts[1] + y) * (counts[2] // kinds) + rest

    me = slot_of(*place)
    padded = block[2] != plan.width

    loads = [pltpu.make_async_copy(density, s.raw if padded else s.own, sem(s, OWN))]
    loads[0].start()
    if not padded:
        loads.append(
            pltpu.make_async_copy(
                density,
                s.field.at[pl.ds(8, block[0]), pl.ds(0, block[1]), pl.ds(0, block[2])],
                sem(s, FIELD),
            )
        )
    fill = pltpu.make_async_copy(dense, s.matrix, sem(s, MATRIX))

    for ref in s.land + [s.swap_land, s.swap_side]:
        ref[...] = jnp.zeros(ref.shape, F32)

    axes = [partners(place[axis], counts[axis]) for axis in range(3)]
    offsets = [
        (a, b, c) for a in range(counts[0]) for b in range(counts[1]) for c in range(counts[2]) if (a, b, c) != (0, 0, 0)
    ]
    offsets.sort(key=lambda off: -(off[0] + off[1] + off[2] / 2))

    def peer(off, way):
        target = tuple(axes[axis][off[axis]][way] for axis in range(3))
        return target, slot_of(*target)

    other = peer(offsets[0], 0)[0]
    barrier = pltpu.get_barrier_semaphore()
    close = max(counts) <= 4
    waited = total - 1
    if close:
        waited = 1
        for axis in range(3):
            waited = waited * (1 + jnp.minimum(place[axis], 2) + jnp.minimum(counts[axis] - 1 - place[axis], 2))
        waited = waited - 1
    for off in offsets:
        target = peer(off, 0)[0]
        apart = [target[axis] - place[axis] for axis in range(3) if off[axis] and counts[axis] > 3]
        near = None
        for step in apart if close else []:
            here = (step <= 2) & (step >= -2)
            near = here if near is None else near & here
        if near is None:
            pl.semaphore_signal(barrier, inc=1, device_id=target, device_id_type=MESH)
            continue

        @pl.when(near)
        def _():
            pl.semaphore_signal(barrier, inc=1, device_id=target, device_id_type=MESH)

    for ref in [s.top.f, s.top.g] + s.top.R + s.top.B:
        ref[...] = jnp.zeros(ref.shape, F32)
    for v, grid in ((s.top, top), (s.wide, wide), (s.next, next_)):
        grid.guard(v)
        grid.masks(v, place, counts)
    for v, grid in zip(s.levels, plan.levels):
        grid.guard(v)
        grid.masks(v, (0, 0, 0), (1, 1, 1))
    loads[0].wait()
    for load in loads[1:] + [fill]:
        load.start()
    own = s.own
    if padded:
        own[...] = jnp.zeros(own.shape, F32)
        own[:, :, 0 : block[2]] = s.raw[...]

    even_own = parity_of(block[1], plan.width)
    for number in range(top.inner):
        one, two = own[2 * number], own[2 * number + 1]
        red = jnp.where(even_own, one, two)
        spot = number + top.margins[0]
        s.top.f[spot, 0 : block[1], 0 : plan.width] = red
        s.top.g[spot, 0 : block[1], 0 : plan.width] = jnp.where(even_own, two, one)
        for tile in range(plan.width // LANES):
            piece = red[:, tile * LANES : (tile + 1) * LANES] * inverse
            s.top.R[tile][spot + 1, 8 : 8 + block[1]] = piece
            s.top.R[tile][spot + 1, 8 + top.rows :] = piece[0:8]
    even_top = parity_of(top.rows, top.lanes)
    count = top.count
    if top.lanes == plan.width + LANES:
        first_black(plan, s, even_own)
    else:
        top.half(s.top, 1, even_top, 1, count - 1)
    top.half(s.top, 0, even_top, 1, count - 1)
    top.half(s.top, 1, even_top, 0, count)
    for number, value in top.residue(s.top, even_top, 0, count):
        for tile in range(plan.tiles):
            piece = value[:, tile * LANES : (tile + 1) * LANES]
            s.rows[tile][number, 0 : top.rows] = piece
            s.rows[tile][number, top.rows : top.rows + 8] = piece[block[1] :]
    flat = jnp.concatenate(
        [
            pair_sums(s.rows[tile], block[1] + 16, count).reshape(count * plan.high, LANES)
            for tile in range(plan.tiles)
        ],
        axis=1,
    )

    def fine_cell(shape, dim):
        index = iota(shape, dim)
        used = (index < block[2] + 4) | (index >= top.lanes - 4)
        cell = half_down(local_of(index, block[2], 4, top.lanes))
        return jnp.where(cell < 0, cell + LANES, cell), used

    shape = (top.lanes, LANES)
    cell, used = fine_cell(shape, 0)
    down = weights(shape, (cell == iota(shape, 1)) & used, 0.5)
    s.part[...] = dot(flat, down).reshape(count, plan.high, LANES)
    pack_part(plan, s)

    lane = iota((block[1], LANES), 1)
    for side in range(2):
        begin = 0 if side == 0 else block[2] - 8
        tile = begin // LANES
        for pack in range(plan.far_packs):
            value = jnp.zeros((block[1], LANES), F32)
            for slot in range(16):
                plane = own[16 * pack + slot, :, tile * LANES : (tile + 1) * LANES]
                moved = pltpu.roll(plane, (8 * slot - begin) % LANES, 1)
                value = jnp.where(lane // 8 == slot, moved, value)
            s.far[side, pack] = value
    pl.semaphore_wait(barrier, waited)
    part = functools.partial(send_part, plan, s, place)
    far = functools.partial(send_far, plan, s, place)
    each(place, counts, part)

    each(place, counts, far)
    field, far_land = s.field, s.far_land
    if padded:
        field[8 : 8 + block[0], 0 : block[1], 0 : plan.width] = own[...]
    for dim, step in ((0, -1), (0, 1), (1, -1), (1, 1), (2, -1), (2, 1)):
        steps = tuple(step if which == dim else 0 for which in range(3))

        @pl.when(jnp.logical_not(exists(place, steps, counts)))
        def _():
            if dim == 0:
                begin = 0 if step < 0 else 8 + block[0]
                field[begin : begin + 8] = jnp.zeros((8,) + field.shape[1:], F32)
                pack = 0 if step < 0 else plan.far_packs + 1
                far_land[:, pack] = jnp.zeros((2,) + far_land.shape[2:], F32)
            if dim == 1:
                begin = block[1] if step > 0 else block[1] + 8
                field[:, begin : begin + 8] = jnp.zeros((field.shape[0], 8, field.shape[2]), F32)
                far_land[:, :, begin : begin + 8] = jnp.zeros(far_land.shape[:2] + (8, LANES), F32)
            if dim == 2:
                far_land[(1 - step) // 2] = jnp.zeros(far_land.shape[1:], F32)

    wait_all(plan, s, place, size_part, PART + 1, other)
    gather_part(plan, s)
    even_next = parity_of(next_.rows, LANES)
    n = next_.count
    next_.first(s.next, 0, n)
    next_.half(s.next, 1, even_next, 1, n - 1)
    next_.half(s.next, 0, even_next, 2, n - 2)
    next_.half(s.next, 1, even_next, 2, n - 2)
    pairs = s.pairs
    rows1 = plan.block1[1]
    height = max(rows1, 16)
    if rows1 < height:
        pairs[0 : next_.inner, rows1:height] = jnp.zeros((next_.inner, height - rows1, LANES), F32)
    for number, value in next_.residue(s.next, even_next, 3, n - 3):
        pairs[number - 3, 0:rows1] = value[0:rows1]
    flat = pair_sums(pairs, height, next_.inner).reshape(next_.inner * (height // 2), LANES)
    row, column = iota((LANES, LANES), 0), iota((LANES, LANES), 1)
    down = weights((LANES, LANES), (row // 2 == column) & (row < plan.block1[2]), 0.5)
    below = dot(flat, down).reshape(next_.inner, height // 2, LANES)
    length = plan.block2
    per = LANES // length[2]
    packed = jnp.zeros((8, LANES), F32)
    for plane in range(length[0]):
        moved = below[plane]
        if plane // per:
            moved = pltpu.roll(moved, length[1] * (plane // per), 0)
        if plane % per:
            moved = pltpu.roll(moved, length[2] * (plane % per), 1)
        packed = packed + moved
    s.mine[...] = packed
    slots = s.slots
    slots[me] = packed

    def send(number, slot):
        return pltpu.make_async_remote_copy(
            src_ref=s.mine,
            dst_ref=slots.at[slot],
            send_sem=sem(s, ALL),
            recv_sem=sem(s, ALL + 1),
            device_id=peer(offsets[number], 0)[0],
            device_id_type=MESH,
        )

    chosen = [number for number, off in enumerate(offsets) if off[2] % kinds == 0]

    def start_sends():
        for number in chosen:
            send(number, me).start()

    def forward():
        half = total // 2
        kind = lax.rem(place[2], 2) * half
        return pltpu.make_async_remote_copy(
            src_ref=slots.at[pl.ds(kind, half)],
            dst_ref=slots.at[pl.ds(kind, half)],
            send_sem=sem(s, PAIR),
            recv_sem=sem(s, PAIR + 1),
            device_id=peer((0, 0, 1), 0)[0],
            device_id_type=MESH,
        )

    start_sends()
    swap = functools.partial(send_swap, plan, s, place)
    pack_swap(plan, s)
    each(place, counts, swap)

    def finish_sends():
        for name in (ALL + 1, ALL):
            pltpu.make_async_remote_copy(
                src_ref=s.bytes.at[pl.ds(0, len(chosen))],
                dst_ref=s.bytes.at[pl.ds(0, len(chosen))],
                send_sem=sem(s, name),
                recv_sem=sem(s, name),
                device_id=other,
                device_id_type=MESH,
            ).wait_recv()

    wait_all(plan, s, place, size_far, FAR + 1, other)
    if not padded:
        loads[1].wait()
    base = wide.lanes - LANES
    shape = (wide.rows, LANES)
    lane = iota(shape, 1)
    even_wide = parity_of(wide.rows, wide.lanes)
    above = block[2] - base

    def wide_plane(number):
        pack, slot = (number + 8) // 16, (number + 8) % 16
        high = pltpu.roll(far_land[0, pack], (above - 8 * slot) % LANES, 1)
        low = pltpu.roll(far_land[1, pack], (LANES - 8 - 8 * slot) % LANES, 1)
        old = field[number, :, 0:LANES] if base == 0 else 0.0
        value = jnp.where((lane >= above) & (lane < above + 8), high, old)
        value = jnp.where(lane >= LANES - 8, low, value)
        return value if base == 0 else jnp.concatenate([field[number, :, 0:base], value], axis=1)

    for number in range(wide.count):
        one, two = wide_plane(2 * number), wide_plane(2 * number + 1)
        s.wide.f[number] = jnp.where(even_wide, one, two)
        s.wide.g[number] = jnp.where(even_wide, two, one)
    n = wide.count
    wide.first(s.wide, 0, n)
    wide.half(s.wide, 1, even_wide, 1, n - 1)
    wide.half(s.wide, 0, even_wide, 1, n - 1)
    wide.half(s.wide, 1, even_wide, 2, n - 2)
    wider = iota((8, wide.lanes), 0) < 4

    def narrow(value):
        both = jnp.where(wider, value[block[1] : block[1] + 8], value[block[1] + 8 :])
        value = jnp.concatenate([value[: block[1]], both], axis=0)
        if top.lanes != wide.lanes:
            value = jnp.concatenate([value[:, : top.lanes - LANES], value[:, -LANES:]], axis=1)
        return value

    shift = wide.margins[0] - top.margins[0]
    for number in range(count):
        s.top.f[number] = narrow(s.wide.f[number + shift])
        s.top.g[number] = narrow(s.wide.g[number + shift])
        top.put(s.top.B, number + 1, narrow(wide.get(s.wide.B, number + shift + 1)))

    finish_sends()
    if paired:
        forward().start()
        forward().wait()
    fill.wait()
    lane = iota((8, LANES), 1)
    whole = s.whole
    first = plan.levels[0]

    def place_x(which):
        for second in range(counts[1]):
            tiles = [slots[slot_of(which, second, third)] for third in range(counts[2])]
            for spot in range(per):
                value = jnp.zeros((8, LANES), F32)
                for third in range(counts[2]):
                    turn = (length[2] * (third - spot)) % LANES
                    moved = pltpu.roll(tiles[third], turn, 1) if turn else tiles[third]
                    value = jnp.where(lane // length[2] == third, moved, value)
                for group in range(8 // length[1]):
                    plane = which * length[0] + group * per + spot
                    whole[plane, second * length[1] : (second + 1) * length[1], :] = value[
                        group * length[1] : (group + 1) * length[1]
                    ]

    for which in range(counts[0]):
        place_x(which)
    even_first = parity_of(first.rows, LANES)
    for number in range(first.count):
        one, two = whole[2 * number], whole[2 * number + 1]
        s.levels[0].f[number] = jnp.where(even_first, one, two)
        s.levels[0].g[number] = jnp.where(even_first, two, one)
    solve(plan, s, 0)
    solved = s.solved
    for number in range(3):
        solved[number] = jnp.zeros((first.rows, LANES), F32)
        solved[first.block[0] + 3 + number] = jnp.zeros((first.rows, LANES), F32)
    for plane in range(first.block[0]):
        solved[plane + 3] = first.planes(s.levels[0], even_first, plane)

    wait_all(plan, s, place, size_swap, SWAP + 1, other)
    wait_all(plan, s, place, size_swap, SWAP, other)
    shape = (LANES, LANES)
    index = iota(shape, 1)
    spot = local_of(index, plan.block1[2], 8, LANES)
    used = (index < plan.block1[2] + 8) | (index >= LANES - 8)
    lanes_to = weights(shape, (half_down(spot) + place[2] * length[2] == iota(shape, 0)) & used, 1.0)
    n = next_.count
    flat = jnp.concatenate([solved[place[0] * length[0] + number] for number in range(n)], axis=0)
    flat = dot(flat, lanes_to).reshape(n, first.rows, LANES)
    spread = s.spread
    spread[:, 0:16] = jnp.zeros((n, 16, LANES), F32)
    spread[:, 16 + 2 * first.rows :] = jnp.zeros((n, 16, LANES), F32)
    spread[0:n, pl.ds(16, first.rows, stride=2), :] = flat
    spread[0:n, pl.ds(17, first.rows, stride=2), :] = flat
    start = 16 + place[1] * rows1
    for number in range(n):
        tiles = [
            spread[number, pl.ds(pl.multiple_of(start + shift, 8), size), :]
            for shift, size in ((0, rows1), (rows1, 8), (-8, 8))
        ]
        next_.put(s.next.B, number + 1, swapped(plan, s, number) + jnp.concatenate(tiles, axis=0))
    for colour, skip in ((0, 0), (1, 1), (0, 1), (1, 2)):
        next_.half(s.next, colour, even_next, skip, n - skip)

    pick = iota((8, LANES), 0) < 4
    planes = []
    for number in range(count):
        value = next_.planes(s.next, even_next, number + 2 * next_.margins[0] - top.margins[0])
        edge = jnp.where(pick, value[rows1 : rows1 + 8], value[rows1 + 8 :])
        planes.append(jnp.concatenate([value[:rows1], edge], axis=0))
    shape = (LANES, top.lanes)
    cell, used = fine_cell(shape, 1)
    spreading = weights(shape, (cell == iota(shape, 0)) & used, 1.0)
    flat = dot(jnp.concatenate(planes, axis=0), spreading).reshape(count, plan.high, top.lanes)
    for tile in range(plan.tiles):
        piece = flat[:, :, tile * LANES : (tile + 1) * LANES]
        s.rows[tile][0:count, pl.ds(0, plan.high, stride=2), :] = piece
        s.rows[tile][0:count, pl.ds(1, plan.high, stride=2), :] = piece
    for number in range(count):
        tiles = []
        for tile in range(plan.tiles):
            rows = s.rows[tile]
            edge = jnp.where(pick, rows[number, block[1] : block[1] + 8], rows[number, block[1] + 8 : block[1] + 16])
            tiles.append(jnp.concatenate([rows[number, 0 : block[1]], edge], axis=0))
        top.put(s.top.B, number + 1, top.get(s.top.B, number + 1) + jnp.concatenate(tiles, axis=1))
    top.half(s.top, 0, even_top, 0, count)
    top.half(s.top, 1, even_top, 1, count - 1)
    top.half(s.top, 0, even_top, 1, count - 1)
    red = s.top.R
    even_out = parity_of(block[1], block[2])
    for number, value in top.totals(red, even_top, 1, top.margins[0], count - top.margins[0]):
        black = ((s.top.g[number] + value) * inverse)[0 : block[1], 0 : block[2]]
        old = top.get(red, number + 1)[0 : block[1], 0 : block[2]]
        plane = 2 * (number - top.margins[0])
        potential[plane] = jnp.where(even_out, old, black)
        potential[plane + 1] = jnp.where(even_out, black, old)
    wait_all(plan, s, place, size_part, PART, other)
    wait_all(plan, s, place, size_far, FAR, other)


def cycle_matrix(size, depth):
    def beside_sum(v):
        p = np.pad(v, ((0, 0), (1, 1), (1, 1), (1, 1)))
        total = p[:, 2:, 1:-1, 1:-1] + p[:, :-2, 1:-1, 1:-1] + p[:, 1:-1, 2:, 1:-1] + p[:, 1:-1, :-2, 1:-1]
        return total + along * (p[:, 1:-1, 1:-1, 2:] + p[:, 1:-1, 1:-1, :-2])

    def cycle(g, left):
        parity = np.indices(g.shape[1:]).sum(0) % 2

        def sweeps(v, number):
            for _ in range(number):
                for colour in (0, 1):
                    v = np.where(parity == colour, (g + beside_sum(v)) / centre, v)
            return v

        v = np.zeros_like(g)
        if left == 0:
            return sweeps(v, CSWEEPS)
        v = sweeps(v, 2)
        r = g - centre * v + beside_sum(v)
        x, y, z = (part // 2 for part in g.shape[1:])
        coarse = 4 * r.reshape(-1, x, 2, y, 2, z, 2).mean((2, 4, 6))
        e = cycle(coarse, left - 1)
        for dim in (1, 2, 3):
            e = np.repeat(e, 2, dim)
        return sweeps(v + e, 2)

    cells = size[0] * size[1] * size[2]
    found = cycle(np.eye(cells).reshape((cells,) + size), depth).reshape(cells, cells)
    parts = []
    for _ in range(3):
        parts.append(found.astype(np.float32).astype(jnp.bfloat16))
        found = found - parts[-1].astype(np.float64)
    return np.stack(parts)


def on_device(counts, density):
    plan = Plan(density.shape, counts)
    scratch, tree = jax.tree.flatten(plan.scratch())
    matrix = jnp.asarray(cycle_matrix(plan.dense, LEVELS - 1 - plan.dense_level))
    return pl.pallas_call(
        functools.partial(kernel, plan, tree),
        out_shape=jax.ShapeDtypeStruct(density.shape, F32),
        in_specs=[pl.BlockSpec(memory_space=pltpu.HBM)] * 2,
        out_specs=pl.BlockSpec(memory_space=pltpu.VMEM),
        scratch_shapes=scratch,
        compiler_params=pltpu.CompilerParams(
            collective_id=0, has_side_effects=True, vmem_limit_bytes=48 * 1024 * 1024
        ),
    )(
        pltpu.with_memory_space_constraint(density, pltpu.HBM),
        pltpu.with_memory_space_constraint(matrix, pltpu.HBM),
    )


def solution(mesh):
    counts = tuple(mesh.shape[axis] for axis in AXES)
    return jax.shard_map(
        functools.partial(on_device, counts),
        mesh=mesh,
        in_specs=(P("gx", "gy", "gz"),),
        out_specs=P("gx", "gy", "gz"),
        check_vma=False,
    )
```
